32 devices in a mesh: seq: 8 (over y, x, core), head: 4 (over z).
Axes of the slice: x: 2, y: 2, z: 4, core: 2. Of those that a mesh axis runs over, the one named last changes fastest.
Arguments:
- hidden: bfloat16 [16384, 1536], P('seq'), may hold values from -6 to 6
- segment_ids: int32 [16384], P('seq'), may hold values from 0 to 15, as said below
- norm_gain: float32 [1536], replicated, may hold values from 0.5 to 1.5
- w_gate: bfloat16 [1536, 3072], P(None, 'head'), may hold values from -0.15625 to 0.15625
- w_value: bfloat16 [1536, 3072], P(None, 'head'), may hold values from -0.15625 to 0.15625
- w_state: bfloat16 [1536, 256], P(None, 'head'), may hold values from -0.15625 to 0.15625
- w_step: bfloat16 [1536, 48], P(None, 'head'), may hold values from -0.15625 to 0.15625
- conv_value: float32 [4, 3072], P(None, 'head'), may hold values from -3 to 3
- conv_value_bias: float32 [3072], P('head'), may hold values from -3 to 3
- conv_state: float32 [4, 256], P(None, 'head'), may hold values from -3 to 3
- conv_state_bias: float32 [256], P('head'), may hold values from -3 to 3
- decay_log: float32 [48], P('head'), may hold values from -2 to 1
- step_bias: float32 [48], P('head'), may hold values from -5 to -1
- skip_gain: float32 [48], P('head'), may hold values from 0.5 to 1.5
- gate_gain: float32 [3072], P('head'), may hold values from 0.5 to 1.5
- w_out: bfloat16 [3072, 1536], P('head'), may hold values from -0.109375 to 0.109375
- cotangent: bfloat16 [16384, 1536], P('seq'), may hold values from -6 to 6
Outputs:
- mixed: bfloat16 [16384, 1536], P('seq')
- grad_hidden: float32 [16384, 1536], P('seq')
- grad_norm_gain: float32 [1536], replicated
- grad_w_gate: float32 [1536, 3072], P(None, 'head')
- grad_w_value: float32 [1536, 3072], P(None, 'head')
- grad_w_state: float32 [1536, 256], P(None, 'head')
- grad_w_step: float32 [1536, 48], P(None, 'head')
- grad_conv_value: float32 [4, 3072], P(None, 'head')
- grad_conv_value_bias: float32 [3072], P('head')
- grad_conv_state: float32 [4, 256], P(None, 'head')
- grad_conv_state_bias: float32 [256], P('head')
- grad_decay_log: float32 [48], P('head')
- grad_step_bias: float32 [48], P('head')
- grad_skip_gain: float32 [48], P('head')
- grad_gate_gain: float32 [3072], P('head')
- grad_w_out: float32 [3072, 1536], P('head')
The draws below stay inside these ranges and needn't reach their ends.
Inputs may be any that keep to these rules, and one draw needn't show every extreme that they name: `segment_ids`: entries start at 0 and rise by one at each document's first token, never falling; each document holds 1 to 2000 consecutive tokens and the first exactly 2000; no document starts at a token whose index is a multiple of 2048 other than 0.
All inputs are finite; a program needn't handle non-finite values.
Results may differ from the reference program's by a relative error of at most 0.0099.
Values may be sent and summed in bfloat16 or wider, within the bound.
A program may use at most 256 MiB of HBM per device.

```python
from functools import partial
import jax
import jax.numpy as jnp
from jax import lax

D = 1536
HEADS = 48
HEAD_DIM = 64
STATE = 128
CONV_K = 4
GROUP = 256
DOC_MOST = 2000
TOK_DEV = 2048
INNER = 3072
TOKENS = 16384


def draw_segment_ids(key, part):
    least = max(DOC_MOST // 10, 2)
    full_pairs = (TOKENS - DOC_MOST) // DOC_MOST
    top_id = 2 * full_pairs + min((TOKENS - DOC_MOST) % DOC_MOST, 1)
    count = full_pairs + 1
    firsts = jax.random.randint(key, (count,), least, DOC_MOST - least + 1, dtype=jnp.int32)
    bases = (DOC_MOST + DOC_MOST * jnp.arange(count, dtype=jnp.int32)).astype(jnp.int32)
    starts = jnp.stack([bases, bases + firsts], 1).reshape(-1).astype(jnp.int32)
    starts = starts - (starts % TOK_DEV == 0).astype(jnp.int32)
    position = jnp.arange(TOKENS, dtype=jnp.int32)
    counted = jnp.sum((starts[None, :] <= position[:, None]).astype(jnp.int32), 1).astype(jnp.int32)
    return jnp.minimum(counted, top_id).astype(jnp.int32)


def shard_levels(key, shape, shards, smallest, top_value):
    def one(axis_at, parts):
        steps = jax.random.uniform(jax.random.fold_in(jax.random.fold_in(key, 6), axis_at), (parts,), jnp.float32, smallest / len(shards), top_value / len(shards))
        return jnp.repeat(jnp.exp(steps), shape[axis_at] // parts).reshape((-1,) + (1,) * (len(shape) - axis_at - 1))

    factor_of = one(*shards[0])
    for cut in shards[1:]:
        factor_of = factor_of * one(*cut)
    return factor_of


def bell_draw(stream_key, extent, width, bound, cuts=(), kind=jnp.bfloat16):
    gain = shard_levels(stream_key, extent, cuts, -0.22, 0.18) if cuts else 1.0
    entries = jax.random.normal(stream_key, extent, jnp.float32) * width * gain
    return jnp.minimum(jnp.maximum(entries, -bound), bound).astype(kind)


def setup_inputs(seed: int = 0) -> dict:
    splits = jax.random.split(jax.random.key(seed), 18)
    return {
        "hidden": bell_draw(splits[0], (TOKENS, D), 1.0, 6.0, ((0, 8),)),
        "segment_ids": draw_segment_ids(jax.random.fold_in(splits[17], 71), 0),
        "norm_gain": jnp.clip(1.0 + 0.1 * jax.random.normal(splits[2], (D,), jnp.float32), 0.5, 1.5),
        "w_gate": bell_draw(splits[3], (D, INNER), D ** -0.5, 0.15625, ((1, 4),)),
        "w_value": bell_draw(splits[4], (D, INNER), D ** -0.5, 0.15625, ((1, 4),)),
        "w_state": bell_draw(splits[5], (D, 2 * STATE), D ** -0.5, 0.15625, ((1, 4),)),
        "w_step": bell_draw(splits[6], (D, HEADS), D ** -0.5, 0.15625, ((1, 4),)),
        "conv_value": bell_draw(splits[7], (CONV_K, INNER), CONV_K ** -0.5, 3.0, ((1, 4),), jnp.float32),
        "conv_value_bias": bell_draw(splits[8], (INNER,), 0.5, 3.0, ((0, 4),), jnp.float32),
        "conv_state": bell_draw(splits[9], (CONV_K, 2 * STATE), CONV_K ** -0.5, 3.0, ((1, 4),), jnp.float32),
        "conv_state_bias": bell_draw(splits[10], (2 * STATE,), 0.5, 3.0, ((0, 4),), jnp.float32),
        "decay_log": jnp.clip(-2.0 + 3.0 * jax.random.uniform(splits[11], (HEADS,), jnp.float32) ** shard_levels(splits[11], (HEADS,), ((0, 4),), -0.2, 0.2), -2.0, 1.0),
        "step_bias": jnp.clip(-5.0 + 4.0 * jax.random.uniform(splits[12], (HEADS,), jnp.float32) ** shard_levels(splits[12], (HEADS,), ((0, 4),), -0.2, 0.2), -5.0, -1.0),
        "skip_gain": jnp.clip(0.5 + 1.0 * jax.random.uniform(splits[13], (HEADS,), jnp.float32) ** shard_levels(splits[13], (HEADS,), ((0, 4),), -0.2, 0.2), 0.5, 1.5),
        "gate_gain": jnp.clip(1.0 + 0.1 * jax.random.normal(splits[14], (INNER,), jnp.float32), 0.5, 1.5),
        "w_out": bell_draw(splits[15], (INNER, D), INNER ** -0.5, 0.109375, ((0, 4),)),
        "cotangent": bell_draw(splits[16], (TOKENS, D), 1.0, 6.0, ((0, 8),)),
    }


EPSILON = 1e-05
VERY_NEGATIVE = -1e+30
PRECISE = lax.Precision.HIGHEST

@jax.custom_vjp
def low(v):
    return lax.optimization_barrier(v.astype(jnp.bfloat16)).astype(jnp.float32)

@jax.custom_vjp
def low_back(v):
    return v

def low_keep(v):
    return (low(v), None)

def low_pass(kept, grad):
    return (grad,)

def back_keep(v):
    return (v, None)

def back_low(kept, grad):
    return (low(grad),)
low.defvjp(low_keep, low_pass)
low_back.defvjp(back_keep, back_low)

def causal_conv(conv_in, kernel, kernel_bias, segments):
    tokens = conv_in.shape[0]
    reach_back = kernel.shape[0] - 1
    padded = jnp.concatenate([jnp.zeros((reach_back, conv_in.shape[1]), jnp.float32), conv_in], 0)
    seg_padded = jnp.concatenate([jnp.full((reach_back,), -1, jnp.int32), segments.astype(jnp.int32)], 0)
    summed = jnp.zeros((tokens, conv_in.shape[1]), jnp.float32) + kernel_bias[None, :]
    for tap_index in range(kernel.shape[0]):
        same_doc = (seg_padded[tap_index:tap_index + tokens] == segments).astype(jnp.float32)
        summed = summed + kernel[tap_index][None, :] * padded[tap_index:tap_index + tokens] * same_doc[:, None]
    return jax.nn.silu(summed)

def ssd_group(carried_in, block_item):
    carried_state, seg_before = carried_in
    values, step_size, log_decay, b_proj, c_proj, segments = block_item
    cumulative = jnp.cumsum(log_decay, axis=0)
    heads_first = cumulative.T
    position = jnp.arange(segments.shape[0])
    visible_pairs = (segments[:, None] == segments[None, :]) & (position[:, None] >= position[None, :])
    log_ratio = heads_first[:, :, None] - heads_first[:, None, :]
    decays = jnp.exp(jnp.where(visible_pairs[None], log_ratio, VERY_NEGATIVE))
    scores = jnp.einsum('in,jn->ij', c_proj, b_proj, precision=PRECISE)
    scaled = values * step_size[:, :, None]
    result = jnp.einsum('hij,jhp->ihp', decays * scores[None], scaled, precision=PRECISE)
    from_start = jnp.exp(jnp.where((segments == seg_before)[:, None], cumulative, VERY_NEGATIVE))
    result = result + jnp.einsum('ih,in,hpn->ihp', from_start, c_proj, carried_state, precision=PRECISE)
    to_end = jnp.exp(jnp.where((segments == segments[-1])[:, None], cumulative[-1:] - cumulative, VERY_NEGATIVE))
    new_state = from_start[-1][:, None, None] * carried_state + jnp.einsum('jh,jhp,jn->hpn', to_end, scaled, b_proj, precision=PRECISE)
    return ((new_state, segments[-1]), result)

def ssd_scan(values, step_size, log_decay, b_proj, c_proj, segments):
    tokens = values.shape[0]
    blocks = tokens // GROUP
    items = (values.reshape(blocks, GROUP, HEADS, HEAD_DIM), step_size.reshape(blocks, GROUP, HEADS), log_decay.reshape(blocks, GROUP, HEADS), b_proj.reshape(blocks, GROUP, STATE), c_proj.reshape(blocks, GROUP, STATE), segments.reshape(blocks, GROUP).astype(jnp.int32))
    initial = (jnp.zeros((HEADS, HEAD_DIM, STATE), jnp.float32), jnp.int32(-1))
    ignored, outputs = lax.scan(jax.checkpoint(ssd_group), initial, items)
    return outputs.reshape(tokens, HEADS, HEAD_DIM)

def forward(hidden, norm_gain, w_gate, w_value, w_state, w_step, conv_value, conv_value_bias, conv_state, conv_state_bias, decay_log, step_bias, skip_gain, gate_gain, w_out, segment_ids):
    inverse = lax.rsqrt(lax.optimization_barrier(jnp.mean(hidden * hidden, -1, keepdims=True)) + EPSILON)
    normed = low(hidden * inverse * norm_gain)
    weights = jnp.concatenate([w_gate, w_value, w_state, w_step], 1)
    projected = jnp.dot(normed, weights, precision=PRECISE, preferred_element_type=jnp.float32)
    gate_raw = low_back(projected[:, :INNER])
    conv_in = low(low_back(projected[:, INNER:2 * INNER + 2 * STATE]))
    step_raw = low_back(projected[:, 2 * INNER + 2 * STATE:])
    kernel = jnp.concatenate([conv_value, conv_state], 1)
    kernel_bias = jnp.concatenate([conv_value_bias, conv_state_bias])
    conv_out = causal_conv(conv_in, kernel, kernel_bias, segment_ids)
    values = conv_out[:, :INNER].reshape(-1, HEADS, HEAD_DIM)
    both_low = low(conv_out[:, INNER:])
    b_proj = both_low[:, :STATE]
    c_proj = both_low[:, STATE:]
    step_size = jax.nn.softplus(step_raw + step_bias)
    log_decay = -jnp.exp(decay_log) * step_size
    ssm_out = ssd_scan(values, step_size, log_decay, b_proj, c_proj, segment_ids) + skip_gain[None, :, None] * values
    gated = ssm_out.reshape(-1, INNER) * jax.nn.silu(gate_raw)
    gate_normed = low(gated * lax.rsqrt(lax.optimization_barrier(jnp.mean(gated * gated, -1, keepdims=True)) + EPSILON) * gate_gain)
    return hidden + jnp.dot(gate_normed, w_out, precision=PRECISE, preferred_element_type=jnp.float32)

def reference(hidden, segment_ids, norm_gain, w_gate, w_value, w_state, w_step, conv_value, conv_value_bias, conv_state, conv_state_bias, decay_log, step_bias, skip_gain, gate_gain, w_out, cotangent):
    inputs = (hidden.astype(jnp.float32), norm_gain, w_gate.astype(jnp.float32), w_value.astype(jnp.float32), w_state.astype(jnp.float32), w_step.astype(jnp.float32), conv_value, conv_value_bias, conv_state, conv_state_bias, decay_log, step_bias, skip_gain, gate_gain, w_out.astype(jnp.float32))
    mixed, pullback = jax.vjp(partial(forward, segment_ids=segment_ids), *inputs)
    gradients = pullback(cotangent.astype(jnp.float32))
    return (mixed.astype(jnp.bfloat16), gradients[0], gradients[1], gradients[2], gradients[3], gradients[4], gradients[5], gradients[6], gradients[7], gradients[8], gradients[9], gradients[10], gradients[11], gradients[12], gradients[13], gradients[14])
```

```python
from functools import partial

import jax
import jax.numpy as jnp
from jax import lax
from jax.experimental import pallas as pl
from jax.experimental.layout import Layout, with_layout_constraint
from jax.experimental.pallas import tpu as pltpu
from jax.sharding import PartitionSpec as P


EPSILON = 1e-05
VERY_NEGATIVE = -1e30
CHUNK = 256
SPAN = 128
STATE = 128
WIDTH = 64
LANES = 128
F32 = jnp.float32
BF16 = jnp.bfloat16
ONE = pl.Buffered(1)
EARLY = 40


def nn(a, b):
    return lax.dot_general(a, b, (((1,), (0,)), ((), ())), preferred_element_type=F32)


def nt(a, b):
    return lax.dot_general(a, b, (((1,), (1,)), ((), ())), preferred_element_type=F32)


def tn(a, b):
    return lax.dot_general(a, b, (((0,), (0,)), ((), ())), preferred_element_type=F32)


def exact(a, b):
    return lax.dot_general(
        a, b, (((1,), (0,)), ((), ())), preferred_element_type=F32, precision=lax.Precision.HIGHEST
    )


def iota(shape, axis):
    return lax.broadcasted_iota(jnp.int32, shape, axis)


def pair_of(columns, pair):
    rows = columns.shape[0]
    first = jnp.broadcast_to(columns[:, 2 * pair : 2 * pair + 1], (rows, LANES))
    second = jnp.broadcast_to(columns[:, 2 * pair + 1 : 2 * pair + 2], (rows, LANES))
    return jnp.where(iota((rows, LANES), 1) < WIDTH, first, second)


def spread(columns, low, width):
    parts = [pair_of(columns, (low + at) // LANES) for at in range(0, width, LANES)]
    return jnp.concatenate(parts, 1) if len(parts) > 1 else parts[0]


def head_sums(values, low):
    shape = (values.shape[1], LANES)
    picks = jnp.where(iota(shape, 1) == (iota(shape, 0) + low) // WIDTH, 1.0, 0.0).astype(BF16)
    high, rest = halves(values)
    return nn(high, picks) + nn(rest, picks)


def groups(inner):
    return [(low, min(2 * LANES, inner - low)) for low in range(0, inner, 2 * LANES)]


def from_before(rows, previous, steps):
    turned = pltpu.roll(rows, steps, 0)
    head = pltpu.roll(previous, steps, 0)
    top = jnp.where(iota(head.shape, 0) < steps, head, turned[:8])
    return jnp.concatenate([top, turned[8:]], 0)


def from_after(rows, following, steps):
    count = rows.shape[0]
    turned = pltpu.roll(rows, count - steps, 0)
    tail = pltpu.roll(following, 8 - steps, 0)
    bottom = jnp.where(iota(tail.shape, 0) >= 8 - steps, tail, turned[count - 8 :])
    return jnp.concatenate([turned[: count - 8], bottom], 0)


def softplus(v):
    return jnp.maximum(v, 0.0) + jnp.log1p(jnp.exp(-jnp.abs(v)))


def sigmoid(v):
    return 0.5 + 0.5 * jnp.tanh(0.5 * v)


def halves(value):
    high = value.astype(BF16)
    return high, (value - high.astype(F32)).astype(BF16)


def column(tokens, index, width=LANES):
    return jnp.broadcast_to(tokens[:, index : index + 1], (tokens.shape[0], width))


def conv_taps(taps, rows, previous, visible):
    pre = taps[4:5] + taps[3:4] * rows
    shifted = [rows]
    for steps in range(1, 4):
        moved = from_before(rows, previous, steps) * visible[steps - 1]
        shifted.append(moved)
        pre = pre + taps[3 - steps : 4 - steps] * moved
    return pre, shifted


def mask_of(tokens, seg_row):
    same = tokens[:, 0:1] == seg_row
    count = tokens.shape[0]
    causal = iota((count, count), 0) >= iota((count, count), 1)
    return jnp.where(same & causal, 0.0, VERY_NEGATIVE)


def prepare_kernel(
    ws_ref, cs_ref, csb_ref, cv_ref, cvb_ref, decay_ref, bias_ref, skip_ref, norm_ref, gain_ref,
    packed_ref, taps_ref, heads_ref, norm_out_ref, gain_out_ref,
):
    width = ws_ref.shape[1]
    packed_ref[:, :width] = ws_ref[...]
    taps = jnp.concatenate([cs_ref[...], csb_ref[...][None], jnp.zeros((3, cs_ref.shape[1]), F32)], 0)
    taps = jnp.transpose(jnp.pad(taps, ((0, LANES - 8), (0, LANES - taps.shape[1]))))[: taps.shape[1]]
    for k in range(3):
        high = taps.astype(BF16)
        packed_ref[:, width + LANES * k : width + LANES * (k + 1)] = high
        taps = taps - high.astype(F32)
    inner = cv_ref.shape[1]
    taps_ref[...] = jnp.concatenate([cv_ref[...], cvb_ref[...][None], jnp.zeros((3, inner), F32)], 0)
    rows = [-jnp.exp(decay_ref[...])[None], bias_ref[...][None], skip_ref[...][None]]
    count = decay_ref.shape[0]
    heads_ref[...] = jnp.pad(
        jnp.concatenate(rows + [jnp.zeros((5, count), F32)], 0), ((0, 0), (0, LANES - count))
    )
    norm_out_ref[...] = norm_ref[...][None]
    gain_out_ref[...] = gain_ref[...][None]


def prepare(w_state_t, conv_state, conv_state_bias, conv_value, conv_value_bias, decay, bias, skip, norm, gain):
    state_local, width = w_state_t.shape
    inner = conv_value.shape[1]
    return pl.pallas_call(
        prepare_kernel,
        out_shape=[
            jax.ShapeDtypeStruct((state_local, width + 3 * LANES), BF16),
            jax.ShapeDtypeStruct((8, inner), F32),
            jax.ShapeDtypeStruct((8, LANES), F32),
            jax.ShapeDtypeStruct((1, width), F32),
            jax.ShapeDtypeStruct((1, inner), F32),
        ],
        name="prepare",
    )(w_state_t, conv_state, conv_state_bias, conv_value, conv_value_bias, decay, bias, skip, norm, gain)


def assemble_kernel(count, taps_value_ref, *refs):
    parts, (weights_ref, taps_ref, columns) = refs[:count], refs[count:]
    rows, width = parts[0].shape[0], weights_ref.shape[1]
    inner = taps_value_ref.shape[1]
    place = lax.axis_index("head")
    for steps, part in enumerate(parts):
        at = pl.multiple_of(lax.rem(place - steps + count, count) * rows, rows)
        weights_ref[pl.ds(at, rows), :] = part[:, :width]
        columns[pl.ds(at, rows), :] = sum(
            part[:, width + LANES * k : width + LANES * (k + 1)].astype(F32) for k in range(3)
        )
    taps_ref[:, :inner] = taps_value_ref[...]
    taps_ref[:, inner:] = jnp.transpose(columns[...])[:8]


def assemble(taps_value, parts):
    rows, width = parts[0].shape[0], parts[0].shape[1] - 3 * LANES
    inner, total = taps_value.shape[1], rows * len(parts)
    return pl.pallas_call(
        partial(assemble_kernel, len(parts)),
        out_shape=[
            jax.ShapeDtypeStruct((total, width), BF16),
            jax.ShapeDtypeStruct((8, inner + total), F32),
        ],
        scratch_shapes=[pltpu.VMEM((total, LANES), F32)],
        name="assemble",
    )(taps_value, *parts)


def project_kernel(x_ref, gain_ref, wg_ref, wv_ref, ws_ref, normed_ref, gate_ref, conv_ref, step_ref):
    x = x_ref[...].astype(F32)
    inverse = lax.rsqrt(jnp.mean(x * x, -1, keepdims=True) + EPSILON)
    normed = (x * inverse * gain_ref[...]).astype(BF16)
    normed_ref[...] = normed
    gate_ref[...] = nn(normed, wg_ref[...])
    conv_ref[...] = nn(normed, wv_ref[...]).astype(BF16)
    step = nt(normed, ws_ref[...])
    step_ref[...] = jnp.concatenate([step, jnp.zeros((CHUNK, LANES - step.shape[1]), F32)], 1)


def project(hidden, gain, w_gate, w_value, w_step_t):
    tokens, width = hidden.shape
    inner = w_gate.shape[1]
    rows = lambda n: pl.BlockSpec((CHUNK, n), lambda i: (i, 0))
    whole = lambda a: pl.BlockSpec(a.shape, lambda i: (0, 0), pipeline_mode=ONE)
    return pl.pallas_call(
        project_kernel,
        grid=(tokens // CHUNK,),
        in_specs=[rows(width), whole(gain), whole(w_gate), whole(w_value), whole(w_step_t)],
        out_specs=[rows(width), rows(inner), rows(inner), rows(LANES)],
        out_shape=[
            jax.ShapeDtypeStruct((tokens, width), BF16),
            jax.ShapeDtypeStruct((tokens, inner), F32),
            jax.ShapeDtypeStruct((tokens, inner), BF16),
            jax.ShapeDtypeStruct((tokens, LANES), F32),
        ],
        cost_estimate=pl.CostEstimate(
            flops=2 * tokens * width * (2 * inner + LANES),
            bytes_accessed=tokens * (4 * width + 6 * inner) + 4 * width * inner,
            transcendentals=0,
        ),
        name="project",
    )(hidden, gain, w_gate, w_value, w_step_t)


def scan_kernel(
    cv_ref, cs_ref, halo_ref, step_ref, ids_ref, before_ref, heads_ref, taps_ref,
    y_ref, bc_ref, cum_ref, reach_ref, enter_ref, end_ref, kept_ref, tok_ref, seg_ref,
    carry, state, offset, reached,
):
    at = pl.program_id(0)
    inner = cv_ref.shape[1]
    count = SPAN

    @pl.when(at == 0)
    def _():
        carry[...] = halo_ref[...].astype(F32)
        state[...] = jnp.zeros_like(state)
        offset[...] = jnp.zeros_like(offset)
        reached[...] = jnp.ones_like(reached)

    blocks = ids_ref.shape[0]
    own_row = lambda index: ids_ref[pl.ds(index, 1), :]
    previous = jnp.where(lax.axis_index("seq") == 0, -1, before_ref[blocks - 1 : blocks])
    here = own_row(at)
    earlier = jnp.where(at == 0, previous, own_row(jnp.maximum(at - 1, 0)))
    later = jnp.where(at == blocks - 1, -2, own_row(jnp.minimum(at + 1, blocks - 1)))
    lane = iota((1, LANES), 1)
    seg = here.astype(F32)
    flags = [here == here]
    for steps in range(1, 4):
        moved = jnp.where(lane < steps, pltpu.roll(earlier, steps, 1), pltpu.roll(here, steps, 1))
        flags.append(moved == here)
    for steps in range(1, 4):
        end = lane >= LANES - steps
        moved = jnp.where(end, pltpu.roll(later, LANES - steps, 1), pltpu.roll(here, LANES - steps, 1))
        flags.append(moved == here)
    first_id = own_row(0)[:, :1]
    flags.append(here == earlier[:, LANES - 1 :])
    flags.append(here == here[:, LANES - 1 :])
    flags.append((here == first_id) & (previous[:, LANES - 1 :] == first_id))
    rows = [seg] + [jnp.where(flag, 1.0, 0.0) for flag in flags[1:]]
    tokens = jnp.transpose(jnp.concatenate(rows + [jnp.zeros((LANES - len(rows), LANES), F32)], 0))
    tok_ref[...] = tokens
    seg_ref[0] = jnp.broadcast_to(seg, (8, LANES))
    heads = heads_ref[...]
    step = softplus(step_ref[...] + heads[1:2])
    log_decay = heads[0:1] * step
    lower = jnp.where(iota((count, count), 0) >= iota((count, count), 1), 1.0, 0.0)
    cum = exact(lower, log_decay)
    cum_ref[...] = cum
    kept_ref[0] = reached[...]
    reach = jnp.exp(cum + offset[0:1]) * column(tokens, 9)
    reach_ref[...] = reach
    last = cum[count - 1 : count]
    offset[...] = offset[...] + last
    reached[...] = jnp.broadcast_to(reach[count - 1 : count], reached.shape)
    start = jnp.exp(cum) * column(tokens, 7)
    end = jnp.exp(last - cum) * column(tokens, 8)
    through = start[count - 1 : count]
    cum_t = jnp.transpose(cum)
    visible = [column(tokens, 1 + k, 2 * LANES) for k in range(3)]

    def conv(ref, low, at_column, width):
        rows = ref[:, low : low + width].astype(F32)
        wide = slice(at_column, at_column + width)
        pre, _ = conv_taps(taps_ref[:, wide], rows, carry[:, wide], [v[:, :width] for v in visible])
        carry[:, wide] = rows[count - 8 :]
        return pre * sigmoid(pre)

    both = conv(cs_ref, 0, inner, 2 * STATE).astype(BF16)
    bc_ref[...] = both
    b_low, c_low = both[:, :LANES], both[:, LANES:]
    scores = nt(c_low, b_low)
    hidden_pairs = mask_of(tokens, seg)
    enter_ref[0] = state[...]
    left = iota((count, LANES), 1) < WIDTH
    b_t = jnp.transpose(b_low.astype(F32)).astype(BF16)

    for low, width in groups(inner):
        wide = slice(low, low + width)
        values = conv(cv_ref, low, low, width)
        scaled = values * spread(step, low, width)
        entering = state[:, wide]
        y = spread(start, low, width) * nn(c_low, entering.astype(BF16))
        y = y + spread(heads[2:3], low, width) * values
        inside = []
        for part in range(0, width, LANES):
            weights, mine = [], []
            for side in range(2):
                head = (low + part) // WIDTH + side
                decay = jnp.exp(cum[:, head : head + 1] - cum_t[head : head + 1] + hidden_pairs)
                here = left if side == 0 else ~left
                mine.append(jnp.where(here, scaled[:, part : part + LANES], 0.0).astype(BF16))
                weights.append((decay * scores).astype(BF16))
            inside.append(nn(jnp.concatenate(weights, 1), jnp.concatenate(mine, 0)))
        y_ref[:, wide] = y + jnp.concatenate(inside, 1)
        state[:, wide] = spread(through, low, width) * entering + nn(
            b_t, (scaled * spread(end, low, width)).astype(BF16)
        )
    end_ref[...] = state[...]


def scan(cv, cs, halo, step_raw, ids, ids_before, heads, taps):
    tokens, inner = cv.shape
    blocks = tokens // SPAN
    rows = lambda n: pl.BlockSpec((SPAN, n), lambda i: (i, 0))
    whole = lambda a: pl.BlockSpec(a.shape, lambda i: (0, 0), pipeline_mode=ONE)
    return pl.pallas_call(
        scan_kernel,
        grid=(blocks,),
        in_specs=[
            rows(inner), rows(2 * STATE), whole(halo), rows(LANES), whole(ids), whole(ids_before), whole(heads),
            whole(taps),
        ],
        out_specs=[
            rows(inner), rows(2 * STATE), rows(LANES), rows(LANES),
            pl.BlockSpec((1, STATE, inner), lambda i: (i, 0, 0)),
            pl.BlockSpec((STATE, inner), lambda i: (0, 0)),
            pl.BlockSpec((1, 8, LANES), lambda i: (i, 0, 0)), rows(LANES), pl.BlockSpec((1, 8, SPAN), lambda i: (i, 0, 0)),
        ],
        out_shape=[
            jax.ShapeDtypeStruct((tokens, inner), F32),
            jax.ShapeDtypeStruct((tokens, 2 * STATE), BF16),
            jax.ShapeDtypeStruct((tokens, LANES), F32),
            jax.ShapeDtypeStruct((tokens, LANES), F32),
            jax.ShapeDtypeStruct((blocks, STATE, inner), F32),
            jax.ShapeDtypeStruct((STATE, inner), F32),
            jax.ShapeDtypeStruct((blocks, 8, LANES), F32),
            jax.ShapeDtypeStruct((tokens, LANES), F32),
            jax.ShapeDtypeStruct((blocks, 8, SPAN), F32),
        ],
        scratch_shapes=[
            pltpu.VMEM((8, inner + 2 * STATE), F32),
            pltpu.VMEM((STATE, inner), F32),
            pltpu.VMEM((8, LANES), F32),
            pltpu.VMEM((8, LANES), F32),
        ],
        cost_estimate=pl.CostEstimate(
            flops=2 * tokens * inner * (2 * SPAN + 2 * STATE),
            bytes_accessed=tokens * (6 * inner + 4 * STATE + 8 * LANES),
            transcendentals=tokens * inner * 4,
        ),
        name="scan",
    )(cv, cs, halo, step_raw, ids, ids_before, heads, taps)


def gate_kernel(y_ref, reach_ref, bc_ref, state_ref, gate_ref, gg_ref, gain_ref, low_ref, sums_ref):
    inner = y_ref.shape[1]
    c_low = bc_ref[:, LANES:]
    reach = reach_ref[...]
    squares = jnp.zeros((CHUNK, LANES), F32)
    dots = jnp.zeros((CHUNK, LANES), F32)
    for pair in range(inner // LANES):
        wide = slice(pair * LANES, (pair + 1) * LANES)
        ssm = y_ref[:, wide] + pair_of(reach, pair) * nn(c_low, state_ref[:, wide].astype(BF16))
        gate = gate_ref[:, wide]
        gated = ssm * gate * sigmoid(gate)
        weighted = gated * gain_ref[:, wide]
        low_ref[:, wide] = weighted.astype(BF16)
        squares = squares + gated * gated
        dots = dots + gg_ref[:, wide].astype(F32) * weighted
    square = jnp.sum(squares, 1, keepdims=True)
    dot = jnp.sum(dots, 1, keepdims=True)
    sums_ref[...] = jnp.transpose(jnp.where(iota((CHUNK, LANES), 1) == 0, square, dot))[:8]


def gate_sums(y, reach, bc, state_in, gate_raw, gg, gain):
    tokens, inner = y.shape
    rows = lambda n: pl.BlockSpec((CHUNK, n), lambda i: (i, 0))
    whole = lambda a: pl.BlockSpec(a.shape, lambda i: (0, 0), pipeline_mode=ONE)
    return pl.pallas_call(
        gate_kernel,
        grid=(tokens // CHUNK,),
        in_specs=[
            rows(inner), rows(LANES), rows(2 * STATE), whole(state_in), rows(inner), rows(inner), whole(gain),
        ],
        out_specs=[rows(inner), pl.BlockSpec((8, CHUNK), lambda i: (0, i))],
        out_shape=[
            jax.ShapeDtypeStruct((tokens, inner), BF16),
            jax.ShapeDtypeStruct((8, tokens), F32),
        ],
        cost_estimate=pl.CostEstimate(
            flops=2 * tokens * inner * STATE, bytes_accessed=tokens * inner * 12, transcendentals=tokens * inner
        ),
        name="gate",
    )(y, reach, bc, state_in, gate_raw, gg, gain)


def ungate_kernel(count, y_ref, gate_ref, gg_ref, gain_ref, reach_ref, bc_ref, in_ref, *refs):
    sums_refs, (gs_ref, ggr_ref, low_ref, scale_ref, gain_sum_ref, state_ref, gain_acc, state_acc) = (
        refs[:count], refs[count:]
    )
    at = pl.program_id(0)
    inner = y_ref.shape[1]

    @pl.when(at == 0)
    def _():
        gain_acc[...] = jnp.zeros_like(gain_acc)
        state_acc[...] = jnp.zeros_like(state_acc)

    sums = sum(ref[...] for ref in sums_refs)
    sums = jnp.transpose(jnp.concatenate([sums, jnp.zeros((LANES - 8, CHUNK), F32)], 0))
    all_inner = count * inner
    scale = lax.rsqrt(column(sums, 0) / all_inner + EPSILON)
    shift = scale * scale * scale * column(sums, 1) / all_inner
    scale_ref[...] = scale
    reach = reach_ref[...]
    c_low = bc_ref[:, LANES:]
    c_t = jnp.transpose(c_low.astype(F32)).astype(BF16)
    for pair in range(inner // LANES):
        wide = slice(pair * LANES, (pair + 1) * LANES)
        reach_pair = pair_of(reach, pair)
        ssm = y_ref[:, wide] + reach_pair * nn(c_low, in_ref[:, wide].astype(BF16))
        gate, gg = gate_ref[:, wide], gg_ref[:, wide].astype(F32)
        sg = sigmoid(gate)
        act = gate * sg
        gated = ssm * act
        scaled = gated * scale
        low_ref[:, wide] = (scaled * gain_ref[:, wide]).astype(BF16)
        gain_acc[:, wide] += jnp.sum((gg * scaled).reshape(CHUNK // 8, 8, LANES), 0)
        grad_gated = scale * gg * gain_ref[:, wide] - gated * shift
        grad_ssm = grad_gated * act
        gs_ref[:, wide] = grad_ssm
        ggr_ref[:, wide] = (grad_gated * ssm * sg * (1.0 + gate * (1.0 - sg))).astype(BF16)
        state_acc[:, wide] += nn(c_t, (grad_ssm * reach_pair).astype(BF16))
    gain_sum_ref[...] = gain_acc[...]
    state_ref[...] = state_acc[...]


def ungate(y, gate_raw, gg, gain, reach, bc, state_in, sums):
    tokens, inner = y.shape
    rows = lambda n: pl.BlockSpec((CHUNK, n), lambda i: (i, 0))
    whole = lambda a: pl.BlockSpec(a.shape, lambda i: (0, 0), pipeline_mode=ONE)
    fixed = lambda m, n: pl.BlockSpec((m, n), lambda i: (0, 0))
    return pl.pallas_call(
        partial(ungate_kernel, len(sums)),
        grid=(tokens // CHUNK,),
        in_specs=[
            rows(inner), rows(inner), rows(inner), whole(gain), rows(LANES), rows(2 * STATE), whole(state_in),
        ] + [pl.BlockSpec((8, CHUNK), lambda i: (0, i))] * len(sums),
        out_specs=[rows(inner), rows(inner), rows(inner), rows(LANES), fixed(8, inner), fixed(STATE, inner)],
        out_shape=[
            jax.ShapeDtypeStruct((tokens, inner), F32),
            jax.ShapeDtypeStruct((tokens, inner), BF16),
            jax.ShapeDtypeStruct((tokens, inner), BF16),
            jax.ShapeDtypeStruct((tokens, LANES), F32),
            jax.ShapeDtypeStruct((8, inner), F32),
            jax.ShapeDtypeStruct((STATE, inner), F32),
        ],
        scratch_shapes=[pltpu.VMEM((8, inner), F32), pltpu.VMEM((STATE, inner), F32)],
        cost_estimate=pl.CostEstimate(
            flops=2 * tokens * inner * STATE, bytes_accessed=tokens * inner * 16, transcendentals=tokens * inner
        ),
        name="ungate",
    )(y, gate_raw, gg, gain, reach, bc, state_in, *sums)


def unscan_kernel(
    gs_ref, cv_ref, cv_before_ref, cs_ref, cs_before_ref, halo_ref, bc_ref, step_ref, cum_ref, tok_ref, seg_ref,
    heads_ref, taps_ref, enter_ref, kept_ref, state_in_ref, grad_end_ref, gain_sum_ref,
    value_ref, rest_ref, small_ref, head_rows_ref,
    carry, grad, taps_acc, heads_acc, skip_acc,
):
    turn = pl.program_id(0)
    at = pl.num_programs(0) - 1 - turn
    inner = gs_ref.shape[1]
    count = SPAN

    @pl.when(turn == 0)
    def _():
        carry[...] = jnp.zeros_like(carry)
        grad[...] = grad_end_ref[...]
        taps_acc[...] = jnp.zeros_like(taps_acc)
        heads_acc[...] = jnp.zeros_like(heads_acc)
        skip_acc[...] = jnp.zeros_like(skip_acc)

    first = at == 0
    tokens = tok_ref[...]
    heads = heads_ref[...]
    step_in = step_ref[...] + heads[1:2]
    step = softplus(step_in)
    log_decay = heads[0:1] * step
    cum = cum_ref[...]
    last = cum[count - 1 : count]
    start = jnp.exp(cum) * column(tokens, 7)
    end = jnp.exp(last - cum) * column(tokens, 8)
    through = start[count - 1 : count]
    cum_t = jnp.transpose(cum)
    visible = [column(tokens, 1 + k, 2 * LANES) for k in range(3)]
    seen = [column(tokens, 4 + k, 2 * LANES) for k in range(3)]
    left = iota((count, LANES), 1) < WIDTH
    b_low, c_low = bc_ref[:, :LANES], bc_ref[:, LANES:]
    scores = nt(c_low, b_low)
    hidden_pairs = mask_of(tokens, seg_ref[0, 0:1])
    c_t = jnp.transpose(c_low.astype(F32)).astype(BF16)
    kept = kept_ref[0]

    def conv(ref, before_ref, low, at_column, width):
        rows = ref[:, low : low + width].astype(F32)
        wide = slice(at_column, at_column + width)
        before = before_ref[8:16, low : low + width].astype(F32)
        before = jnp.where(first, halo_ref[:, wide].astype(F32), before)
        pre, shifted = conv_taps(taps_ref[:, wide], rows, before, [v[:, :width] for v in visible])
        return pre, shifted, sigmoid(pre)

    def unconv(grad_out, pre, sg, shifted, at_column, width):
        wide = slice(at_column, at_column + width)
        gp = grad_out * sg * (1.0 + pre * (1.0 - sg))
        eighths = lambda v: jnp.sum(v.reshape(count // 8, 8, width), 0)
        for k in range(4):
            taps_acc[8 * k : 8 * k + 8, wide] += eighths(gp * shifted[3 - k])
        taps_acc[32:40, wide] += eighths(gp)
        taps = taps_ref[:, wide]
        following = carry[:, wide]
        total = taps[3:4] * gp
        for steps in range(1, 4):
            moved = from_after(gp, following, steps) * seen[steps - 1][:, :width]
            total = total + taps[3 - steps : 4 - steps] * moved
        if at_column < inner:
            value_ref[:, wide] = total.astype(BF16)
        else:
            rest_ref[:, :width], rest_ref[:, width : 2 * width] = halves(total)
        carry[:, wide] = gp[:8]

        @pl.when(first)
        def _():
            back = jnp.zeros((8, width), F32)
            for steps in range(1, 4):
                moved = pltpu.roll(gp[:8] * visible[steps - 1][:8, :width], 8 - steps, 0)
                back = back + jnp.where(iota((8, width), 0) >= 8 - steps, taps[3 - steps : 4 - steps] * moved, 0.0)
            head_rows_ref[:, wide] = back

    grad_b = jnp.zeros((count, STATE), F32)
    grad_c = jnp.zeros((count, STATE), F32)
    grad_scores = jnp.zeros((count, count), F32)
    grad_cum = jnp.zeros((count, LANES), F32)
    grad_step = jnp.zeros((count, LANES), F32)
    at_end = jnp.zeros((8, LANES), F32)
    down = []
    for low, width in groups(inner):
        wide = slice(low, low + width)
        pre, shifted, sg = conv(cv_ref, cv_before_ref, low, low, width)
        values = pre * sg
        step_wide = spread(step, low, width)
        scaled = values * step_wide
        scaled_low = scaled.astype(BF16)
        grad_y = gs_ref[:, wide]
        starts, ends = spread(start, low, width), spread(end, low, width)
        entering = enter_ref[0, :, wide] + spread(kept[0:1], low, width) * state_in_ref[:, wide]
        grad_state = grad[:, wide]
        grad_low = grad_state.astype(BF16)
        state_low, state_rest = halves(entering)
        to_end = ends * nn(b_low, grad_low)
        grad_y_in = grad_y * starts
        moved = scaled * to_end
        grad_cum = grad_cum + head_sums(grad_y_in * nn(c_low, state_low) - moved, low)
        through_wide = spread(through, low, width)
        ending = jnp.sum(moved, 0, keepdims=True) + through_wide * jnp.sum(grad_state * entering, 0, keepdims=True)
        at_end = at_end + head_sums(jnp.broadcast_to(ending, (8, width)), low)
        y_rest = grad_y - grad_y.astype(BF16).astype(F32)
        scaled_rest = (scaled - scaled_low.astype(F32)).astype(BF16)
        inside = []
        for part in range(0, width, LANES):
            here_lanes = slice(part, part + LANES)
            y_part, x_part = grad_y[:, here_lanes], scaled[:, here_lanes]
            y_turned, x_turned = pltpu.roll(y_rest[:, here_lanes], WIDTH, 1), pltpu.roll(x_part, WIDTH, 1)
            low_weights, low_mine = [], []
            for side in range(2):
                head = (low + part) // WIDTH + side
                here = left if side == 0 else ~left
                decay = jnp.exp(cum[:, head : head + 1] - cum_t[head : head + 1] + hidden_pairs)
                mine = jnp.where(here, y_part, 0.0).astype(BF16)
                weights = decay * scores
                grad_weights = nt(
                    jnp.concatenate([jnp.where(here, y_part, y_turned).astype(BF16), mine], 1),
                    jnp.concatenate([jnp.where(here, x_part, x_turned).astype(BF16), scaled_rest[:, here_lanes]], 1),
                )
                grad_scores = grad_scores + grad_weights * decay
                change = grad_weights * weights
                across = jnp.sum(change, 1, keepdims=True)
                down.append(jnp.sum(change, 0, keepdims=True))
                grad_cum = grad_cum + jnp.where(iota((count, LANES), 1) == head, across, 0.0)
                low_weights.append(weights.astype(BF16))
                low_mine.append(mine)
            inside.append(tn(jnp.concatenate(low_weights, 0), jnp.concatenate(low_mine, 0)))
        grad_scaled = to_end + jnp.concatenate(inside, 1)
        grad_low_in, grad_rest_in = halves(grad_y_in)
        grad_c = grad_c + nt(grad_low_in, state_low) + nt(grad_rest_in, state_low) + nt(grad_low_in, state_rest)
        grad_b = grad_b + nt((scaled * ends).astype(BF16), grad_low)
        grad[:, wide] = through_wide * grad_state + nn(c_t, grad_low_in)
        grad_step = grad_step + head_sums(grad_scaled * values, low)
        skip_acc[:, wide] += jnp.sum((grad_y * values).reshape(count // 8, 8, width), 0)
        grad_values = grad_scaled * step_wide + spread(heads[2:3], low, width) * grad_y
        unconv(grad_values, pre, sg, shifted, low, width)
    down.append(jnp.zeros((LANES - len(down), count), F32))
    grad_cum = grad_cum - jnp.transpose(jnp.concatenate(down, 0))
    for part in halves(grad_scores):
        grad_c = grad_c + nn(part, b_low)
        grad_b = grad_b + tn(part, c_low)
    pre, shifted, sg = conv(cs_ref, cs_before_ref, 0, inner, 2 * STATE)
    unconv(jnp.concatenate([grad_b, grad_c], 1), pre, sg, shifted, inner, 2 * STATE)
    upper = jnp.where(iota((count, count), 0) <= iota((count, count), 1), 1.0, 0.0)
    grad_log = exact(upper, grad_cum) + at_end[0:1]
    grad_step = grad_step + heads[0:1] * grad_log
    grad_raw = grad_step * sigmoid(step_in)
    rest_ref[:, 4 * STATE :] = grad_raw.astype(BF16)
    heads_acc[...] += jnp.concatenate(
        [
            jnp.sum(grad_log * log_decay, 0, keepdims=True),
            jnp.sum(grad_raw, 0, keepdims=True),
            jnp.zeros((6, LANES), F32),
        ],
        0,
    )

    @pl.when(first)
    def _():
        down_rows = lambda v: jnp.sum(v, 0, keepdims=True)
        skip = sum(head_sums(skip_acc[:, low : low + width], low) for low, width in groups(inner))
        wide = [down_rows(taps_acc[8 * k : 8 * k + 8]) for k in range(5)]
        wide += [heads_acc[0:1], heads_acc[1:2], down_rows(skip), down_rows(gain_sum_ref[...])]
        full = small_ref.shape[1]
        wide = [jnp.concatenate([v, jnp.zeros((1, full - v.shape[1]), F32)], 1) for v in wide]
        small_ref[...] = jnp.concatenate(wide + [jnp.zeros((16 - len(wide), full), F32)], 0)


def unscan(
    gs, cv, cs, halo, bc, step_raw, cum, tokens_info, seg_rows, heads, taps, enter, kept, state_in, grad_end, gain_sum,
    full,
):
    tokens, inner = gs.shape
    blocks = tokens // SPAN
    total = inner + 2 * STATE
    back = lambda i: blocks - 1 - i
    rows = lambda n: pl.BlockSpec((SPAN, n), lambda i: (back(i), 0))
    before = lambda n: pl.BlockSpec((16, n), lambda i: (jnp.maximum(back(i) * (SPAN // 16) - 1, 0), 0))
    whole = lambda a: pl.BlockSpec(a.shape, lambda i: (0, 0), pipeline_mode=ONE)
    fixed = lambda m, n: pl.BlockSpec((m, n), lambda i: (0, 0))
    return pl.pallas_call(
        unscan_kernel,
        grid=(blocks,),
        in_specs=[
            rows(inner), rows(inner), before(inner), rows(2 * STATE), before(2 * STATE), whole(halo), rows(2 * STATE),
            rows(LANES), rows(LANES), rows(LANES), pl.BlockSpec((1, 8, SPAN), lambda i: (back(i), 0, 0)),
            whole(heads), whole(taps), pl.BlockSpec((1, STATE, inner), lambda i: (back(i), 0, 0)),
            pl.BlockSpec((1, 8, LANES), lambda i: (back(i), 0, 0)), whole(state_in), whole(grad_end), whole(gain_sum),
        ],
        out_specs=[rows(inner), rows(4 * STATE + LANES), fixed(16, full), fixed(8, total)],
        out_shape=[
            jax.ShapeDtypeStruct((tokens, inner), BF16),
            jax.ShapeDtypeStruct((tokens, 4 * STATE + LANES), BF16),
            jax.ShapeDtypeStruct((16, full), F32),
            jax.ShapeDtypeStruct((8, total), F32),
        ],
        scratch_shapes=[
            pltpu.VMEM((8, total), F32),
            pltpu.VMEM((STATE, inner), F32),
            pltpu.VMEM((40, total), F32),
            pltpu.VMEM((8, LANES), F32),
            pltpu.VMEM((8, inner), F32),
        ],
        cost_estimate=pl.CostEstimate(
            flops=2 * tokens * inner * (6 * SPAN + 4 * STATE),
            bytes_accessed=tokens * (12 * inner),
            transcendentals=tokens * inner * 6,
        ),
        name="unscan",
    )(gs, cv, cv, cs, cs, halo, bc, step_raw, cum, tokens_info, seg_rows, heads, taps, enter, kept, state_in, grad_end, gain_sum)


def chain_kernel(
    first, size, part_ref, ggr_ref, gv_ref, gr_ref, wg_ref, wv_ref, wb_ref, ws_ref, out_ref,
    mine, outer, inner, sent_in, sent_out, came_outer, came_inner,
):
    turn = pl.program_id(0)
    items = mine.shape[0]
    place = lax.axis_index("head")
    half = size // 2
    low_side = place < half
    depth = jnp.where(low_side, place, size - 1 - place)
    toward = jnp.where(low_side, place + 1, place - 1)
    away = jnp.where(low_side, place - 1, place + 1)
    middle, edge = depth == half - 1, depth == 0
    away = jnp.where(edge, toward, away)

    def signal(target):
        pl.semaphore_signal(
            pltpu.get_barrier_semaphore(), inc=1, device_id={"head": target}, device_id_type=pl.DeviceIdType.MESH
        )

    def copy(source, target, sent, came, device):
        return pltpu.make_async_remote_copy(
            src_ref=source, dst_ref=target, send_sem=sent, recv_sem=came,
            device_id={"head": device}, device_id_type=pl.DeviceIdType.MESH,
        )

    def across(item):
        return copy(mine.at[item], inner.at[item], sent_in.at[item], came_inner.at[item], toward)

    def inward(item):
        return copy(mine.at[item], outer.at[item], sent_in.at[item], came_outer.at[item], toward)

    def outward(item):
        return copy(inner.at[item], inner.at[item], sent_out.at[item], came_inner.at[item], away)

    @pl.when(turn == 0)
    def _():
        signal(toward)

        @pl.when(jnp.logical_not(edge))
        def _():
            signal(away)
            pl.semaphore_wait(pltpu.get_barrier_semaphore(), 2)

        @pl.when(edge)
        def _():
            pl.semaphore_wait(pltpu.get_barrier_semaphore(), 1)

    @pl.when(turn < first)
    def _():
        mine[turn] = part_ref[...]

    @pl.when((turn >= first) & (turn < items) & ((turn - first) % GROUP == 0))
    def _():
        product = nt(ggr_ref[...], wg_ref[...]) + nt(gv_ref[...], wv_ref[...])
        both, steps = wb_ref.shape[0], ws_ref.shape[0]
        product = product + nn(gr_ref[:, :both], wb_ref[...]) + nn(gr_ref[:, both : 2 * both], wb_ref[...])
        product = product + nn(gr_ref[:, 2 * both : 2 * both + steps], ws_ref[...])
        for k in range(GROUP):
            mine[turn + k] = product[k * ITEM : (k + 1) * ITEM].astype(BF16)

    done = turn - behind(size)

    @pl.when(done >= 0)
    def _():
        across(done).wait_recv()

        @pl.when(middle)
        def _():
            inner[done] = (inner[done].astype(F32) + mine[done].astype(F32)).astype(BF16)

        @pl.when(jnp.logical_not(edge))
        def _():
            outward(done).start()

        out_ref[...] = inner[done]
        across(done).wait_send()

    item = turn - LAG * depth

    @pl.when((item >= 0) & (item < items))
    def _():
        @pl.when(jnp.logical_not(edge))
        def _():
            inward(item).wait_recv()
            mine[item] = (mine[item].astype(F32) + outer[item].astype(F32)).astype(BF16)

        @pl.when(middle)
        def _():
            across(item).start()

        @pl.when(jnp.logical_not(middle))
        def _():
            inward(item).start()

    @pl.when(turn == pl.num_programs(0) - 1)
    def _():
        @pl.when(jnp.logical_not(edge))
        def _():
            def wait(item, none):
                outward(item).wait_send()
                return none

            lax.fori_loop(0, items, wait, 0)


LAG = 8


def behind(size):
    return LAG * (size // 2 - 1) + 3


ITEM = 32
GROUP = 8


def chain_sums(part, ggr, grad_value, grad_rest, w_gate, w_value, w_both_t, w_step_t):
    tokens, inner = ggr.shape
    width, columns = w_gate.shape[0], grad_rest.shape[1]
    first = part.shape[0] // ITEM
    items = first + tokens // ITEM
    size = lax.axis_size("head")
    rows = lambda n, at: pl.BlockSpec((ITEM, n), lambda i: (at(i), 0))
    own = lambda n: pl.BlockSpec(
        (GROUP * ITEM, n), lambda i: (jnp.clip((i - first) // GROUP, 0, tokens // ITEM // GROUP - 1), 0)
    )
    whole = lambda a: pl.BlockSpec(a.shape, lambda i: (0, 0), pipeline_mode=ONE)
    slots = lambda: pltpu.VMEM((items, ITEM, width), BF16)
    return pl.pallas_call(
        partial(chain_kernel, first, size),
        grid=(items + behind(size),),
        in_specs=[
            rows(width, lambda i: jnp.minimum(i, first - 1)), own(inner), own(inner), own(columns), whole(w_gate),
            whole(w_value), whole(w_both_t), whole(w_step_t),
        ],
        out_specs=rows(width, lambda i: jnp.maximum(i - behind(size), 0)),
        out_shape=jax.ShapeDtypeStruct((items * ITEM, width), BF16),
        scratch_shapes=[slots(), slots(), slots()] + [pltpu.SemaphoreType.DMA((items,))] * 4,
        compiler_params=pltpu.CompilerParams(collective_id=0, has_side_effects=True),
        cost_estimate=pl.CostEstimate(
            flops=2 * tokens * width * (2 * inner + columns), bytes_accessed=600_000_000, transcendentals=0
        ),
        name="chain",
    )(part, ggr, grad_value, grad_rest, w_gate, w_value, w_both_t, w_step_t)


def finish_kernel(
    early, scale_ref, out_a_ref, out_b_ref, grad_ref, x_ref, cot_ref, gain_ref, a_ref, b_ref, c_ref,
    mixed_ref, grad_out_ref, a_out_ref, b_out_ref, c_out_ref,
):
    at = pl.program_id(0)
    x = x_ref[...].astype(F32)
    scale = scale_ref[:, 0:1]

    @pl.when(at < early)
    def _():
        mixed_ref[...] = (x + scale * out_a_ref[...].astype(F32)).astype(BF16)

    @pl.when(at >= early)
    def _():
        mixed_ref[...] = (x + scale * out_b_ref[...].astype(F32)).astype(BF16)

    width = x.shape[1]
    inverse = lax.rsqrt(jnp.mean(x * x, -1, keepdims=True) + EPSILON)
    weighted = grad_ref[...].astype(F32) * gain_ref[...]
    dot = jnp.sum(weighted * x, -1, keepdims=True)
    grad_out_ref[...] = cot_ref[...].astype(F32) + inverse * weighted - x * (inverse**3 * dot / width)
    a_out_ref[...] = a_ref[...].astype(F32)
    b_out_ref[...] = b_ref[...].astype(F32)
    c_out_ref[...] = c_ref[...].astype(F32)


def finish(scale, out_early, chained, hidden, cotangent, gain, sums):
    tokens, width = hidden.shape
    steps = tokens // SPAN
    early = out_early.shape[0] // SPAN
    late = steps - early
    rows = lambda n, at=lambda i: i: pl.BlockSpec((SPAN, n), lambda i: (at(i), 0))
    parts = [pl.BlockSpec((a.shape[0] // steps, a.shape[1]), lambda i: (i, 0)) for a in sums]
    return pl.pallas_call(
        partial(finish_kernel, early),
        grid=(steps,),
        in_specs=[
            rows(LANES), rows(width, lambda i: jnp.minimum(i, early - 1)), rows(width, lambda i: jnp.maximum(i - early, 0)),
            rows(width, lambda i: i + late), rows(width), rows(width), pl.BlockSpec((1, width), lambda i: (0, 0)),
        ] + parts,
        out_specs=[rows(width), rows(width)] + parts,
        out_shape=[jax.ShapeDtypeStruct((tokens, width), BF16), jax.ShapeDtypeStruct((tokens, width), F32)]
        + [jax.ShapeDtypeStruct(a.shape, F32) for a in sums],
        cost_estimate=pl.CostEstimate(flops=0, bytes_accessed=80_000_000, transcendentals=0),
        name="finish",
    )(scale, out_early, chained, chained, hidden, cotangent, gain, *sums)


def pack_kernel(rest_ref, wb_ref, ws_ref, pg_ref, pv_ref, norm_ref, small_ref, packed_ref):
    both, steps = wb_ref.shape[0], ws_ref.shape[0]
    state = rest_ref[:both] + rest_ref[both : 2 * both]
    step = rest_ref[2 * both : 2 * both + steps]
    products = jnp.sum(state * wb_ref[...].astype(F32), 0, keepdims=True) + pg_ref[...][None] + pv_ref[...][None]
    products = products + jnp.sum(step * ws_ref[...].astype(F32), 0, keepdims=True)
    packed_ref[:both] = state
    packed_ref[both : both + 16] = rest_ref[2 * both : 2 * both + 16]
    small = small_ref[...]
    packed_ref[both + 16 :] = jnp.where(iota(small.shape, 0) == 9, products / norm_ref[...], small)


def pack(grad_rest_t, w_both_t, w_step_t, products_gate, products_value, norm, small):
    both, width = w_both_t.shape
    return pl.pallas_call(
        pack_kernel,
        out_shape=jax.ShapeDtypeStruct((both + 32, width), F32),
        name="pack",
    )(grad_rest_t, w_both_t, w_step_t, products_gate, products_value, norm, small)


def unpack_kernel(
    count, packed_ref, *refs
):
    others, refs = refs[: count - 1], refs[count - 1 :]
    state_ref, step_ref, norm_ref, cv_ref, cvb_ref, cs_ref, csb_ref, decay_ref, bias_ref, skip_ref, gain_ref = refs
    state_local, heads, inner = state_ref.shape[0], step_ref.shape[0], cv_ref.shape[1]
    both = state_local * count
    place = lax.axis_index("head")
    own = packed_ref[pl.ds(pl.multiple_of(place * state_local, state_local), state_local), :]
    state_ref[...] = own + sum(ref[:state_local].astype(F32) for ref in others)
    step_ref[...] = packed_ref[both : both + heads]
    small = packed_ref[both + 16 :]
    total = small + sum(ref[state_local:].astype(F32) for ref in others)
    norm_ref[...] = total[9]
    cv_ref[...] = small[:4, :inner]
    cvb_ref[...] = small[4, :inner]
    for q in range(count):
        @pl.when(place == q)
        def _(q=q):
            mine = total[:8, inner + q * state_local : inner + (q + 1) * state_local]
            cs_ref[...] = mine[:4]
            csb_ref[...] = mine[4]
    decay_ref[...] = small[5, :heads]
    bias_ref[...] = small[6, :heads]
    skip_ref[...] = small[7, :heads]
    gain_ref[...] = small[8, :inner]


def unpack(packed, others, inner, heads, state_local):
    width = packed.shape[1]
    shapes = [
        (state_local, width), (heads, width), (width,), (4, inner), (inner,), (4, state_local), (state_local,),
        (heads,), (heads,), (heads,), (inner,),
    ]
    return pl.pallas_call(
        partial(unpack_kernel, len(others) + 1),
        out_shape=[jax.ShapeDtypeStruct(shape, F32) for shape in shapes],
        name="unpack",
    )(packed, *others)


def passed_along(value, axis, steps):
    count = lax.axis_size(axis)
    first, last = (max(0, -steps), min(count, count - steps))
    return lax.ppermute(value, axis, [(source, source + steps) for source in range(first, last)])


def from_all(value, axis):
    count = lax.axis_size(axis)
    moved = lambda steps: lax.ppermute(value, axis, [(s, (s + steps) % count) for s in range(count)])
    return [value] + [moved(steps) for steps in range(1, count)]


def row_major(value):
    return with_layout_constraint(value, Layout(major_to_minor=(0, 1)))


def on_device(
    hidden, segment_ids, norm_gain, w_gate, w_value, w_state, w_step, conv_value, conv_value_bias, conv_state,
    conv_state_bias, decay_log, step_bias, skip_gain, gate_gain, w_out, cotangent,
):
    tokens, width = hidden.shape
    inner, heads_local, state_local = w_value.shape[1], w_step.shape[1], w_state.shape[1]
    count, place = lax.axis_size("head"), lax.axis_index("head")

    ids = segment_ids.reshape(tokens // SPAN, SPAN)
    packed, taps_value, heads, norm, gain = prepare(
        w_state.T, conv_state, conv_state_bias, conv_value, conv_value_bias, decay_log, step_bias, skip_gain,
        norm_gain, gate_gain,
    )
    parts = from_all(packed, "head")
    ids_before = passed_along(ids, "seq", 1)
    w_step_t = jnp.pad(w_step.T, ((0, 16 - heads_local), (0, 0)))

    normed, gate_raw, cv, step_raw = project(hidden, norm, w_gate, w_value, w_step_t)
    w_both_t, taps = assemble(taps_value, parts)
    cs = nt(normed, w_both_t).astype(BF16)
    tail = jnp.concatenate([cv[tokens - 8 :], cs[tokens - 8 :]], 1)
    halo = passed_along(tail, "seq", 1)
    gg = nt(cotangent, w_out).astype(BF16)
    y, bc, cum, reach, enter, local_end, kept, tokens_info, seg_rows = scan(
        cv, cs, halo, step_raw, ids, ids_before, heads, taps
    )
    state_in = passed_along(local_end, "seq", 1)
    low, sums = gate_sums(y, reach, bc, state_in, gate_raw, gg, gain)
    sums = from_all(sums, "head")
    early = EARLY * ITEM
    out_early = lax.psum(nn(low[:early], w_out).astype(BF16), "head")
    out_late = nn(low[early:], w_out).astype(BF16)

    gs, grad_gate_raw, gate_low, scale, gain_sum, grad_state_in = ungate(
        y, gate_raw, gg, gain, reach, bc, state_in, sums
    )
    grad_end = passed_along(grad_state_in, "seq", -1)
    grad_w_out = row_major(tn(gate_low, cotangent))
    grad_value, grad_rest, small, head_rows = unscan(
        gs, cv, cs, halo, bc, step_raw, cum, tokens_info, seg_rows, heads, taps, enter, kept, state_in, grad_end,
        gain_sum, width,
    )
    from_next = passed_along(head_rows, "seq", -1)
    grad_w_gate = row_major(tn(normed, grad_gate_raw))

    def with_next(a, low, high):
        tail = (a[tokens - 8 :, : high - low].astype(F32) + from_next[:, low:high]).astype(BF16)
        return lax.dynamic_update_slice(a, tail, (tokens - 8, 0))

    grad_value = with_next(grad_value, 0, inner)
    grad_rest = with_next(grad_rest, inner, inner + 2 * STATE)
    grad_w_value = row_major(tn(normed, grad_value))
    grad_rest_t = row_major(tn(grad_rest, normed))
    chained = chain_sums(out_late, grad_gate_raw, grad_value, grad_rest, w_gate, w_value, w_both_t, w_step_t)

    packed = pack(
        grad_rest_t, w_both_t, w_step_t, jnp.sum(w_gate.astype(F32) * grad_w_gate, 1),
        jnp.sum(w_value.astype(F32) * grad_w_value, 1), norm, small,
    )
    weights = lax.psum(tuple(a.astype(BF16) for a in (grad_w_gate, grad_w_value, grad_w_out)), "seq")
    packed = lax.psum(packed, "seq")

    def part(steps):
        rows = lax.dynamic_slice_in_dim(packed, lax.rem(place + steps, count) * state_local, state_local, 0)
        return jnp.concatenate([rows, packed[2 * STATE + 16 :]], 0).astype(BF16)

    others = [
        lax.ppermute(part(steps), "head", [(s, (s + steps) % count) for s in range(count)])
        for steps in range(1, count)
    ]
    mixed, grad_hidden, *weights = finish(scale, out_early, chained, hidden, cotangent, norm, weights)
    state_t, step_t, *rest = unpack(packed, others, inner, heads_local, state_local)
    return (mixed, grad_hidden, rest[0], weights[0], weights[1], state_t.T, step_t.T, *rest[1:], weights[2])


def solution(mesh):
    columns, split = P(None, "head"), P("head")
    rows = P("seq", None)

    return jax.shard_map(
        on_device,
        mesh=mesh,
        in_specs=(
            rows, P("seq"), P(), columns, columns, columns, columns, columns, split, columns, split, split, split,
            split, split, P("head", None), rows,
        ),
        out_specs=(
            rows, rows, P(), columns, columns, columns, columns, columns, split, columns, split, split, split, split,
            split, P("head", None),
        ),
        check_vma=False,
    )
```

```python
from functools import partial

import jax
import jax.numpy as jnp
from jax import lax
from jax.experimental import pallas as pl
from jax.experimental.layout import Layout, with_layout_constraint
from jax.experimental.pallas import tpu as pltpu
from jax.sharding import PartitionSpec as P


EPSILON = 1e-05
VERY_NEGATIVE = -1e30
CHUNK = 256
SPAN = 128
STATE = 128
WIDTH = 64
LANES = 128
F32 = jnp.float32
BF16 = jnp.bfloat16
ONE = pl.Buffered(1)
EARLY = 36


def nn(a, b):
    return lax.dot_general(a, b, (((1,), (0,)), ((), ())), preferred_element_type=F32)


def nt(a, b):
    return lax.dot_general(a, b, (((1,), (1,)), ((), ())), preferred_element_type=F32)


def tn(a, b):
    return lax.dot_general(a, b, (((0,), (0,)), ((), ())), preferred_element_type=F32)


def exact(a, b):
    return lax.dot_general(
        a, b, (((1,), (0,)), ((), ())), preferred_element_type=F32, precision=lax.Precision.HIGHEST
    )


def iota(shape, axis):
    return lax.broadcasted_iota(jnp.int32, shape, axis)


def pair_of(columns, pair):
    rows = columns.shape[0]
    first = jnp.broadcast_to(columns[:, 2 * pair : 2 * pair + 1], (rows, LANES))
    second = jnp.broadcast_to(columns[:, 2 * pair + 1 : 2 * pair + 2], (rows, LANES))
    return jnp.where(iota((rows, LANES), 1) < WIDTH, first, second)


def spread(columns, low, width):
    parts = [pair_of(columns, (low + at) // LANES) for at in range(0, width, LANES)]
    return jnp.concatenate(parts, 1) if len(parts) > 1 else parts[0]


def head_sums(values, sums):
    high, rest = halves(values)
    return nn(high, sums) + nn(rest, sums)


def groups(inner):
    return [(low, min(2 * LANES, inner - low)) for low in range(0, inner, 2 * LANES)]


def from_before(rows, previous, steps):
    turned = pltpu.roll(rows, steps, 0)
    head = pltpu.roll(previous, steps, 0)
    top = jnp.where(iota(head.shape, 0) < steps, head, turned[:8])
    return jnp.concatenate([top, turned[8:]], 0)


def from_after(rows, following, steps):
    count = rows.shape[0]
    turned = pltpu.roll(rows, count - steps, 0)
    tail = pltpu.roll(following, 8 - steps, 0)
    bottom = jnp.where(iota(tail.shape, 0) >= 8 - steps, tail, turned[count - 8 :])
    return jnp.concatenate([turned[: count - 8], bottom], 0)


def softplus(v):
    return jnp.maximum(v, 0.0) + jnp.log1p(jnp.exp(-jnp.abs(v)))


def sigmoid(v):
    return 0.5 + 0.5 * jnp.tanh(0.5 * v)


def halves(value):
    high = value.astype(BF16)
    return high, (value - high.astype(F32)).astype(BF16)


def column(tokens, index, width=LANES):
    return jnp.broadcast_to(tokens[:, index : index + 1], (tokens.shape[0], width))


def conv_taps(taps, rows, previous, visible):
    pre = taps[4:5] + taps[3:4] * rows
    shifted = [rows]
    for steps in range(1, 4):
        moved = from_before(rows, previous, steps) * visible[steps - 1]
        shifted.append(moved)
        pre = pre + taps[3 - steps : 4 - steps] * moved
    return pre, shifted


def mask_of(tokens, seg_row):
    same = tokens[:, 0:1] == seg_row
    count = tokens.shape[0]
    causal = iota((count, count), 0) >= iota((count, count), 1)
    return jnp.where(same & causal, 0.0, VERY_NEGATIVE)


def prepare_kernel(
    ws_ref, cs_ref, csb_ref, cv_ref, cvb_ref, decay_ref, bias_ref, skip_ref, norm_ref, gain_ref, wstep_ref,
    packed_ref, taps_ref, heads_ref, norm_out_ref, gain_out_ref, wstep_out_ref, picks_ref, sums_ref,
):
    width = ws_ref.shape[1]
    packed_ref[:, :width] = ws_ref[...]
    taps = jnp.concatenate([cs_ref[...], csb_ref[...][None], jnp.zeros((3, cs_ref.shape[1]), F32)], 0)
    taps = jnp.transpose(jnp.pad(taps, ((0, LANES - 8), (0, LANES - taps.shape[1]))))[: taps.shape[1]]
    for k in range(3):
        high = taps.astype(BF16)
        packed_ref[:, width + LANES * k : width + LANES * (k + 1)] = high
        taps = taps - high.astype(F32)
    packed_ref[:, width + 3 * LANES :] = jnp.zeros((taps.shape[0], LANES), BF16)
    inner = cv_ref.shape[1]
    taps_ref[...] = jnp.concatenate([cv_ref[...], cvb_ref[...][None], jnp.zeros((3, inner), F32)], 0)
    rows = [-jnp.exp(decay_ref[...])[None], bias_ref[...][None], skip_ref[...][None]]
    count = decay_ref.shape[0]
    heads_ref[...] = jnp.pad(
        jnp.concatenate(rows + [jnp.zeros((5, count), F32)], 0), ((0, 0), (0, LANES - count))
    )
    norm_out_ref[...] = norm_ref[...][None]
    gain_out_ref[...] = gain_ref[...][None]
    wstep_out_ref[...] = jnp.concatenate([wstep_ref[...].astype(F32), jnp.zeros((16 - count, width), F32)], 0).astype(BF16)
    shape = picks_ref.shape
    picks_ref[...] = jnp.where(iota(shape, 0) % LANES == iota(shape, 1) // WIDTH, 1.0, 0.0).astype(BF16)
    shape = sums_ref.shape
    sums_ref[...] = jnp.where(iota(shape, 0) // WIDTH == iota(shape, 1), 1.0, 0.0).astype(BF16)


def prepare(w_state_t, conv_state, conv_state_bias, conv_value, conv_value_bias, decay, bias, skip, norm, gain, w_step_t
):
    state_local, width = w_state_t.shape
    inner = conv_value.shape[1]
    return pl.pallas_call(
        prepare_kernel,
        out_shape=[
            jax.ShapeDtypeStruct((state_local, width + 4 * LANES), BF16),
            jax.ShapeDtypeStruct((8, inner), F32),
            jax.ShapeDtypeStruct((8, LANES), F32),
            jax.ShapeDtypeStruct((1, width), F32),
            jax.ShapeDtypeStruct((1, inner), F32),
            jax.ShapeDtypeStruct((16, width), BF16),
            jax.ShapeDtypeStruct((2 * LANES, inner), BF16),
            jax.ShapeDtypeStruct((inner, LANES), BF16),
        ],
        name="prepare",
    )(w_state_t, conv_state, conv_state_bias, conv_value, conv_value_bias, decay, bias, skip, norm, gain, w_step_t)


def project_kernel(x_ref, gain_ref, wg_ref, wv_ref, ws_ref, normed_ref, gate_ref, conv_ref, step_ref):
    x = x_ref[...].astype(F32)
    inverse = lax.rsqrt(jnp.mean(x * x, -1, keepdims=True) + EPSILON)
    normed = (x * inverse * gain_ref[...]).astype(BF16)
    normed_ref[...] = normed
    gate_ref[...] = nn(normed, wg_ref[...]).astype(BF16)
    conv_ref[...] = nn(normed, wv_ref[...]).astype(BF16)
    step = nt(normed, ws_ref[...])
    step_ref[...] = jnp.concatenate([step, jnp.zeros((CHUNK, LANES - step.shape[1]), F32)], 1)


def project(hidden, gain, w_gate, w_value, w_step_t):
    tokens, width = hidden.shape
    inner = w_gate.shape[1]
    rows = lambda n: pl.BlockSpec((CHUNK, n), lambda i: (i, 0))
    whole = lambda a: pl.BlockSpec(a.shape, lambda i: (0, 0), pipeline_mode=ONE)
    return pl.pallas_call(
        project_kernel,
        grid=(tokens // CHUNK,),
        in_specs=[rows(width), whole(gain), whole(w_gate), whole(w_value), whole(w_step_t)],
        out_specs=[rows(width), rows(inner), rows(inner), rows(LANES)],
        out_shape=[
            jax.ShapeDtypeStruct((tokens, width), BF16),
            jax.ShapeDtypeStruct((tokens, inner), BF16),
            jax.ShapeDtypeStruct((tokens, inner), BF16),
            jax.ShapeDtypeStruct((tokens, LANES), F32),
        ],
        cost_estimate=pl.CostEstimate(
            flops=2 * tokens * width * (2 * inner + LANES),
            bytes_accessed=tokens * (4 * width + 6 * inner) + 4 * width * inner,
            transcendentals=0,
        ),
        name="project",
    )(hidden, gain, w_gate, w_value, w_step_t)


def scan_kernel(
    cv_ref, normed_ref, halo_ref, step_ref, ids_ref, heads_ref, taps_value_ref, gathered_ref, picks_ref,
    y_ref, bc_ref, cum_ref, reach_ref, enter_ref, end_ref, kept_ref, tok_ref, seg_ref, cs_ref, taps_ref, rim_ref,
    carry, state, offset, reached, before,
):
    at = pl.program_id(0)
    inner, width = cv_ref.shape[1], normed_ref.shape[1]
    count = SPAN

    @pl.when(at == 0)
    def _():
        columns = sum(gathered_ref[:, width + LANES * k : width + LANES * (k + 1)].astype(F32) for k in range(3))
        taps_ref[:, :inner] = taps_value_ref[...]
        taps_ref[:, inner:] = jnp.transpose(columns)[:8]
        halo = halo_ref[...].astype(F32)
        rim_rows = halo[:, inner + LANES :].astype(BF16)
        rim_state = nt(jnp.concatenate([rim_rows, rim_rows], 0), gathered_ref[:, :width])[:8].astype(BF16)
        rim = jnp.concatenate([halo[:, :inner], rim_state.astype(F32)], 1)
        carry[...] = rim
        rim_ref[...] = rim
        turned = jnp.concatenate([halo[:, inner : inner + LANES], jnp.zeros((LANES - 8, LANES), F32)], 0)
        turned = pltpu.roll(jnp.transpose(turned)[:8], LANES - 8, 1)
        before[...] = jnp.where(lax.axis_index("seq") == 0, -1.0, turned)
        state[...] = jnp.zeros_like(state)
        offset[...] = jnp.zeros_like(offset)
        reached[...] = jnp.ones_like(reached)

    blocks = ids_ref.shape[0]
    own_row = lambda index: ids_ref[pl.ds(index, 1), :].astype(F32)
    previous = before[0:1]
    here = own_row(at)
    earlier = jnp.where(at == 0, previous, own_row(jnp.maximum(at - 1, 0)))
    later = jnp.where(at == blocks - 1, -2.0, own_row(jnp.minimum(at + 1, blocks - 1)))
    lane = iota((1, LANES), 1)
    seg = here
    flags = [here == here]
    for steps in range(1, 4):
        moved = jnp.where(lane < steps, pltpu.roll(earlier, steps, 1), pltpu.roll(here, steps, 1))
        flags.append(moved == here)
    for steps in range(1, 4):
        end = lane >= LANES - steps
        moved = jnp.where(end, pltpu.roll(later, LANES - steps, 1), pltpu.roll(here, LANES - steps, 1))
        flags.append(moved == here)
    first_id = own_row(0)[:, :1]
    flags.append(here == earlier[:, LANES - 1 :])
    flags.append(here == here[:, LANES - 1 :])
    flags.append((here == first_id) & (previous[:, LANES - 1 :] == first_id))
    rows = [seg] + [jnp.where(flag, 1.0, 0.0) for flag in flags[1:]]
    tokens = jnp.transpose(jnp.concatenate(rows + [jnp.zeros((LANES - len(rows), LANES), F32)], 0))
    tok_ref[...] = tokens
    seg_ref[0] = jnp.broadcast_to(seg, (8, LANES))
    heads = heads_ref[...]
    step = softplus(step_ref[...] + heads[1:2])
    log_decay = heads[0:1] * step
    lower = jnp.where(iota((count, count), 0) >= iota((count, count), 1), 1.0, 0.0)
    cum = exact(lower, log_decay)
    cum_ref[...] = cum
    kept_ref[0] = reached[...]
    reach = jnp.exp(cum + offset[0:1]) * column(tokens, 9)
    reach_ref[...] = reach
    last = cum[count - 1 : count]
    offset[...] = offset[...] + last
    reached[...] = jnp.broadcast_to(reach[count - 1 : count], reached.shape)
    start = jnp.exp(cum) * column(tokens, 7)
    end = jnp.exp(last - cum) * column(tokens, 8)
    through = start[count - 1 : count]
    cum_t = jnp.transpose(cum)
    visible = [column(tokens, 1 + k, 2 * LANES) for k in range(3)]

    def conv(rows, at_column):
        width = rows.shape[1]
        wide = slice(at_column, at_column + width)
        pre, _ = conv_taps(taps_ref[:, wide], rows, carry[:, wide], [v[:, :width] for v in visible])
        carry[:, wide] = rows[count - 8 :]
        return pre * sigmoid(pre)

    cs = nt(normed_ref[...], gathered_ref[:, :width]).astype(BF16)
    cs_ref[...] = cs
    both = conv(cs.astype(F32), inner).astype(BF16)
    bc_ref[...] = both
    b_low, c_low = both[:, :LANES], both[:, LANES:]
    scores = nt(c_low, b_low)
    hidden_pairs = mask_of(tokens, seg)
    enter_ref[0] = state[...]
    left = iota((count, LANES), 1) < WIDTH
    b_t = jnp.transpose(b_low.astype(F32)).astype(BF16)
    factors = jnp.concatenate(halves(jnp.concatenate([step, start, end], 0)), 1)

    for low, width in groups(inner):
        wide = slice(low, low + width)
        values = conv(cv_ref[:, wide].astype(F32), low)
        steps_wide, starts, ends = jnp.split(nn(factors, picks_ref[:, wide]), 3)
        scaled = values * steps_wide
        entering = state[:, wide]
        y = starts * nn(c_low, entering.astype(BF16))
        y = y + spread(heads[2:3], low, width) * values
        inside = []
        for part in range(0, width, LANES):
            weights, mine = [], []
            for side in range(2):
                head = (low + part) // WIDTH + side
                decay = jnp.exp(cum[:, head : head + 1] - cum_t[head : head + 1] + hidden_pairs)
                here = left if side == 0 else ~left
                mine.append(jnp.where(here, scaled[:, part : part + LANES], 0.0).astype(BF16))
                weights.append((decay * scores).astype(BF16))
            inside.append(nn(jnp.concatenate(weights, 1), jnp.concatenate(mine, 0)))
        y_ref[:, wide] = (y + jnp.concatenate(inside, 1)).astype(BF16)
        state[:, wide] = spread(through, low, width) * entering + nn(
            b_t, (scaled * ends).astype(BF16)
        )
    end_ref[...] = state[...]


def scan(cv, normed, halo, step_raw, ids, heads, taps_value, gathered, picks):
    tokens, inner = cv.shape
    blocks, total = tokens // SPAN, inner + 2 * STATE
    fixed = lambda n: pl.BlockSpec((8, n), lambda i: (0, 0))
    rows = lambda n: pl.BlockSpec((SPAN, n), lambda i: (i, 0))
    whole = lambda a: pl.BlockSpec(a.shape, lambda i: (0, 0), pipeline_mode=ONE)
    return pl.pallas_call(
        scan_kernel,
        grid=(blocks,),
        in_specs=[
            rows(inner), rows(normed.shape[1]), whole(halo), rows(LANES), whole(ids), whole(heads), whole(taps_value),
            whole(gathered), whole(picks),
        ],
        out_specs=[
            rows(inner), rows(2 * STATE), rows(LANES), rows(LANES),
            pl.BlockSpec((1, STATE, inner), lambda i: (i, 0, 0)),
            pl.BlockSpec((STATE, inner), lambda i: (0, 0)),
            pl.BlockSpec((1, 8, LANES), lambda i: (i, 0, 0)), rows(LANES), pl.BlockSpec((1, 8, SPAN), lambda i: (i, 0, 0)),
            rows(2 * STATE), fixed(total), fixed(total),
        ],
        out_shape=[
            jax.ShapeDtypeStruct((tokens, inner), BF16),
            jax.ShapeDtypeStruct((tokens, 2 * STATE), BF16),
            jax.ShapeDtypeStruct((tokens, LANES), F32),
            jax.ShapeDtypeStruct((tokens, LANES), F32),
            jax.ShapeDtypeStruct((blocks, STATE, inner), F32),
            jax.ShapeDtypeStruct((STATE, inner), F32),
            jax.ShapeDtypeStruct((blocks, 8, LANES), F32),
            jax.ShapeDtypeStruct((tokens, LANES), F32),
            jax.ShapeDtypeStruct((blocks, 8, SPAN), F32),
            jax.ShapeDtypeStruct((tokens, 2 * STATE), BF16),
            jax.ShapeDtypeStruct((8, total), F32),
            jax.ShapeDtypeStruct((8, total), F32),
        ],
        scratch_shapes=[
            pltpu.VMEM((8, inner + 2 * STATE), F32),
            pltpu.VMEM((STATE, inner), F32),
            pltpu.VMEM((8, LANES), F32),
            pltpu.VMEM((8, LANES), F32),
            pltpu.VMEM((8, LANES), F32),
        ],
        cost_estimate=pl.CostEstimate(
            flops=2 * tokens * inner * (2 * SPAN + 2 * STATE),
            bytes_accessed=tokens * (6 * inner + 4 * STATE + 8 * LANES),
            transcendentals=tokens * inner * 4,
        ),
        name="scan",
    )(cv, normed, halo, step_raw, ids, heads, taps_value, gathered, picks)


def gate_kernel(
    y_ref, reach_ref, bc_ref, state_ref, gate_ref, gg_ref, gain_ref, picks_ref, low_ref, sums_ref
):
    inner = y_ref.shape[1]
    c_low = bc_ref[:, LANES:]
    reach = jnp.concatenate(halves(reach_ref[...]), 1)
    squares = jnp.zeros((CHUNK, LANES), F32)
    dots = jnp.zeros((CHUNK, LANES), F32)
    for pair in range(inner // LANES):
        wide = slice(pair * LANES, (pair + 1) * LANES)
        reach_pair = nn(reach, picks_ref[:, wide])
        ssm = y_ref[:, wide].astype(F32) + reach_pair * nn(c_low, state_ref[:, wide].astype(BF16))
        gate = gate_ref[:, wide].astype(F32)
        gated = ssm * gate * sigmoid(gate)
        weighted = gated * gain_ref[:, wide]
        low_ref[:, wide] = weighted.astype(BF16)
        squares = squares + gated * gated
        dots = dots + gg_ref[:, wide].astype(F32) * weighted
    square = jnp.sum(squares, 1, keepdims=True)
    dot = jnp.sum(dots, 1, keepdims=True)
    sums_ref[...] = jnp.transpose(jnp.where(iota((CHUNK, LANES), 1) == 0, square, dot))[:8]


def gate_sums(y, reach, bc, state_in, gate_raw, gg, gain, picks):
    tokens, inner = y.shape
    rows = lambda n: pl.BlockSpec((CHUNK, n), lambda i: (i, 0))
    whole = lambda a: pl.BlockSpec(a.shape, lambda i: (0, 0), pipeline_mode=ONE)
    return pl.pallas_call(
        gate_kernel,
        grid=(tokens // CHUNK,),
        in_specs=[
            rows(inner), rows(LANES), rows(2 * STATE), whole(state_in), rows(inner), rows(inner), whole(gain),
            whole(picks),
        ],
        out_specs=[rows(inner), pl.BlockSpec((8, CHUNK), lambda i: (0, i))],
        out_shape=[
            jax.ShapeDtypeStruct((tokens, inner), BF16),
            jax.ShapeDtypeStruct((8, tokens), F32),
        ],
        cost_estimate=pl.CostEstimate(
            flops=2 * tokens * inner * STATE, bytes_accessed=tokens * inner * 12, transcendentals=tokens * inner
        ),
        name="gate",
    )(y, reach, bc, state_in, gate_raw, gg, gain, picks)


def ungate_kernel(count, y_ref, gate_ref, gg_ref, gain_ref, reach_ref, bc_ref, in_ref, picks_ref, *refs):
    sums_refs, (gs_ref, ggr_ref, low_ref, scale_ref, gain_sum_ref, state_ref, gain_acc, state_acc) = (
        refs[:count], refs[count:]
    )
    at = pl.program_id(0)
    inner = y_ref.shape[1]

    @pl.when(at == 0)
    def _():
        gain_acc[...] = jnp.zeros_like(gain_acc)
        state_acc[...] = jnp.zeros_like(state_acc)

    sums = sum(ref[...] for ref in sums_refs)
    sums = jnp.transpose(jnp.concatenate([sums, jnp.zeros((LANES - 8, CHUNK), F32)], 0))
    all_inner = count * inner
    scale = lax.rsqrt(column(sums, 0) / all_inner + EPSILON)
    shift = scale * scale * scale * column(sums, 1) / all_inner
    scale_ref[...] = scale
    reach = jnp.concatenate(halves(reach_ref[...]), 1)
    c_low = bc_ref[:, LANES:]
    c_t = jnp.transpose(c_low.astype(F32)).astype(BF16)
    for pair in range(inner // LANES):
        wide = slice(pair * LANES, (pair + 1) * LANES)
        reach_pair = nn(reach, picks_ref[:, wide])
        ssm = y_ref[:, wide].astype(F32) + reach_pair * nn(c_low, in_ref[:, wide].astype(BF16))
        gate, gg = gate_ref[:, wide].astype(F32), gg_ref[:, wide].astype(F32)
        sg = sigmoid(gate)
        act = gate * sg
        gated = ssm * act
        scaled = gated * scale
        low_ref[:, wide] = (scaled * gain_ref[:, wide]).astype(BF16)
        gain_acc[:, wide] += jnp.sum((gg * scaled).reshape(CHUNK // 8, 8, LANES), 0)
        grad_gated = scale * gg * gain_ref[:, wide] - gated * shift
        grad_ssm = grad_gated * act
        gs_ref[:, wide] = grad_ssm
        ggr_ref[:, wide] = (grad_gated * ssm * sg * (1.0 + gate * (1.0 - sg))).astype(BF16)
        state_acc[:, wide] += nn(c_t, (grad_ssm * reach_pair).astype(BF16))
    gain_sum_ref[...] = gain_acc[...]
    state_ref[...] = state_acc[...]


def ungate(y, gate_raw, gg, gain, reach, bc, state_in, picks, sums):
    tokens, inner = y.shape
    rows = lambda n: pl.BlockSpec((CHUNK, n), lambda i: (i, 0))
    whole = lambda a: pl.BlockSpec(a.shape, lambda i: (0, 0), pipeline_mode=ONE)
    fixed = lambda m, n: pl.BlockSpec((m, n), lambda i: (0, 0))
    return pl.pallas_call(
        partial(ungate_kernel, len(sums)),
        grid=(tokens // CHUNK,),
        in_specs=[
            rows(inner), rows(inner), rows(inner), whole(gain), rows(LANES), rows(2 * STATE), whole(state_in),
            whole(picks),
        ] + [pl.BlockSpec((8, CHUNK), lambda i: (0, i))] * len(sums),
        out_specs=[rows(inner), rows(inner), rows(inner), rows(LANES), fixed(8, inner), fixed(STATE, inner)],
        out_shape=[
            jax.ShapeDtypeStruct((tokens, inner), F32),
            jax.ShapeDtypeStruct((tokens, inner), BF16),
            jax.ShapeDtypeStruct((tokens, inner), BF16),
            jax.ShapeDtypeStruct((tokens, LANES), F32),
            jax.ShapeDtypeStruct((8, inner), F32),
            jax.ShapeDtypeStruct((STATE, inner), F32),
        ],
        scratch_shapes=[pltpu.VMEM((8, inner), F32), pltpu.VMEM((STATE, inner), F32)],
        cost_estimate=pl.CostEstimate(
            flops=2 * tokens * inner * STATE, bytes_accessed=tokens * inner * 16, transcendentals=tokens * inner
        ),
        name="ungate",
    )(y, gate_raw, gg, gain, reach, bc, state_in, picks, *sums)


def unscan_kernel(
    gs_ref, cv_ref, cv_before_ref, cs_ref, cs_before_ref, halo_ref, bc_ref, step_ref, cum_ref, tok_ref, seg_ref,
    heads_ref, taps_ref, enter_ref, kept_ref, state_in_ref, grad_end_ref, gain_sum_ref, picks_ref, sums_ref,
    value_ref, rest_ref, small_ref, head_rows_ref,
    carry, grad, taps_acc, heads_acc, skip_acc,
):
    turn = pl.program_id(0)
    at = pl.num_programs(0) - 1 - turn
    inner = gs_ref.shape[1]
    count = SPAN

    @pl.when(turn == 0)
    def _():
        carry[...] = jnp.zeros_like(carry)
        grad[...] = grad_end_ref[...]
        taps_acc[...] = jnp.zeros_like(taps_acc)
        heads_acc[...] = jnp.zeros_like(heads_acc)
        skip_acc[...] = jnp.zeros_like(skip_acc)

    first = at == 0
    tokens = tok_ref[...]
    heads = heads_ref[...]
    step_in = step_ref[...] + heads[1:2]
    step = softplus(step_in)
    log_decay = heads[0:1] * step
    cum = cum_ref[...]
    last = cum[count - 1 : count]
    start = jnp.exp(cum) * column(tokens, 7)
    end = jnp.exp(last - cum) * column(tokens, 8)
    through = start[count - 1 : count]
    cum_t = jnp.transpose(cum)
    visible = [column(tokens, 1 + k, 2 * LANES) for k in range(3)]
    seen = [column(tokens, 4 + k, 2 * LANES) for k in range(3)]
    left = iota((count, LANES), 1) < WIDTH
    b_low, c_low = bc_ref[:, :LANES], bc_ref[:, LANES:]
    scores = nt(c_low, b_low)
    hidden_pairs = mask_of(tokens, seg_ref[0, 0:1])
    c_t = jnp.transpose(c_low.astype(F32)).astype(BF16)
    kept = kept_ref[0]

    def conv(ref, before_ref, low, at_column, width):
        rows = ref[:, low : low + width].astype(F32)
        wide = slice(at_column, at_column + width)
        before = before_ref[8:16, low : low + width].astype(F32)
        before = jnp.where(first, halo_ref[:, wide].astype(F32), before)
        pre, shifted = conv_taps(taps_ref[:, wide], rows, before, [v[:, :width] for v in visible])
        return pre, shifted, sigmoid(pre)

    def unconv(grad_out, pre, sg, shifted, at_column, width):
        wide = slice(at_column, at_column + width)
        gp = grad_out * sg * (1.0 + pre * (1.0 - sg))
        eighths = lambda v: jnp.sum(v.reshape(count // 8, 8, width), 0)
        for k in range(4):
            taps_acc[8 * k : 8 * k + 8, wide] += eighths(gp * shifted[3 - k])
        taps_acc[32:40, wide] += eighths(gp)
        taps = taps_ref[:, wide]
        following = carry[:, wide]
        total = taps[3:4] * gp
        for steps in range(1, 4):
            moved = from_after(gp, following, steps) * seen[steps - 1][:, :width]
            total = total + taps[3 - steps : 4 - steps] * moved
        if at_column < inner:
            value_ref[:, wide] = total.astype(BF16)
        else:
            rest_ref[:, :width], rest_ref[:, width : 2 * width] = halves(total)
        carry[:, wide] = gp[:8]

        @pl.when(first)
        def _():
            back = jnp.zeros((8, width), F32)
            for steps in range(1, 4):
                moved = pltpu.roll(gp[:8] * visible[steps - 1][:8, :width], 8 - steps, 0)
                back = back + jnp.where(iota((8, width), 0) >= 8 - steps, taps[3 - steps : 4 - steps] * moved, 0.0)
            head_rows_ref[:, wide] = back

    grad_b = jnp.zeros((count, STATE), F32)
    grad_c = jnp.zeros((count, STATE), F32)
    grad_scores = jnp.zeros((count, count), F32)
    grad_cum = jnp.zeros((count, LANES), F32)
    grad_step = jnp.zeros((count, LANES), F32)
    at_end = jnp.zeros((8, LANES), F32)
    down = []
    factors = jnp.concatenate(halves(jnp.concatenate([step, start, end], 0)), 1)
    for low, width in groups(inner):
        wide = slice(low, low + width)
        pre, shifted, sg = conv(cv_ref, cv_before_ref, low, low, width)
        values = pre * sg
        step_wide, starts, ends = jnp.split(nn(factors, picks_ref[:, wide]), 3)
        scaled = values * step_wide
        scaled_low = scaled.astype(BF16)
        grad_y = gs_ref[:, wide]
        entering = enter_ref[0, :, wide] + spread(kept[0:1], low, width) * state_in_ref[:, wide]
        grad_state = grad[:, wide]
        grad_low = grad_state.astype(BF16)
        state_low, state_rest = halves(entering)
        to_end = ends * nn(b_low, grad_low)
        grad_y_in = grad_y * starts
        moved = scaled * to_end
        grad_cum = grad_cum + head_sums(grad_y_in * nn(c_low, state_low) - moved, sums_ref[wide])
        through_wide = spread(through, low, width)
        ending = jnp.sum(moved, 0, keepdims=True) + through_wide * jnp.sum(grad_state * entering, 0, keepdims=True)
        at_end = at_end + head_sums(jnp.broadcast_to(ending, (8, width)), sums_ref[wide])
        y_rest = grad_y - grad_y.astype(BF16).astype(F32)
        scaled_rest = (scaled - scaled_low.astype(F32)).astype(BF16)
        inside = []
        for part in range(0, width, LANES):
            here_lanes = slice(part, part + LANES)
            y_part, x_part = grad_y[:, here_lanes], scaled[:, here_lanes]
            y_turned, x_turned = pltpu.roll(y_rest[:, here_lanes], WIDTH, 1), pltpu.roll(x_part, WIDTH, 1)
            low_weights, low_mine = [], []
            for side in range(2):
                head = (low + part) // WIDTH + side
                here = left if side == 0 else ~left
                decay = jnp.exp(cum[:, head : head + 1] - cum_t[head : head + 1] + hidden_pairs)
                mine = jnp.where(here, y_part, 0.0).astype(BF16)
                weights = decay * scores
                grad_weights = nt(
                    jnp.concatenate([jnp.where(here, y_part, y_turned).astype(BF16), mine], 1),
                    jnp.concatenate([jnp.where(here, x_part, x_turned).astype(BF16), scaled_rest[:, here_lanes]], 1),
                )
                grad_scores = grad_scores + grad_weights * decay
                change = grad_weights * weights
                across = jnp.sum(change, 1, keepdims=True)
                down.append(jnp.sum(change, 0, keepdims=True))
                grad_cum = grad_cum + jnp.where(iota((count, LANES), 1) == head, across, 0.0)
                low_weights.append(weights.astype(BF16))
                low_mine.append(mine)
            inside.append(tn(jnp.concatenate(low_weights, 0), jnp.concatenate(low_mine, 0)))
        grad_scaled = to_end + jnp.concatenate(inside, 1)
        grad_low_in, grad_rest_in = halves(grad_y_in)
        grad_c = grad_c + nt(grad_low_in, state_low) + nt(grad_rest_in, state_low) + nt(grad_low_in, state_rest)
        grad_b = grad_b + nt((scaled * ends).astype(BF16), grad_low)
        grad[:, wide] = through_wide * grad_state + nn(c_t, grad_low_in)
        grad_step = grad_step + head_sums(grad_scaled * values, sums_ref[wide])
        skip_acc[:, wide] += jnp.sum((grad_y * values).reshape(count // 8, 8, width), 0)
        grad_values = grad_scaled * step_wide + spread(heads[2:3], low, width) * grad_y
        unconv(grad_values, pre, sg, shifted, low, width)
    down.append(jnp.zeros((LANES - len(down), count), F32))
    grad_cum = grad_cum - jnp.transpose(jnp.concatenate(down, 0))
    for part in halves(grad_scores):
        grad_c = grad_c + nn(part, b_low)
        grad_b = grad_b + tn(part, c_low)
    pre, shifted, sg = conv(cs_ref, cs_before_ref, 0, inner, 2 * STATE)
    unconv(jnp.concatenate([grad_b, grad_c], 1), pre, sg, shifted, inner, 2 * STATE)
    upper = jnp.where(iota((count, count), 0) <= iota((count, count), 1), 1.0, 0.0)
    grad_log = exact(upper, grad_cum) + at_end[0:1]
    grad_step = grad_step + heads[0:1] * grad_log
    grad_raw = grad_step * sigmoid(step_in)
    rest_ref[:, 4 * STATE :] = grad_raw.astype(BF16)
    heads_acc[...] += jnp.concatenate(
        [
            jnp.sum(grad_log * log_decay, 0, keepdims=True),
            jnp.sum(grad_raw, 0, keepdims=True),
            jnp.zeros((6, LANES), F32),
        ],
        0,
    )

    @pl.when(first)
    def _():
        down_rows = lambda v: jnp.sum(v, 0, keepdims=True)
        skip = sum(head_sums(skip_acc[:, low : low + width], sums_ref[low : low + width]) for low, width in groups(inner))
        wide = [down_rows(taps_acc[8 * k : 8 * k + 8]) for k in range(5)]
        wide += [heads_acc[0:1], heads_acc[1:2], down_rows(skip), down_rows(gain_sum_ref[...])]
        full = small_ref.shape[1]
        wide = [jnp.concatenate([v, jnp.zeros((1, full - v.shape[1]), F32)], 1) for v in wide]
        small_ref[...] = jnp.concatenate(wide + [jnp.zeros((16 - len(wide), full), F32)], 0)


def unscan(
    gs, cv, cs, halo, bc, step_raw, cum, tokens_info, seg_rows, heads, taps, enter, kept, state_in, grad_end, gain_sum,
    picks, sums, full,
):
    tokens, inner = gs.shape
    blocks = tokens // SPAN
    total = inner + 2 * STATE
    back = lambda i: blocks - 1 - i
    rows = lambda n: pl.BlockSpec((SPAN, n), lambda i: (back(i), 0))
    before = lambda n: pl.BlockSpec((16, n), lambda i: (jnp.maximum(back(i) * (SPAN // 16) - 1, 0), 0))
    whole = lambda a: pl.BlockSpec(a.shape, lambda i: (0, 0), pipeline_mode=ONE)
    fixed = lambda m, n: pl.BlockSpec((m, n), lambda i: (0, 0))
    return pl.pallas_call(
        unscan_kernel,
        grid=(blocks,),
        in_specs=[
            rows(inner), rows(inner), before(inner), rows(2 * STATE), before(2 * STATE), whole(halo), rows(2 * STATE),
            rows(LANES), rows(LANES), rows(LANES), pl.BlockSpec((1, 8, SPAN), lambda i: (back(i), 0, 0)),
            whole(heads), whole(taps), pl.BlockSpec((1, STATE, inner), lambda i: (back(i), 0, 0)),
            pl.BlockSpec((1, 8, LANES), lambda i: (back(i), 0, 0)), whole(state_in), whole(grad_end), whole(gain_sum),
            whole(picks), whole(sums),
        ],
        out_specs=[rows(inner), rows(4 * STATE + LANES), fixed(16, full), fixed(8, total)],
        out_shape=[
            jax.ShapeDtypeStruct((tokens, inner), BF16),
            jax.ShapeDtypeStruct((tokens, 4 * STATE + LANES), BF16),
            jax.ShapeDtypeStruct((16, full), F32),
            jax.ShapeDtypeStruct((8, total), F32),
        ],
        scratch_shapes=[
            pltpu.VMEM((8, total), F32),
            pltpu.VMEM((STATE, inner), F32),
            pltpu.VMEM((40, total), F32),
            pltpu.VMEM((8, LANES), F32),
            pltpu.VMEM((8, inner), F32),
        ],
        cost_estimate=pl.CostEstimate(
            flops=2 * tokens * inner * (6 * SPAN + 4 * STATE),
            bytes_accessed=tokens * (12 * inner),
            transcendentals=tokens * inner * 6,
        ),
        name="unscan",
    )(gs, cv, cv, cs, cs, halo, bc, step_raw, cum, tokens_info, seg_rows, heads, taps, enter, kept, state_in, grad_end, gain_sum, picks, sums)


def chain_kernel(
    first, size, part_ref, ggr_ref, gv_ref, gr_ref, wg_ref, wv_ref, wb_ref, ws_ref, out_ref,
    mine, outer, inner, sent_in, sent_out, came_outer, came_inner,
):
    turn = pl.program_id(0)
    items = mine.shape[0]
    place = lax.axis_index("head")
    half = size // 2
    low_side = place < half
    depth = jnp.where(low_side, place, size - 1 - place)
    toward = jnp.where(low_side, place + 1, place - 1)
    away = jnp.where(low_side, place - 1, place + 1)
    middle, edge = depth == half - 1, depth == 0
    away = jnp.where(edge, toward, away)

    def signal(target):
        pl.semaphore_signal(
            pltpu.get_barrier_semaphore(), inc=1, device_id={"head": target}, device_id_type=pl.DeviceIdType.MESH
        )

    def copy(source, target, sent, came, device):
        return pltpu.make_async_remote_copy(
            src_ref=source, dst_ref=target, send_sem=sent, recv_sem=came,
            device_id={"head": device}, device_id_type=pl.DeviceIdType.MESH,
        )

    def across(item):
        return copy(mine.at[item], inner.at[item], sent_in.at[item], came_inner.at[item], toward)

    def inward(item):
        return copy(mine.at[item], outer.at[item], sent_in.at[item], came_outer.at[item], toward)

    def outward(item):
        return copy(inner.at[item], inner.at[item], sent_out.at[item], came_inner.at[item], away)

    @pl.when(turn == 0)
    def _():
        signal(toward)

        @pl.when(jnp.logical_not(edge))
        def _():
            signal(away)
            pl.semaphore_wait(pltpu.get_barrier_semaphore(), 2)

        @pl.when(edge)
        def _():
            pl.semaphore_wait(pltpu.get_barrier_semaphore(), 1)

    @pl.when(turn < first)
    def _():
        mine[turn] = part_ref[...]

    @pl.when((turn >= first) & (turn < items) & ((turn - first) % GROUP == 0))
    def _():
        product = nt(ggr_ref[...], wg_ref[...]) + nt(gv_ref[...], wv_ref[...])
        both, steps = wb_ref.shape[0], ws_ref.shape[0]
        product = product + nn(gr_ref[:, :both], wb_ref[...]) + nn(gr_ref[:, both : 2 * both], wb_ref[...])
        product = product + nn(gr_ref[:, 2 * both : 2 * both + steps], ws_ref[...])
        for k in range(GROUP):
            mine[turn + k] = product[k * ITEM : (k + 1) * ITEM].astype(BF16)

    done = turn - behind(size)

    @pl.when(done >= 0)
    def _():
        across(done).wait_recv()

        @pl.when(middle)
        def _():
            inner[done] = (inner[done].astype(F32) + mine[done].astype(F32)).astype(BF16)

        @pl.when(jnp.logical_not(edge))
        def _():
            outward(done).start()

        out_ref[...] = inner[done]
        across(done).wait_send()

    item = turn - LAG * depth

    @pl.when((item >= 0) & (item < items))
    def _():
        @pl.when(jnp.logical_not(edge))
        def _():
            inward(item).wait_recv()
            mine[item] = (mine[item].astype(F32) + outer[item].astype(F32)).astype(BF16)

        @pl.when(middle)
        def _():
            across(item).start()

        @pl.when(jnp.logical_not(middle))
        def _():
            inward(item).start()

    @pl.when(turn == pl.num_programs(0) - 1)
    def _():
        @pl.when(jnp.logical_not(edge))
        def _():
            def wait(item, none):
                outward(item).wait_send()
                return none

            lax.fori_loop(0, items, wait, 0)


LAG = 8


def behind(size):
    return LAG * (size // 2 - 1) + 3


ITEM = 32
GROUP = 8


def chain_sums(part, ggr, grad_value, grad_rest, w_gate, w_value, w_both_t, w_step_t):
    tokens, inner = ggr.shape
    width, columns = w_gate.shape[0], grad_rest.shape[1]
    first = part.shape[0] // ITEM
    items = first + tokens // ITEM
    size = lax.axis_size("head")
    rows = lambda n, at: pl.BlockSpec((ITEM, n), lambda i: (at(i), 0))
    own = lambda n: pl.BlockSpec(
        (GROUP * ITEM, n), lambda i: (jnp.clip((i - first) // GROUP, 0, tokens // ITEM // GROUP - 1), 0)
    )
    whole = lambda a: pl.BlockSpec(a.shape, lambda i: (0, 0), pipeline_mode=ONE)
    slots = lambda: pltpu.VMEM((items, ITEM, width), BF16)
    return pl.pallas_call(
        partial(chain_kernel, first, size),
        grid=(items + behind(size),),
        in_specs=[
            rows(width, lambda i: jnp.minimum(i, first - 1)), own(inner), own(inner), own(columns), whole(w_gate),
            whole(w_value), pl.BlockSpec((2 * STATE, width), lambda i: (0, 0), pipeline_mode=ONE), whole(w_step_t),
        ],
        out_specs=rows(width, lambda i: jnp.maximum(i - behind(size), 0)),
        out_shape=jax.ShapeDtypeStruct((items * ITEM, width), BF16),
        scratch_shapes=[slots(), slots(), slots()] + [pltpu.SemaphoreType.DMA((items,))] * 4,
        compiler_params=pltpu.CompilerParams(collective_id=0, has_side_effects=True),
        cost_estimate=pl.CostEstimate(
            flops=2 * tokens * width * (2 * inner + columns), bytes_accessed=600_000_000, transcendentals=0
        ),
        name="chain",
    )(part, ggr, grad_value, grad_rest, w_gate, w_value, w_both_t, w_step_t)


def finish_kernel(
    early, scale_ref, out_a_ref, out_b_ref, grad_ref, x_ref, cot_ref, gain_ref, a_ref, b_ref, c_ref,
    mixed_ref, grad_out_ref, a_out_ref, b_out_ref, c_out_ref,
):
    at = pl.program_id(0)
    width = x_ref.shape[1]
    count = x_ref.shape[0] // 64

    def part(k, none):
        rows = pl.ds(pl.multiple_of(k * 64, 64), 64)
        x = x_ref[rows, :].astype(F32)
        scale = scale_ref[rows, 0:1]
        total = jnp.where(at < early, out_a_ref[rows, :].astype(F32), out_b_ref[rows, :].astype(F32))
        mixed_ref[rows, :] = (x + scale * total).astype(BF16)
        inverse = lax.rsqrt(jnp.mean(x * x, -1, keepdims=True) + EPSILON)
        weighted = grad_ref[rows, :].astype(F32) * gain_ref[...]
        dot = jnp.sum(weighted * x, -1, keepdims=True)
        grad_out_ref[rows, :] = cot_ref[rows, :].astype(F32) + inverse * weighted - x * (inverse**3 * dot / width)
        return none

    lax.fori_loop(0, count, part, 0)
    for source, target in ((a_ref, a_out_ref), (b_ref, b_out_ref), (c_ref, c_out_ref)):
        target[...] = source[...].astype(F32)


def finish(scale, out_early, chained, hidden, cotangent, gain, sums):
    tokens, width = hidden.shape
    per_step = 128
    steps = tokens // per_step
    early = out_early.shape[0] // per_step
    late = steps - early
    rows = lambda n, at=lambda i: i: pl.BlockSpec((per_step, n), lambda i: (at(i), 0))
    parts = [pl.BlockSpec((a.shape[0] // steps, a.shape[1]), lambda i: (i, 0)) for a in sums]
    return pl.pallas_call(
        partial(finish_kernel, early),
        grid=(steps,),
        in_specs=[
            rows(LANES), rows(width, lambda i: jnp.minimum(i, early - 1)), rows(width, lambda i: jnp.maximum(i - early, 0)),
            rows(width, lambda i: i + late), rows(width), rows(width), pl.BlockSpec((1, width), lambda i: (0, 0)),
        ] + parts,
        out_specs=[rows(width), rows(width)] + parts,
        out_shape=[jax.ShapeDtypeStruct((tokens, width), BF16), jax.ShapeDtypeStruct((tokens, width), F32)]
        + [jax.ShapeDtypeStruct(a.shape, F32) for a in sums],
        cost_estimate=pl.CostEstimate(flops=0, bytes_accessed=80_000_000, transcendentals=0),
        name="finish",
    )(scale, out_early, chained, chained, hidden, cotangent, gain, *sums)


def pack_kernel(rest_ref, wb_ref, ws_ref, pg_ref, pv_ref, norm_ref, small_ref, packed_ref):
    both, steps, width = wb_ref.shape[0], ws_ref.shape[0], ws_ref.shape[1]
    state = rest_ref[:both] + rest_ref[both : 2 * both]
    step = rest_ref[2 * both : 2 * both + steps]
    products = jnp.sum(state * wb_ref[:, :width].astype(F32), 0, keepdims=True) + pg_ref[...][None] + pv_ref[...][None]
    products = products + jnp.sum(step * ws_ref[...].astype(F32), 0, keepdims=True)
    packed_ref[:both] = state
    packed_ref[both : both + 16] = rest_ref[2 * both : 2 * both + 16]
    small = small_ref[...]
    packed_ref[both + 16 :] = jnp.where(iota(small.shape, 0) == 9, products / norm_ref[...], small)


def pack(grad_rest_t, w_both_t, w_step_t, products_gate, products_value, norm, small):
    both, width = w_both_t.shape[0], w_step_t.shape[1]
    return pl.pallas_call(
        pack_kernel,
        out_shape=jax.ShapeDtypeStruct((both + 32, width), F32),
        name="pack",
    )(grad_rest_t, w_both_t, w_step_t, products_gate, products_value, norm, small)


def late_kernel(packed_ref, *parts):
    state_local, count = parts[0].shape[0] - 16, len(parts) + 1
    place = lax.axis_index("head")
    small = packed_ref[count * state_local + 16 :].astype(BF16)
    for steps, part in enumerate(parts, 1):
        at = pl.multiple_of(lax.rem(place + steps, count) * state_local, state_local)
        part[:state_local] = packed_ref[pl.ds(at, state_local), :].astype(BF16)
        part[state_local:] = small


def late_parts(packed, state_local, count):
    shape = jax.ShapeDtypeStruct((state_local + 16, packed.shape[1]), BF16)
    return pl.pallas_call(late_kernel, out_shape=[shape] * (count - 1), name="late")(packed)


def unpack_kernel(count, packed_ref, *refs):
    others, refs = refs[: count - 1], refs[count - 1 :]
    state_ref, step_ref, norm_ref, cv_ref, cvb_ref, cs_ref, csb_ref, decay_ref, bias_ref, skip_ref, gain_ref = refs
    state_local, heads, inner = state_ref.shape[0], step_ref.shape[0], cv_ref.shape[1]
    both = state_local * count
    place = lax.axis_index("head")
    own = packed_ref[pl.ds(pl.multiple_of(place * state_local, state_local), state_local), :]
    state_ref[...] = own + sum(ref[:state_local].astype(F32) for ref in others)
    step_ref[...] = packed_ref[both : both + heads]
    small = packed_ref[both + 16 :]
    total = small + sum(ref[state_local:].astype(F32) for ref in others)
    norm_ref[...] = total[9]
    cv_ref[...] = small[:4, :inner]
    cvb_ref[...] = small[4, :inner]
    for q in range(count):
        @pl.when(place == q)
        def _(q=q):
            mine = total[:8, inner + q * state_local : inner + (q + 1) * state_local]
            cs_ref[...] = mine[:4]
            csb_ref[...] = mine[4]
    decay_ref[...] = small[5, :heads]
    bias_ref[...] = small[6, :heads]
    skip_ref[...] = small[7, :heads]
    gain_ref[...] = small[8, :inner]


def unpack(packed, others, inner, heads, state_local):
    width = packed.shape[1]
    shapes = [
        (state_local, width), (heads, width), (width,), (4, inner), (inner,), (4, state_local), (state_local,),
        (heads,), (heads,), (heads,), (inner,),
    ]
    return pl.pallas_call(
        partial(unpack_kernel, len(others) + 1),
        out_shape=[jax.ShapeDtypeStruct(shape, F32) for shape in shapes],
        name="unpack",
    )(packed, *others)


def passed_along(value, axis, steps):
    count = lax.axis_size(axis)
    first, last = (max(0, -steps), min(count, count - steps))
    return lax.ppermute(value, axis, [(source, source + steps) for source in range(first, last)])


def from_all(value, axis):
    count = lax.axis_size(axis)
    moved = lambda steps: lax.ppermute(value, axis, [(s, (s + steps) % count) for s in range(count)])
    return [value] + [moved(steps) for steps in range(1, count)]


def row_major(value):
    return with_layout_constraint(value, Layout(major_to_minor=(0, 1)))


def on_device(
    hidden, segment_ids, norm_gain, w_gate, w_value, w_state, w_step, conv_value, conv_value_bias, conv_state,
    conv_state_bias, decay_log, step_bias, skip_gain, gate_gain, w_out, cotangent,
):
    tokens, width = hidden.shape
    inner, heads_local, state_local = w_value.shape[1], w_step.shape[1], w_state.shape[1]
    count = lax.axis_size("head")

    ids = segment_ids.reshape(tokens // SPAN, SPAN)
    packed, taps_value, heads, norm, gain, w_step_t, picks, sums_of = prepare(
        w_state.T, conv_state, conv_state_bias, conv_value, conv_value_bias, decay_log, step_bias, skip_gain,
        norm_gain, gate_gain, w_step.T,
    )
    gathered = lax.all_gather(packed, "head", axis=0, tiled=True)

    normed, gate_raw, cv, step_raw = project(hidden, norm, w_gate, w_value, w_step_t)
    last_ids = jnp.pad(segment_ids[tokens - 8 :].astype(F32).astype(BF16)[:, None], ((0, 0), (0, LANES - 1)))
    tail = jnp.concatenate([cv[tokens - 8 :], last_ids, normed[tokens - 8 :]], 1)
    halo = passed_along(tail, "seq", 1)
    gg = nt(cotangent, w_out).astype(BF16)
    y, bc, cum, reach, enter, local_end, kept, tokens_info, seg_rows, cs, taps, rim = scan(
        cv, normed, halo, step_raw, ids, heads, taps_value, gathered, picks
    )
    state_in = passed_along(local_end, "seq", 1)
    low, sums = gate_sums(y, reach, bc, state_in, gate_raw, gg, gain, picks)
    sums = from_all(sums, "head")
    early = EARLY * ITEM
    out_early = lax.psum(nn(low[:early], w_out).astype(BF16), "head")
    out_late = nn(low[early:], w_out).astype(BF16)

    gs, grad_gate_raw, gate_low, scale, gain_sum, grad_state_in = ungate(
        y, gate_raw, gg, gain, reach, bc, state_in, picks, sums
    )
    grad_end = passed_along(grad_state_in, "seq", -1)
    grad_w_out = row_major(tn(gate_low, cotangent))
    grad_value, grad_rest, small, head_rows = unscan(
        gs, cv, cs, rim, bc, step_raw, cum, tokens_info, seg_rows, heads, taps, enter, kept, state_in, grad_end,
        gain_sum, picks, sums_of, width,
    )
    from_next = passed_along(head_rows, "seq", -1)
    grad_w_gate = row_major(tn(normed, grad_gate_raw))

    def with_next(a, low, high):
        tail = (a[tokens - 8 :, : high - low].astype(F32) + from_next[:, low:high]).astype(BF16)
        return lax.dynamic_update_slice(a, tail, (tokens - 8, 0))

    grad_value = with_next(grad_value, 0, inner)
    grad_rest = with_next(grad_rest, inner, inner + 2 * STATE)
    grad_w_value = row_major(tn(normed, grad_value))
    grad_rest_t = row_major(tn(grad_rest, normed))
    chained = chain_sums(out_late, grad_gate_raw, grad_value, grad_rest, w_gate, w_value, gathered, w_step_t)

    packed = pack(
        grad_rest_t, gathered, w_step_t, jnp.sum(w_gate.astype(F32) * grad_w_gate, 1),
        jnp.sum(w_value.astype(F32) * grad_w_value, 1), norm, small,
    )
    weights = lax.psum(tuple(a.astype(BF16) for a in (grad_w_gate, grad_w_value, grad_w_out)), "seq")
    packed = lax.psum(packed, "seq")

    others = [
        lax.ppermute(part, "head", [(s, (s + steps) % count) for s in range(count)])
        for steps, part in enumerate(late_parts(packed, state_local, count), 1)
    ]
    mixed, grad_hidden, *weights = finish(scale, out_early, chained, hidden, cotangent, norm, weights)
    state_t, step_t, *rest = unpack(packed, others, inner, heads_local, state_local)
    return (mixed, grad_hidden, rest[0], weights[0], weights[1], state_t.T, step_t.T, *rest[1:], weights[2])


def solution(mesh):
    columns, split = P(None, "head"), P("head")
    rows = P("seq", None)

    return jax.shard_map(
        on_device,
        mesh=mesh,
        in_specs=(
            rows, P("seq"), P(), columns, columns, columns, columns, columns, split, columns, split, split, split,
            split, split, P("head", None), rows,
        ),
        out_specs=(
            rows, rows, P(), columns, columns, columns, columns, columns, split, columns, split, split, split, split,
            split, P("head", None),
        ),
        check_vma=False,
    )
```

```python
from functools import partial

import jax
import jax.numpy as jnp
from jax import lax
from jax.experimental import pallas as pl
from jax.experimental.layout import Layout, with_layout_constraint
from jax.experimental.pallas import tpu as pltpu
from jax.sharding import PartitionSpec as P


EPSILON = 1e-05
VERY_NEGATIVE = -1e30
CHUNK = 256
SPAN = 128
STATE = 128
WIDTH = 64
LANES = 128
F32 = jnp.float32
BF16 = jnp.bfloat16
ONE = pl.Buffered(1)
EARLY = 36


def nn(a, b):
    return lax.dot_general(a, b, (((1,), (0,)), ((), ())), preferred_element_type=F32)


def nt(a, b):
    return lax.dot_general(a, b, (((1,), (1,)), ((), ())), preferred_element_type=F32)


def tn(a, b):
    return lax.dot_general(a, b, (((0,), (0,)), ((), ())), preferred_element_type=F32)


def exact(a, b):
    return lax.dot_general(
        a, b, (((1,), (0,)), ((), ())), preferred_element_type=F32, precision=lax.Precision.HIGHEST
    )


def iota(shape, axis):
    return lax.broadcasted_iota(jnp.int32, shape, axis)


def pair_of(columns, pair):
    rows = columns.shape[0]
    first = jnp.broadcast_to(columns[:, 2 * pair : 2 * pair + 1], (rows, LANES))
    second = jnp.broadcast_to(columns[:, 2 * pair + 1 : 2 * pair + 2], (rows, LANES))
    return jnp.where(iota((rows, LANES), 1) < WIDTH, first, second)


def spread(columns, low, width):
    parts = [pair_of(columns, (low + at) // LANES) for at in range(0, width, LANES)]
    return jnp.concatenate(parts, 1) if len(parts) > 1 else parts[0]


def head_sums(values, sums):
    high, rest = halves(values)
    return nn(high, sums) + nn(rest, sums)


def groups(inner):
    return [(low, min(2 * LANES, inner - low)) for low in range(0, inner, 2 * LANES)]


def from_before(rows, previous, steps):
    turned = pltpu.roll(rows, steps, 0)
    head = pltpu.roll(previous, steps, 0)
    top = jnp.where(iota(head.shape, 0) < steps, head, turned[:8])
    return jnp.concatenate([top, turned[8:]], 0)


def from_after(rows, following, steps):
    count = rows.shape[0]
    turned = pltpu.roll(rows, count - steps, 0)
    tail = pltpu.roll(following, 8 - steps, 0)
    bottom = jnp.where(iota(tail.shape, 0) >= 8 - steps, tail, turned[count - 8 :])
    return jnp.concatenate([turned[: count - 8], bottom], 0)


def softplus(v):
    return jnp.maximum(v, 0.0) + jnp.log1p(jnp.exp(-jnp.abs(v)))


def sigmoid(v):
    return 0.5 + 0.5 * jnp.tanh(0.5 * v)


def halves(value):
    high = value.astype(BF16)
    return high, (value - high.astype(F32)).astype(BF16)


def column(tokens, index, width=LANES):
    return jnp.broadcast_to(tokens[:, index : index + 1], (tokens.shape[0], width))


def conv_taps(taps, rows, previous, visible):
    pre = taps[4:5] + taps[3:4] * rows
    shifted = [rows]
    for steps in range(1, 4):
        moved = from_before(rows, previous, steps) * visible[steps - 1]
        shifted.append(moved)
        pre = pre + taps[3 - steps : 4 - steps] * moved
    return pre, shifted


def mask_of(tokens, seg_row):
    same = tokens[:, 0:1] == seg_row
    count = tokens.shape[0]
    causal = iota((count, count), 0) >= iota((count, count), 1)
    return jnp.where(same & causal, 0.0, VERY_NEGATIVE)


def prepare_kernel(
    ws_ref, cs_ref, csb_ref, cv_ref, cvb_ref, decay_ref, bias_ref, skip_ref, norm_ref, gain_ref, wstep_ref,
    packed_ref, taps_ref, heads_ref, norm_out_ref, gain_out_ref, wstep_out_ref, picks_ref, sums_ref,
):
    width = ws_ref.shape[1]
    packed_ref[:, :width] = ws_ref[...]
    taps = jnp.concatenate([cs_ref[...], csb_ref[...][None], jnp.zeros((3, cs_ref.shape[1]), F32)], 0)
    taps = jnp.transpose(jnp.pad(taps, ((0, LANES - 8), (0, LANES - taps.shape[1]))))[: taps.shape[1]]
    for k in range(3):
        high = taps.astype(BF16)
        packed_ref[:, width + LANES * k : width + LANES * (k + 1)] = high
        taps = taps - high.astype(F32)
    packed_ref[:, width + 3 * LANES :] = jnp.zeros((taps.shape[0], LANES), BF16)
    inner = cv_ref.shape[1]
    taps_ref[...] = jnp.concatenate([cv_ref[...], cvb_ref[...][None], jnp.zeros((3, inner), F32)], 0)
    rows = [-jnp.exp(decay_ref[...])[None], bias_ref[...][None], skip_ref[...][None]]
    count = decay_ref.shape[0]
    heads_ref[...] = jnp.pad(
        jnp.concatenate(rows + [jnp.zeros((5, count), F32)], 0), ((0, 0), (0, LANES - count))
    )
    norm_out_ref[...] = norm_ref[...][None]
    gain_out_ref[...] = gain_ref[...][None]
    wstep_out_ref[...] = jnp.concatenate([wstep_ref[...].astype(F32), jnp.zeros((16 - count, width), F32)], 0).astype(BF16)
    shape = picks_ref.shape
    picks_ref[...] = jnp.where(iota(shape, 0) % LANES == iota(shape, 1) // WIDTH, 1.0, 0.0).astype(BF16)
    shape = sums_ref.shape
    sums_ref[...] = jnp.where(iota(shape, 0) // WIDTH == iota(shape, 1), 1.0, 0.0).astype(BF16)


def prepare(w_state_t, conv_state, conv_state_bias, conv_value, conv_value_bias, decay, bias, skip, norm, gain, w_step_t
):
    state_local, width = w_state_t.shape
    inner = conv_value.shape[1]
    return pl.pallas_call(
        prepare_kernel,
        out_shape=[
            jax.ShapeDtypeStruct((state_local, width + 4 * LANES), BF16),
            jax.ShapeDtypeStruct((8, inner), F32),
            jax.ShapeDtypeStruct((8, LANES), F32),
            jax.ShapeDtypeStruct((1, width), F32),
            jax.ShapeDtypeStruct((1, inner), F32),
            jax.ShapeDtypeStruct((16, width), BF16),
            jax.ShapeDtypeStruct((2 * LANES, inner), BF16),
            jax.ShapeDtypeStruct((inner, LANES), BF16),
        ],
        name="prepare",
    )(w_state_t, conv_state, conv_state_bias, conv_value, conv_value_bias, decay, bias, skip, norm, gain, w_step_t)


def project_kernel(x_ref, gain_ref, wg_ref, wv_ref, ws_ref, normed_ref, gate_ref, conv_ref, step_ref):
    x = x_ref[...].astype(F32)
    inverse = lax.rsqrt(jnp.mean(x * x, -1, keepdims=True) + EPSILON)
    normed = (x * inverse * gain_ref[...]).astype(BF16)
    normed_ref[...] = normed
    gate_ref[...] = nn(normed, wg_ref[...]).astype(BF16)
    conv_ref[...] = nn(normed, wv_ref[...]).astype(BF16)
    step = nt(normed, ws_ref[...])
    step_ref[...] = jnp.concatenate([step, jnp.zeros((CHUNK, LANES - step.shape[1]), F32)], 1)


def project(hidden, gain, w_gate, w_value, w_step_t):
    tokens, width = hidden.shape
    inner = w_gate.shape[1]
    rows = lambda n: pl.BlockSpec((CHUNK, n), lambda i: (i, 0))
    whole = lambda a: pl.BlockSpec(a.shape, lambda i: (0, 0), pipeline_mode=ONE)
    return pl.pallas_call(
        project_kernel,
        grid=(tokens // CHUNK,),
        in_specs=[rows(width), whole(gain), whole(w_gate), whole(w_value), whole(w_step_t)],
        out_specs=[rows(width), rows(inner), rows(inner), rows(LANES)],
        out_shape=[
            jax.ShapeDtypeStruct((tokens, width), BF16),
            jax.ShapeDtypeStruct((tokens, inner), BF16),
            jax.ShapeDtypeStruct((tokens, inner), BF16),
            jax.ShapeDtypeStruct((tokens, LANES), F32),
        ],
        cost_estimate=pl.CostEstimate(
            flops=2 * tokens * width * (2 * inner + LANES),
            bytes_accessed=tokens * (4 * width + 6 * inner) + 4 * width * inner,
            transcendentals=0,
        ),
        name="project",
    )(hidden, gain, w_gate, w_value, w_step_t)


def scan_kernel(
    cv_ref, normed_ref, halo_ref, step_ref, ids_ref, heads_ref, taps_value_ref, gathered_ref, picks_ref,
    y_ref, bc_ref, cum_ref, reach_ref, enter_ref, end_ref, kept_ref, tok_ref, seg_ref, cs_ref, taps_ref, rim_ref,
    carry, state, offset, reached, before,
):
    at = pl.program_id(0)
    inner, width = cv_ref.shape[1], normed_ref.shape[1]
    count = SPAN

    @pl.when(at == 0)
    def _():
        columns = sum(gathered_ref[:, width + LANES * k : width + LANES * (k + 1)].astype(F32) for k in range(3))
        taps_ref[:, :inner] = taps_value_ref[...]
        taps_ref[:, inner:] = jnp.transpose(columns)[:8]
        halo = halo_ref[...].astype(F32)
        rim_rows = halo[:, inner + LANES :].astype(BF16)
        rim_state = nt(jnp.concatenate([rim_rows, rim_rows], 0), gathered_ref[:, :width])[:8].astype(BF16)
        rim = jnp.concatenate([halo[:, :inner], rim_state.astype(F32)], 1)
        carry[...] = rim
        rim_ref[...] = rim
        turned = jnp.concatenate([halo[:, inner : inner + LANES], jnp.zeros((LANES - 8, LANES), F32)], 0)
        turned = pltpu.roll(jnp.transpose(turned)[:8], LANES - 8, 1)
        before[...] = jnp.where(lax.axis_index("seq") == 0, -1.0, turned)
        state[...] = jnp.zeros_like(state)
        offset[...] = jnp.zeros_like(offset)
        reached[...] = jnp.ones_like(reached)

    blocks = ids_ref.shape[0]
    own_row = lambda index: ids_ref[pl.ds(index, 1), :].astype(F32)
    previous = before[0:1]
    here = own_row(at)
    earlier = jnp.where(at == 0, previous, own_row(jnp.maximum(at - 1, 0)))
    later = jnp.where(at == blocks - 1, -2.0, own_row(jnp.minimum(at + 1, blocks - 1)))
    lane = iota((1, LANES), 1)
    seg = here
    flags = [here == here]
    for steps in range(1, 4):
        moved = jnp.where(lane < steps, pltpu.roll(earlier, steps, 1), pltpu.roll(here, steps, 1))
        flags.append(moved == here)
    for steps in range(1, 4):
        end = lane >= LANES - steps
        moved = jnp.where(end, pltpu.roll(later, LANES - steps, 1), pltpu.roll(here, LANES - steps, 1))
        flags.append(moved == here)
    first_id = own_row(0)[:, :1]
    flags.append(here == earlier[:, LANES - 1 :])
    flags.append(here == here[:, LANES - 1 :])
    flags.append((here == first_id) & (previous[:, LANES - 1 :] == first_id))
    rows = [seg] + [jnp.where(flag, 1.0, 0.0) for flag in flags[1:]]
    tokens = jnp.transpose(jnp.concatenate(rows + [jnp.zeros((LANES - len(rows), LANES), F32)], 0))
    tok_ref[...] = tokens
    seg_ref[0] = jnp.broadcast_to(seg, (8, LANES))
    heads = heads_ref[...]
    step = softplus(step_ref[...] + heads[1:2])
    log_decay = heads[0:1] * step
    lower = jnp.where(iota((count, count), 0) >= iota((count, count), 1), 1.0, 0.0)
    cum = exact(lower, log_decay)
    cum_ref[...] = cum
    kept_ref[0] = reached[...]
    reach = jnp.exp(cum + offset[0:1]) * column(tokens, 9)
    reach_ref[...] = reach
    last = cum[count - 1 : count]
    offset[...] = offset[...] + last
    reached[...] = jnp.broadcast_to(reach[count - 1 : count], reached.shape)
    start = jnp.exp(cum) * column(tokens, 7)
    end = jnp.exp(last - cum) * column(tokens, 8)
    through = start[count - 1 : count]
    cum_t = jnp.transpose(cum)
    visible = [column(tokens, 1 + k, 2 * LANES) for k in range(3)]

    def conv(rows, at_column):
        width = rows.shape[1]
        wide = slice(at_column, at_column + width)
        pre, _ = conv_taps(taps_ref[:, wide], rows, carry[:, wide], [v[:, :width] for v in visible])
        carry[:, wide] = rows[count - 8 :]
        return pre * sigmoid(pre)

    cs = nt(normed_ref[...], gathered_ref[:, :width]).astype(BF16)
    cs_ref[...] = cs
    both = conv(cs.astype(F32), inner).astype(BF16)
    bc_ref[...] = both
    b_low, c_low = both[:, :LANES], both[:, LANES:]
    scores = nt(c_low, b_low)
    hidden_pairs = mask_of(tokens, seg)
    enter_ref[0] = state[...]
    left = iota((count, LANES), 1) < WIDTH
    b_t = jnp.transpose(b_low.astype(F32)).astype(BF16)
    factors = jnp.concatenate(halves(jnp.concatenate([step, start, end], 0)), 1)

    for low, width in groups(inner):
        wide = slice(low, low + width)
        values = conv(cv_ref[:, wide].astype(F32), low)
        steps_wide, starts, ends = jnp.split(nn(factors, picks_ref[:, wide]), 3)
        scaled = values * steps_wide
        entering = state[:, wide]
        y = starts * nn(c_low, entering.astype(BF16))
        y = y + spread(heads[2:3], low, width) * values
        inside = []
        for part in range(0, width, LANES):
            weights, mine = [], []
            for side in range(2):
                head = (low + part) // WIDTH + side
                decay = jnp.exp(cum[:, head : head + 1] - cum_t[head : head + 1] + hidden_pairs)
                here = left if side == 0 else ~left
                mine.append(jnp.where(here, scaled[:, part : part + LANES], 0.0).astype(BF16))
                weights.append((decay * scores).astype(BF16))
            inside.append(nn(jnp.concatenate(weights, 1), jnp.concatenate(mine, 0)))
        y_ref[:, wide] = (y + jnp.concatenate(inside, 1)).astype(BF16)
        state[:, wide] = spread(through, low, width) * entering + nn(
            b_t, (scaled * ends).astype(BF16)
        )
    end_ref[...] = state[...]


def scan(cv, normed, halo, step_raw, ids, heads, taps_value, gathered, picks):
    tokens, inner = cv.shape
    blocks, total = tokens // SPAN, inner + 2 * STATE
    fixed = lambda n: pl.BlockSpec((8, n), lambda i: (0, 0))
    rows = lambda n: pl.BlockSpec((SPAN, n), lambda i: (i, 0))
    whole = lambda a: pl.BlockSpec(a.shape, lambda i: (0, 0), pipeline_mode=ONE)
    return pl.pallas_call(
        scan_kernel,
        grid=(blocks,),
        in_specs=[
            rows(inner), rows(normed.shape[1]), whole(halo), rows(LANES), whole(ids), whole(heads), whole(taps_value),
            whole(gathered), whole(picks),
        ],
        out_specs=[
            rows(inner), rows(2 * STATE), rows(LANES), rows(LANES),
            pl.BlockSpec((1, STATE, inner), lambda i: (i, 0, 0)),
            pl.BlockSpec((STATE, inner), lambda i: (0, 0)),
            pl.BlockSpec((1, 8, LANES), lambda i: (i, 0, 0)), rows(LANES), pl.BlockSpec((1, 8, SPAN), lambda i: (i, 0, 0)),
            rows(2 * STATE), fixed(total), fixed(total),
        ],
        out_shape=[
            jax.ShapeDtypeStruct((tokens, inner), BF16),
            jax.ShapeDtypeStruct((tokens, 2 * STATE), BF16),
            jax.ShapeDtypeStruct((tokens, LANES), F32),
            jax.ShapeDtypeStruct((tokens, LANES), F32),
            jax.ShapeDtypeStruct((blocks, STATE, inner), F32),
            jax.ShapeDtypeStruct((STATE, inner), F32),
            jax.ShapeDtypeStruct((blocks, 8, LANES), F32),
            jax.ShapeDtypeStruct((tokens, LANES), F32),
            jax.ShapeDtypeStruct((blocks, 8, SPAN), F32),
            jax.ShapeDtypeStruct((tokens, 2 * STATE), BF16),
            jax.ShapeDtypeStruct((8, total), F32),
            jax.ShapeDtypeStruct((8, total), F32),
        ],
        scratch_shapes=[
            pltpu.VMEM((8, inner + 2 * STATE), F32),
            pltpu.VMEM((STATE, inner), F32),
            pltpu.VMEM((8, LANES), F32),
            pltpu.VMEM((8, LANES), F32),
            pltpu.VMEM((8, LANES), F32),
        ],
        cost_estimate=pl.CostEstimate(
            flops=2 * tokens * inner * (2 * SPAN + 2 * STATE),
            bytes_accessed=tokens * (6 * inner + 4 * STATE + 8 * LANES),
            transcendentals=tokens * inner * 4,
        ),
        name="scan",
    )(cv, normed, halo, step_raw, ids, heads, taps_value, gathered, picks)


def gate_kernel(
    y_ref, reach_ref, bc_ref, state_ref, gate_ref, gg_ref, gain_ref, picks_ref, low_ref, sums_ref
):
    inner = y_ref.shape[1]
    c_low = bc_ref[:, LANES:]
    reach = jnp.concatenate(halves(reach_ref[...]), 1)
    squares = jnp.zeros((CHUNK, LANES), F32)
    dots = jnp.zeros((CHUNK, LANES), F32)
    for pair in range(inner // LANES):
        wide = slice(pair * LANES, (pair + 1) * LANES)
        reach_pair = nn(reach, picks_ref[:, wide])
        ssm = y_ref[:, wide].astype(F32) + reach_pair * nn(c_low, state_ref[:, wide].astype(BF16))
        gate = gate_ref[:, wide].astype(F32)
        gated = ssm * gate * sigmoid(gate)
        weighted = gated * gain_ref[:, wide]
        low_ref[:, wide] = weighted.astype(BF16)
        squares = squares + gated * gated
        dots = dots + gg_ref[:, wide].astype(F32) * weighted
    square = jnp.sum(squares, 1, keepdims=True)
    dot = jnp.sum(dots, 1, keepdims=True)
    sums_ref[...] = jnp.transpose(jnp.where(iota((CHUNK, LANES), 1) == 0, square, dot))[:8]


def gate_sums(y, reach, bc, state_in, gate_raw, gg, gain, picks):
    tokens, inner = y.shape
    rows = lambda n: pl.BlockSpec((CHUNK, n), lambda i: (i, 0))
    whole = lambda a: pl.BlockSpec(a.shape, lambda i: (0, 0), pipeline_mode=ONE)
    return pl.pallas_call(
        gate_kernel,
        grid=(tokens // CHUNK,),
        in_specs=[
            rows(inner), rows(LANES), rows(2 * STATE), whole(state_in), rows(inner), rows(inner), whole(gain),
            whole(picks),
        ],
        out_specs=[rows(inner), pl.BlockSpec((8, CHUNK), lambda i: (0, i))],
        out_shape=[
            jax.ShapeDtypeStruct((tokens, inner), BF16),
            jax.ShapeDtypeStruct((8, tokens), F32),
        ],
        cost_estimate=pl.CostEstimate(
            flops=2 * tokens * inner * STATE, bytes_accessed=tokens * inner * 12, transcendentals=tokens * inner
        ),
        name="gate",
    )(y, reach, bc, state_in, gate_raw, gg, gain, picks)


def ungate_kernel(count, y_ref, gate_ref, gg_ref, gain_ref, reach_ref, bc_ref, in_ref, picks_ref, *refs):
    sums_refs, (gs_ref, ggr_ref, low_ref, scale_ref, gain_sum_ref, state_ref, gain_acc, state_acc) = (
        refs[:count], refs[count:]
    )
    at = pl.program_id(0)
    inner = y_ref.shape[1]

    @pl.when(at == 0)
    def _():
        gain_acc[...] = jnp.zeros_like(gain_acc)
        state_acc[...] = jnp.zeros_like(state_acc)

    sums = sum(ref[...] for ref in sums_refs)
    sums = jnp.transpose(jnp.concatenate([sums, jnp.zeros((LANES - 8, CHUNK), F32)], 0))
    all_inner = count * inner
    scale = lax.rsqrt(column(sums, 0) / all_inner + EPSILON)
    shift = scale * scale * scale * column(sums, 1) / all_inner
    scale_ref[...] = scale
    reach = jnp.concatenate(halves(reach_ref[...]), 1)
    c_low = bc_ref[:, LANES:]
    c_t = jnp.transpose(c_low.astype(F32)).astype(BF16)
    for pair in range(inner // LANES):
        wide = slice(pair * LANES, (pair + 1) * LANES)
        reach_pair = nn(reach, picks_ref[:, wide])
        ssm = y_ref[:, wide].astype(F32) + reach_pair * nn(c_low, in_ref[:, wide].astype(BF16))
        gate, gg = gate_ref[:, wide].astype(F32), gg_ref[:, wide].astype(F32)
        sg = sigmoid(gate)
        act = gate * sg
        gated = ssm * act
        scaled = gated * scale
        low_ref[:, wide] = (scaled * gain_ref[:, wide]).astype(BF16)
        gain_acc[:, wide] += jnp.sum((gg * scaled).reshape(CHUNK // 8, 8, LANES), 0)
        grad_gated = scale * gg * gain_ref[:, wide] - gated * shift
        grad_ssm = grad_gated * act
        gs_ref[:, wide] = grad_ssm
        ggr_ref[:, wide] = (grad_gated * ssm * sg * (1.0 + gate * (1.0 - sg))).astype(BF16)
        state_acc[:, wide] += nn(c_t, (grad_ssm * reach_pair).astype(BF16))
    gain_sum_ref[...] = gain_acc[...]
    state_ref[...] = state_acc[...]


def ungate(y, gate_raw, gg, gain, reach, bc, state_in, picks, sums):
    tokens, inner = y.shape
    rows = lambda n: pl.BlockSpec((CHUNK, n), lambda i: (i, 0))
    whole = lambda a: pl.BlockSpec(a.shape, lambda i: (0, 0), pipeline_mode=ONE)
    fixed = lambda m, n: pl.BlockSpec((m, n), lambda i: (0, 0))
    return pl.pallas_call(
        partial(ungate_kernel, len(sums)),
        grid=(tokens // CHUNK,),
        in_specs=[
            rows(inner), rows(inner), rows(inner), whole(gain), rows(LANES), rows(2 * STATE), whole(state_in),
            whole(picks),
        ] + [pl.BlockSpec((8, CHUNK), lambda i: (0, i))] * len(sums),
        out_specs=[rows(inner), rows(inner), rows(inner), rows(LANES), fixed(8, inner), fixed(STATE, inner)],
        out_shape=[
            jax.ShapeDtypeStruct((tokens, inner), F32),
            jax.ShapeDtypeStruct((tokens, inner), BF16),
            jax.ShapeDtypeStruct((tokens, inner), BF16),
            jax.ShapeDtypeStruct((tokens, LANES), F32),
            jax.ShapeDtypeStruct((8, inner), F32),
            jax.ShapeDtypeStruct((STATE, inner), F32),
        ],
        scratch_shapes=[pltpu.VMEM((8, inner), F32), pltpu.VMEM((STATE, inner), F32)],
        cost_estimate=pl.CostEstimate(
            flops=2 * tokens * inner * STATE, bytes_accessed=tokens * inner * 16, transcendentals=tokens * inner
        ),
        name="ungate",
    )(y, gate_raw, gg, gain, reach, bc, state_in, picks, *sums)


def unscan_kernel(
    gs_ref, cv_ref, cv_before_ref, cs_ref, cs_before_ref, halo_ref, bc_ref, step_ref, cum_ref, tok_ref, seg_ref,
    heads_ref, taps_ref, enter_ref, kept_ref, state_in_ref, grad_end_ref, gain_sum_ref, picks_ref, sums_ref,
    value_ref, rest_ref, small_ref, head_rows_ref,
    carry, grad, taps_acc, heads_acc, skip_acc,
):
    turn = pl.program_id(0)
    at = pl.num_programs(0) - 1 - turn
    inner = gs_ref.shape[1]
    count = SPAN

    @pl.when(turn == 0)
    def _():
        carry[...] = jnp.zeros_like(carry)
        grad[...] = grad_end_ref[...]
        taps_acc[...] = jnp.zeros_like(taps_acc)
        heads_acc[...] = jnp.zeros_like(heads_acc)
        skip_acc[...] = jnp.zeros_like(skip_acc)

    first = at == 0
    tokens = tok_ref[...]
    heads = heads_ref[...]
    step_in = step_ref[...] + heads[1:2]
    step = softplus(step_in)
    log_decay = heads[0:1] * step
    cum = cum_ref[...]
    last = cum[count - 1 : count]
    start = jnp.exp(cum) * column(tokens, 7)
    end = jnp.exp(last - cum) * column(tokens, 8)
    through = start[count - 1 : count]
    cum_t = jnp.transpose(cum)
    visible = [column(tokens, 1 + k, 2 * LANES) for k in range(3)]
    seen = [column(tokens, 4 + k, 2 * LANES) for k in range(3)]
    left = iota((count, LANES), 1) < WIDTH
    b_low, c_low = bc_ref[:, :LANES], bc_ref[:, LANES:]
    scores = nt(c_low, b_low)
    hidden_pairs = mask_of(tokens, seg_ref[0, 0:1])
    c_t = jnp.transpose(c_low.astype(F32)).astype(BF16)
    kept = kept_ref[0]

    def conv(ref, before_ref, low, at_column, width):
        rows = ref[:, low : low + width].astype(F32)
        wide = slice(at_column, at_column + width)
        before = before_ref[8:16, low : low + width].astype(F32)
        before = jnp.where(first, halo_ref[:, wide].astype(F32), before)
        pre, shifted = conv_taps(taps_ref[:, wide], rows, before, [v[:, :width] for v in visible])
        return pre, shifted, sigmoid(pre)

    def unconv(grad_out, pre, sg, shifted, at_column, width):
        wide = slice(at_column, at_column + width)
        gp = grad_out * sg * (1.0 + pre * (1.0 - sg))
        eighths = lambda v: jnp.sum(v.reshape(count // 8, 8, width), 0)
        for k in range(4):
            taps_acc[8 * k : 8 * k + 8, wide] += eighths(gp * shifted[3 - k])
        taps_acc[32:40, wide] += eighths(gp)
        taps = taps_ref[:, wide]
        following = carry[:, wide]
        total = taps[3:4] * gp
        for steps in range(1, 4):
            moved = from_after(gp, following, steps) * seen[steps - 1][:, :width]
            total = total + taps[3 - steps : 4 - steps] * moved
        if at_column < inner:
            value_ref[:, wide] = total.astype(BF16)
        else:
            rest_ref[:, :width], rest_ref[:, width : 2 * width] = halves(total)
        carry[:, wide] = gp[:8]

        @pl.when(first)
        def _():
            back = jnp.zeros((8, width), F32)
            for steps in range(1, 4):
                moved = pltpu.roll(gp[:8] * visible[steps - 1][:8, :width], 8 - steps, 0)
                back = back + jnp.where(iota((8, width), 0) >= 8 - steps, taps[3 - steps : 4 - steps] * moved, 0.0)
            head_rows_ref[:, wide] = back

    grad_b = jnp.zeros((count, STATE), F32)
    grad_c = jnp.zeros((count, STATE), F32)
    grad_scores = jnp.zeros((count, count), F32)
    grad_cum = jnp.zeros((count, LANES), F32)
    grad_step = jnp.zeros((count, LANES), F32)
    at_end = jnp.zeros((8, LANES), F32)
    down = []
    factors = jnp.concatenate(halves(jnp.concatenate([step, start, end], 0)), 1)
    for low, width in groups(inner):
        wide = slice(low, low + width)
        pre, shifted, sg = conv(cv_ref, cv_before_ref, low, low, width)
        values = pre * sg
        step_wide, starts, ends = jnp.split(nn(factors, picks_ref[:, wide]), 3)
        scaled = values * step_wide
        scaled_low = scaled.astype(BF16)
        grad_y = gs_ref[:, wide]
        entering = enter_ref[0, :, wide] + spread(kept[0:1], low, width) * state_in_ref[:, wide]
        grad_state = grad[:, wide]
        grad_low = grad_state.astype(BF16)
        state_low, state_rest = halves(entering)
        to_end = ends * nn(b_low, grad_low)
        grad_y_in = grad_y * starts
        moved = scaled * to_end
        grad_cum = grad_cum + head_sums(grad_y_in * nn(c_low, state_low) - moved, sums_ref[wide])
        through_wide = spread(through, low, width)
        ending = jnp.sum(moved, 0, keepdims=True) + through_wide * jnp.sum(grad_state * entering, 0, keepdims=True)
        at_end = at_end + head_sums(jnp.broadcast_to(ending, (8, width)), sums_ref[wide])
        y_rest = grad_y - grad_y.astype(BF16).astype(F32)
        scaled_rest = (scaled - scaled_low.astype(F32)).astype(BF16)
        inside = []
        for part in range(0, width, LANES):
            here_lanes = slice(part, part + LANES)
            y_part, x_part = grad_y[:, here_lanes], scaled[:, here_lanes]
            y_turned, x_turned = pltpu.roll(y_rest[:, here_lanes], WIDTH, 1), pltpu.roll(x_part, WIDTH, 1)
            low_weights, low_mine = [], []
            for side in range(2):
                head = (low + part) // WIDTH + side
                here = left if side == 0 else ~left
                decay = jnp.exp(cum[:, head : head + 1] - cum_t[head : head + 1] + hidden_pairs)
                mine = jnp.where(here, y_part, 0.0).astype(BF16)
                weights = decay * scores
                grad_weights = nt(
                    jnp.concatenate([jnp.where(here, y_part, y_turned).astype(BF16), mine], 1),
                    jnp.concatenate([jnp.where(here, x_part, x_turned).astype(BF16), scaled_rest[:, here_lanes]], 1),
                )
                grad_scores = grad_scores + grad_weights * decay
                change = grad_weights * weights
                across = jnp.sum(change, 1, keepdims=True)
                down.append(jnp.sum(change, 0, keepdims=True))
                grad_cum = grad_cum + jnp.where(iota((count, LANES), 1) == head, across, 0.0)
                low_weights.append(weights.astype(BF16))
                low_mine.append(mine)
            inside.append(tn(jnp.concatenate(low_weights, 0), jnp.concatenate(low_mine, 0)))
        grad_scaled = to_end + jnp.concatenate(inside, 1)
        grad_low_in, grad_rest_in = halves(grad_y_in)
        grad_c = grad_c + nt(grad_low_in, state_low) + nt(grad_rest_in, state_low) + nt(grad_low_in, state_rest)
        grad_b = grad_b + nt((scaled * ends).astype(BF16), grad_low)
        grad[:, wide] = through_wide * grad_state + nn(c_t, grad_low_in)
        grad_step = grad_step + head_sums(grad_scaled * values, sums_ref[wide])
        skip_acc[:, wide] += jnp.sum((grad_y * values).reshape(count // 8, 8, width), 0)
        grad_values = grad_scaled * step_wide + spread(heads[2:3], low, width) * grad_y
        unconv(grad_values, pre, sg, shifted, low, width)
    down.append(jnp.zeros((LANES - len(down), count), F32))
    grad_cum = grad_cum - jnp.transpose(jnp.concatenate(down, 0))
    for part in halves(grad_scores):
        grad_c = grad_c + nn(part, b_low)
        grad_b = grad_b + tn(part, c_low)
    pre, shifted, sg = conv(cs_ref, cs_before_ref, 0, inner, 2 * STATE)
    unconv(jnp.concatenate([grad_b, grad_c], 1), pre, sg, shifted, inner, 2 * STATE)
    upper = jnp.where(iota((count, count), 0) <= iota((count, count), 1), 1.0, 0.0)
    grad_log = exact(upper, grad_cum) + at_end[0:1]
    grad_step = grad_step + heads[0:1] * grad_log
    grad_raw = grad_step * sigmoid(step_in)
    rest_ref[:, 4 * STATE :] = grad_raw.astype(BF16)
    heads_acc[...] += jnp.concatenate(
        [
            jnp.sum(grad_log * log_decay, 0, keepdims=True),
            jnp.sum(grad_raw, 0, keepdims=True),
            jnp.zeros((6, LANES), F32),
        ],
        0,
    )

    @pl.when(first)
    def _():
        down_rows = lambda v: jnp.sum(v, 0, keepdims=True)
        skip = sum(head_sums(skip_acc[:, low : low + width], sums_ref[low : low + width]) for low, width in groups(inner))
        wide = [down_rows(taps_acc[8 * k : 8 * k + 8]) for k in range(5)]
        wide += [heads_acc[0:1], heads_acc[1:2], down_rows(skip), down_rows(gain_sum_ref[...])]
        full = small_ref.shape[1]
        wide = [jnp.concatenate([v, jnp.zeros((1, full - v.shape[1]), F32)], 1) for v in wide]
        small_ref[...] = jnp.concatenate(wide + [jnp.zeros((16 - len(wide), full), F32)], 0)


def unscan(
    gs, cv, cs, halo, bc, step_raw, cum, tokens_info, seg_rows, heads, taps, enter, kept, state_in, grad_end, gain_sum,
    picks, sums, full,
):
    tokens, inner = gs.shape
    blocks = tokens // SPAN
    total = inner + 2 * STATE
    back = lambda i: blocks - 1 - i
    rows = lambda n: pl.BlockSpec((SPAN, n), lambda i: (back(i), 0))
    before = lambda n: pl.BlockSpec((16, n), lambda i: (jnp.maximum(back(i) * (SPAN // 16) - 1, 0), 0))
    whole = lambda a: pl.BlockSpec(a.shape, lambda i: (0, 0), pipeline_mode=ONE)
    fixed = lambda m, n: pl.BlockSpec((m, n), lambda i: (0, 0))
    return pl.pallas_call(
        unscan_kernel,
        grid=(blocks,),
        in_specs=[
            rows(inner), rows(inner), before(inner), rows(2 * STATE), before(2 * STATE), whole(halo), rows(2 * STATE),
            rows(LANES), rows(LANES), rows(LANES), pl.BlockSpec((1, 8, SPAN), lambda i: (back(i), 0, 0)),
            whole(heads), whole(taps), pl.BlockSpec((1, STATE, inner), lambda i: (back(i), 0, 0)),
            pl.BlockSpec((1, 8, LANES), lambda i: (back(i), 0, 0)), whole(state_in), whole(grad_end), whole(gain_sum),
            whole(picks), whole(sums),
        ],
        out_specs=[rows(inner), rows(4 * STATE + LANES), fixed(16, full), fixed(8, total)],
        out_shape=[
            jax.ShapeDtypeStruct((tokens, inner), BF16),
            jax.ShapeDtypeStruct((tokens, 4 * STATE + LANES), BF16),
            jax.ShapeDtypeStruct((16, full), F32),
            jax.ShapeDtypeStruct((8, total), F32),
        ],
        scratch_shapes=[
            pltpu.VMEM((8, total), F32),
            pltpu.VMEM((STATE, inner), F32),
            pltpu.VMEM((40, total), F32),
            pltpu.VMEM((8, LANES), F32),
            pltpu.VMEM((8, inner), F32),
        ],
        cost_estimate=pl.CostEstimate(
            flops=2 * tokens * inner * (6 * SPAN + 4 * STATE),
            bytes_accessed=tokens * (12 * inner),
            transcendentals=tokens * inner * 6,
        ),
        name="unscan",
    )(gs, cv, cv, cs, cs, halo, bc, step_raw, cum, tokens_info, seg_rows, heads, taps, enter, kept, state_in, grad_end, gain_sum, picks, sums)


def chain_kernel(
    first, size, part_ref, ggr_ref, gv_ref, gr_ref, wg_ref, wv_ref, wb_ref, ws_ref, out_ref,
    mine, outer, inner, sent_in, sent_out, came_outer, came_inner,
):
    turn = pl.program_id(0)
    items = mine.shape[0]
    place = lax.axis_index("head")
    half = size // 2
    low_side = place < half
    depth = jnp.where(low_side, place, size - 1 - place)
    toward = jnp.where(low_side, place + 1, place - 1)
    away = jnp.where(low_side, place - 1, place + 1)
    middle, edge = depth == half - 1, depth == 0
    away = jnp.where(edge, toward, away)

    def signal(target):
        pl.semaphore_signal(
            pltpu.get_barrier_semaphore(), inc=1, device_id={"head": target}, device_id_type=pl.DeviceIdType.MESH
        )

    def copy(source, target, sent, came, device):
        return pltpu.make_async_remote_copy(
            src_ref=source, dst_ref=target, send_sem=sent, recv_sem=came,
            device_id={"head": device}, device_id_type=pl.DeviceIdType.MESH,
        )

    def across(item):
        return copy(mine.at[item], inner.at[item], sent_in.at[item], came_inner.at[item], toward)

    def inward(item):
        return copy(mine.at[item], outer.at[item], sent_in.at[item], came_outer.at[item], toward)

    def outward(item):
        return copy(inner.at[item], inner.at[item], sent_out.at[item], came_inner.at[item], away)

    @pl.when(turn == 0)
    def _():
        signal(toward)

        @pl.when(jnp.logical_not(edge))
        def _():
            signal(away)
            pl.semaphore_wait(pltpu.get_barrier_semaphore(), 2)

        @pl.when(edge)
        def _():
            pl.semaphore_wait(pltpu.get_barrier_semaphore(), 1)

    @pl.when(turn < first)
    def _():
        mine[turn] = part_ref[...]

    @pl.when((turn >= first) & (turn < items) & ((turn - first) % GROUP == 0))
    def _():
        product = nt(ggr_ref[...], wg_ref[...]) + nt(gv_ref[...], wv_ref[...])
        both, steps = wb_ref.shape[0], ws_ref.shape[0]
        product = product + nn(gr_ref[:, :both], wb_ref[...]) + nn(gr_ref[:, both : 2 * both], wb_ref[...])
        product = product + nn(gr_ref[:, 2 * both : 2 * both + steps], ws_ref[...])
        for k in range(GROUP):
            mine[turn + k] = product[k * ITEM : (k + 1) * ITEM].astype(BF16)

    done = turn - behind(size)

    @pl.when(done >= 0)
    def _():
        across(done).wait_recv()

        @pl.when(middle)
        def _():
            inner[done] = (inner[done].astype(F32) + mine[done].astype(F32)).astype(BF16)

        @pl.when(jnp.logical_not(edge))
        def _():
            outward(done).start()

        out_ref[...] = inner[done]
        across(done).wait_send()

    item = turn - LAG * depth

    @pl.when((item >= 0) & (item < items))
    def _():
        @pl.when(jnp.logical_not(edge))
        def _():
            inward(item).wait_recv()
            mine[item] = (mine[item].astype(F32) + outer[item].astype(F32)).astype(BF16)

        @pl.when(middle)
        def _():
            across(item).start()

        @pl.when(jnp.logical_not(middle))
        def _():
            inward(item).start()

    @pl.when(turn == pl.num_programs(0) - 1)
    def _():
        @pl.when(jnp.logical_not(edge))
        def _():
            def wait(item, none):
                outward(item).wait_send()
                return none

            lax.fori_loop(0, items, wait, 0)


LAG = 8


def behind(size):
    return LAG * (size // 2 - 1) + 3


ITEM = 32
GROUP = 8


def chain_sums(part, ggr, grad_value, grad_rest, w_gate, w_value, w_both_t, w_step_t):
    tokens, inner = ggr.shape
    width, columns = w_gate.shape[0], grad_rest.shape[1]
    first = part.shape[0] // ITEM
    items = first + tokens // ITEM
    size = lax.axis_size("head")
    rows = lambda n, at: pl.BlockSpec((ITEM, n), lambda i: (at(i), 0))
    own = lambda n: pl.BlockSpec(
        (GROUP * ITEM, n), lambda i: (jnp.clip((i - first) // GROUP, 0, tokens // ITEM // GROUP - 1), 0)
    )
    whole = lambda a: pl.BlockSpec(a.shape, lambda i: (0, 0), pipeline_mode=ONE)
    slots = lambda: pltpu.VMEM((items, ITEM, width), BF16)
    return pl.pallas_call(
        partial(chain_kernel, first, size),
        grid=(items + behind(size),),
        in_specs=[
            rows(width, lambda i: jnp.minimum(i, first - 1)), own(inner), own(inner), own(columns), whole(w_gate),
            whole(w_value), pl.BlockSpec((2 * STATE, width), lambda i: (0, 0), pipeline_mode=ONE), whole(w_step_t),
        ],
        out_specs=rows(width, lambda i: jnp.maximum(i - behind(size), 0)),
        out_shape=jax.ShapeDtypeStruct((items * ITEM, width), BF16),
        scratch_shapes=[slots(), slots(), slots()] + [pltpu.SemaphoreType.DMA((items,))] * 4,
        compiler_params=pltpu.CompilerParams(collective_id=0, has_side_effects=True),
        cost_estimate=pl.CostEstimate(
            flops=2 * tokens * width * (2 * inner + columns), bytes_accessed=600_000_000, transcendentals=0
        ),
        name="chain",
    )(part, ggr, grad_value, grad_rest, w_gate, w_value, w_both_t, w_step_t)


def finish_kernel(
    early, scale_ref, early_a_ref, early_b_ref, late_a_ref, late_b_ref, grad_a_ref, grad_b_ref, x_ref, cot_ref, gain_ref,
    a_ref, b_ref, c_ref, mixed_ref, grad_out_ref, a_out_ref, b_out_ref, c_out_ref,
):
    at = pl.program_id(0)
    width = x_ref.shape[1]

    def half(side, early_ref, late_ref, grad_ref):
        def part(k, none):
            own = pl.ds(pl.multiple_of(k * 64, 64), 64)
            rows = pl.ds(pl.multiple_of(side * SPAN + k * 64, 64), 64)
            x = x_ref[rows, :].astype(F32)
            is_early = 2 * at + side < early
            total = jnp.where(is_early, early_ref[own, :].astype(F32), late_ref[own, :].astype(F32))
            mixed_ref[rows, :] = (x + scale_ref[rows, 0:1] * total).astype(BF16)
            inverse = lax.rsqrt(jnp.mean(x * x, -1, keepdims=True) + EPSILON)
            weighted = grad_ref[own, :].astype(F32) * gain_ref[...]
            dot = jnp.sum(weighted * x, -1, keepdims=True)
            grad_out_ref[rows, :] = cot_ref[rows, :].astype(F32) + inverse * weighted - x * (inverse**3 * dot / width)
            return none

        lax.fori_loop(0, SPAN // 64, part, 0)

    half(0, early_a_ref, late_a_ref, grad_a_ref)
    half(1, early_b_ref, late_b_ref, grad_b_ref)
    for source, target in ((a_ref, a_out_ref), (b_ref, b_out_ref), (c_ref, c_out_ref)):
        target[...] = source[...].astype(F32)


def finish(scale, out_early, chained, hidden, cotangent, gain, sums):
    tokens, width = hidden.shape
    steps = tokens // CHUNK
    early = out_early.shape[0] // SPAN
    late = tokens // SPAN - early
    rows = lambda n: pl.BlockSpec((CHUNK, n), lambda i: (i, 0))
    some = lambda at: pl.BlockSpec((SPAN, width), lambda i: (at(i), 0))
    parts = [pl.BlockSpec((a.shape[0] // steps, a.shape[1]), lambda i: (i, 0)) for a in sums]
    return pl.pallas_call(
        partial(finish_kernel, early),
        grid=(steps,),
        in_specs=[
            rows(LANES),
            some(lambda i: jnp.minimum(2 * i, early - 1)), some(lambda i: jnp.minimum(2 * i + 1, early - 1)),
            some(lambda i: jnp.maximum(2 * i - early, 0)), some(lambda i: jnp.maximum(2 * i + 1 - early, 0)),
            some(lambda i: late + 2 * i), some(lambda i: late + 2 * i + 1),
            rows(width), rows(width), pl.BlockSpec((1, width), lambda i: (0, 0)),
        ] + parts,
        out_specs=[rows(width), rows(width)] + parts,
        out_shape=[jax.ShapeDtypeStruct((tokens, width), BF16), jax.ShapeDtypeStruct((tokens, width), F32)]
        + [jax.ShapeDtypeStruct(a.shape, F32) for a in sums],
        cost_estimate=pl.CostEstimate(flops=0, bytes_accessed=80_000_000, transcendentals=0),
        name="finish",
    )(scale, out_early, out_early, chained, chained, chained, chained, hidden, cotangent, gain, *sums)


def pack_kernel(rest_ref, wb_ref, ws_ref, pg_ref, pv_ref, norm_ref, small_ref, packed_ref):
    both, steps, width = wb_ref.shape[0], ws_ref.shape[0], ws_ref.shape[1]
    state = rest_ref[:both] + rest_ref[both : 2 * both]
    step = rest_ref[2 * both : 2 * both + steps]
    products = jnp.sum(state * wb_ref[:, :width].astype(F32), 0, keepdims=True) + pg_ref[...][None] + pv_ref[...][None]
    products = products + jnp.sum(step * ws_ref[...].astype(F32), 0, keepdims=True)
    packed_ref[:both] = state
    packed_ref[both : both + 16] = rest_ref[2 * both : 2 * both + 16]
    small = small_ref[...]
    packed_ref[both + 16 :] = jnp.where(iota(small.shape, 0) == 9, products / norm_ref[...], small)


def pack(grad_rest_t, w_both_t, w_step_t, products_gate, products_value, norm, small):
    both, width = w_both_t.shape[0], w_step_t.shape[1]
    return pl.pallas_call(
        pack_kernel,
        out_shape=jax.ShapeDtypeStruct((both + 32, width), F32),
        name="pack",
    )(grad_rest_t, w_both_t, w_step_t, products_gate, products_value, norm, small)


def late_kernel(packed_ref, *parts):
    state_local, count = parts[0].shape[0] - 16, len(parts) + 1
    place = lax.axis_index("head")
    small = packed_ref[count * state_local + 16 :].astype(BF16)
    for steps, part in enumerate(parts, 1):
        at = pl.multiple_of(lax.rem(place + steps, count) * state_local, state_local)
        part[:state_local] = packed_ref[pl.ds(at, state_local), :].astype(BF16)
        part[state_local:] = small


def late_parts(packed, state_local, count):
    shape = jax.ShapeDtypeStruct((state_local + 16, packed.shape[1]), BF16)
    return pl.pallas_call(late_kernel, out_shape=[shape] * (count - 1), name="late")(packed)


def unpack_kernel(count, packed_ref, *refs):
    others, refs = refs[: count - 1], refs[count - 1 :]
    state_ref, step_ref, norm_ref, cv_ref, cvb_ref, cs_ref, csb_ref, decay_ref, bias_ref, skip_ref, gain_ref = refs
    state_local, heads, inner = state_ref.shape[0], step_ref.shape[0], cv_ref.shape[1]
    both = state_local * count
    place = lax.axis_index("head")
    own = packed_ref[pl.ds(pl.multiple_of(place * state_local, state_local), state_local), :]
    state_ref[...] = own + sum(ref[:state_local].astype(F32) for ref in others)
    step_ref[...] = packed_ref[both : both + heads]
    small = packed_ref[both + 16 :]
    total = small + sum(ref[state_local:].astype(F32) for ref in others)
    norm_ref[...] = total[9]
    cv_ref[...] = small[:4, :inner]
    cvb_ref[...] = small[4, :inner]
    for q in range(count):
        @pl.when(place == q)
        def _(q=q):
            mine = total[:8, inner + q * state_local : inner + (q + 1) * state_local]
            cs_ref[...] = mine[:4]
            csb_ref[...] = mine[4]
    decay_ref[...] = small[5, :heads]
    bias_ref[...] = small[6, :heads]
    skip_ref[...] = small[7, :heads]
    gain_ref[...] = small[8, :inner]


def unpack(packed, others, inner, heads, state_local):
    width = packed.shape[1]
    shapes = [
        (state_local, width), (heads, width), (width,), (4, inner), (inner,), (4, state_local), (state_local,),
        (heads,), (heads,), (heads,), (inner,),
    ]
    return pl.pallas_call(
        partial(unpack_kernel, len(others) + 1),
        out_shape=[jax.ShapeDtypeStruct(shape, F32) for shape in shapes],
        name="unpack",
    )(packed, *others)


def passed_along(value, axis, steps):
    count = lax.axis_size(axis)
    first, last = (max(0, -steps), min(count, count - steps))
    return lax.ppermute(value, axis, [(source, source + steps) for source in range(first, last)])


def from_all(value, axis):
    count = lax.axis_size(axis)
    moved = lambda steps: lax.ppermute(value, axis, [(s, (s + steps) % count) for s in range(count)])
    return [value] + [moved(steps) for steps in range(1, count)]


def row_major(value):
    return with_layout_constraint(value, Layout(major_to_minor=(0, 1)))


def on_device(
    hidden, segment_ids, norm_gain, w_gate, w_value, w_state, w_step, conv_value, conv_value_bias, conv_state,
    conv_state_bias, decay_log, step_bias, skip_gain, gate_gain, w_out, cotangent,
):
    tokens, width = hidden.shape
    inner, heads_local, state_local = w_value.shape[1], w_step.shape[1], w_state.shape[1]
    count = lax.axis_size("head")

    ids = segment_ids.reshape(tokens // SPAN, SPAN)
    packed, taps_value, heads, norm, gain, w_step_t, picks, sums_of = prepare(
        w_state.T, conv_state, conv_state_bias, conv_value, conv_value_bias, decay_log, step_bias, skip_gain,
        norm_gain, gate_gain, w_step.T,
    )
    gathered = lax.all_gather(packed, "head", axis=0, tiled=True)

    normed, gate_raw, cv, step_raw = project(hidden, norm, w_gate, w_value, w_step_t)
    last_ids = jnp.pad(segment_ids[tokens - 8 :].astype(F32).astype(BF16)[:, None], ((0, 0), (0, LANES - 1)))
    tail = jnp.concatenate([cv[tokens - 8 :], last_ids, normed[tokens - 8 :]], 1)
    halo = passed_along(tail, "seq", 1)
    gg = nt(cotangent, w_out).astype(BF16)
    y, bc, cum, reach, enter, local_end, kept, tokens_info, seg_rows, cs, taps, rim = scan(
        cv, normed, halo, step_raw, ids, heads, taps_value, gathered, picks
    )
    state_in = passed_along(local_end, "seq", 1)
    low, sums = gate_sums(y, reach, bc, state_in, gate_raw, gg, gain, picks)
    early = EARLY * ITEM
    out_early = lax.psum(nn(low[:early], w_out).astype(BF16), "head")
    sums = from_all(sums, "head")
    out_late = nn(low[early:], w_out).astype(BF16)

    gs, grad_gate_raw, gate_low, scale, gain_sum, grad_state_in = ungate(
        y, gate_raw, gg, gain, reach, bc, state_in, picks, sums
    )
    grad_end = passed_along(grad_state_in, "seq", -1)
    grad_w_out = row_major(tn(gate_low, cotangent))
    grad_value, grad_rest, small, head_rows = unscan(
        gs, cv, cs, rim, bc, step_raw, cum, tokens_info, seg_rows, heads, taps, enter, kept, state_in, grad_end,
        gain_sum, picks, sums_of, width,
    )
    from_next = passed_along(head_rows, "seq", -1)
    grad_w_gate = row_major(tn(normed, grad_gate_raw))
    products_gate = jnp.sum(w_gate.astype(F32) * grad_w_gate, 1)

    def with_next(a, low, high):
        tail = (a[tokens - 8 :, : high - low].astype(F32) + from_next[:, low:high]).astype(BF16)
        return lax.dynamic_update_slice(a, tail, (tokens - 8, 0))

    grad_value = with_next(grad_value, 0, inner)
    grad_rest = with_next(grad_rest, inner, inner + 2 * STATE)
    grad_w_value = row_major(tn(normed, grad_value))
    grad_rest_t = row_major(tn(grad_rest, normed))
    chained = chain_sums(out_late, grad_gate_raw, grad_value, grad_rest, w_gate, w_value, gathered, w_step_t)

    packed = pack(
        grad_rest_t, gathered, w_step_t, products_gate,
        jnp.sum(w_value.astype(F32) * grad_w_value, 1), norm, small,
    )
    weights = lax.psum(tuple(a.astype(BF16) for a in (grad_w_gate, grad_w_value, grad_w_out)), "seq")
    packed = lax.psum(packed, "seq")

    others = [
        lax.ppermute(part, "head", [(s, (s + steps) % count) for s in range(count)])
        for steps, part in enumerate(late_parts(packed, state_local, count), 1)
    ]
    mixed, grad_hidden, *weights = finish(scale, out_early, chained, hidden, cotangent, norm, weights)
    state_t, step_t, *rest = unpack(packed, others, inner, heads_local, state_local)
    return (mixed, grad_hidden, rest[0], weights[0], weights[1], state_t.T, step_t.T, *rest[1:], weights[2])


def solution(mesh):
    columns, split = P(None, "head"), P("head")
    rows = P("seq", None)

    return jax.shard_map(
        on_device,
        mesh=mesh,
        in_specs=(
            rows, P("seq"), P(), columns, columns, columns, columns, columns, split, columns, split, split, split,
            split, split, P("head", None), rows,
        ),
        out_specs=(
            rows, rows, P(), columns, columns, columns, columns, columns, split, columns, split, split, split, split,
            split, P("head", None),
        ),
        check_vma=False,
    )
```

```python
from functools import partial

import jax
import jax.numpy as jnp
from jax import lax
from jax.experimental import pallas as pl
from jax.experimental.layout import Layout, with_layout_constraint
from jax.experimental.pallas import tpu as pltpu
from jax.sharding import PartitionSpec as P


EPSILON = 1e-05
VERY_NEGATIVE = -1e30
CHUNK = 256
SPAN = 128
STATE = 128
WIDTH = 64
LANES = 128
F32 = jnp.float32
BF16 = jnp.bfloat16
ONE = pl.Buffered(1)
EARLY = 40
TOGETHER = 4


def nn(a, b):
    return lax.dot_general(a, b, (((1,), (0,)), ((), ())), preferred_element_type=F32)


def nt(a, b):
    return lax.dot_general(a, b, (((1,), (1,)), ((), ())), preferred_element_type=F32)


def tn(a, b):
    return lax.dot_general(a, b, (((0,), (0,)), ((), ())), preferred_element_type=F32)


def exact(a, b):
    return lax.dot_general(
        a, b, (((1,), (0,)), ((), ())), preferred_element_type=F32, precision=lax.Precision.HIGHEST
    )


def iota(shape, axis):
    return lax.broadcasted_iota(jnp.int32, shape, axis)


def pair_of(columns, pair):
    rows = columns.shape[0]
    first = jnp.broadcast_to(columns[:, 2 * pair : 2 * pair + 1], (rows, LANES))
    second = jnp.broadcast_to(columns[:, 2 * pair + 1 : 2 * pair + 2], (rows, LANES))
    return jnp.where(iota((rows, LANES), 1) < WIDTH, first, second)


def spread(columns, low, width):
    parts = [pair_of(columns, (low + at) // LANES) for at in range(0, width, LANES)]
    return jnp.concatenate(parts, 1) if len(parts) > 1 else parts[0]


def head_sums(values, sums):
    high, rest = halves(values)
    return nn(high, sums) + nn(rest, sums)


def groups(inner):
    return [(low, min(2 * LANES, inner - low)) for low in range(0, inner, 2 * LANES)]


def from_before(rows, previous, steps):
    turned = pltpu.roll(rows, steps, 0)
    head = pltpu.roll(previous, steps, 0)
    top = jnp.where(iota(head.shape, 0) < steps, head, turned[:8])
    return jnp.concatenate([top, turned[8:]], 0)


def from_after(rows, following, steps):
    count = rows.shape[0]
    turned = pltpu.roll(rows, count - steps, 0)
    tail = pltpu.roll(following, 8 - steps, 0)
    bottom = jnp.where(iota(tail.shape, 0) >= 8 - steps, tail, turned[count - 8 :])
    return jnp.concatenate([turned[: count - 8], bottom], 0)


def softplus(v):
    return jnp.maximum(v, 0.0) + jnp.log1p(jnp.exp(-jnp.abs(v)))


def sigmoid(v):
    return 0.5 + 0.5 * jnp.tanh(0.5 * v)


def halves(value):
    high = value.astype(BF16)
    return high, (value - high.astype(F32)).astype(BF16)


def column(tokens, index, width=LANES):
    return jnp.broadcast_to(tokens[:, index : index + 1], (tokens.shape[0], width))


def conv_taps(taps, rows, previous, visible):
    pre = taps[4:5] + taps[3:4] * rows
    shifted = [rows]
    for steps in range(1, 4):
        moved = from_before(rows, previous, steps) * visible[steps - 1]
        shifted.append(moved)
        pre = pre + taps[3 - steps : 4 - steps] * moved
    return pre, shifted


def mask_of(tokens, seg_row):
    same = tokens[:, 0:1] == seg_row
    count = tokens.shape[0]
    causal = iota((count, count), 0) >= iota((count, count), 1)
    return jnp.where(same & causal, 0.0, VERY_NEGATIVE)


def prepare_kernel(
    ws_ref, cs_ref, csb_ref, cv_ref, cvb_ref, decay_ref, bias_ref, skip_ref, norm_ref, gain_ref, wstep_ref,
    packed_ref, taps_ref, heads_ref, norm_out_ref, gain_out_ref, wstep_out_ref, picks_ref, sums_ref,
):
    width = ws_ref.shape[1]
    packed_ref[:, :width] = ws_ref[...]
    taps = jnp.concatenate([cs_ref[...], csb_ref[...][None], jnp.zeros((3, cs_ref.shape[1]), F32)], 0)
    taps = jnp.transpose(jnp.pad(taps, ((0, LANES - 8), (0, LANES - taps.shape[1]))))[: taps.shape[1]]
    for k in range(3):
        high = taps.astype(BF16)
        packed_ref[:, width + LANES * k : width + LANES * (k + 1)] = high
        taps = taps - high.astype(F32)
    packed_ref[:, width + 3 * LANES :] = jnp.zeros((taps.shape[0], LANES), BF16)
    inner = cv_ref.shape[1]
    taps_ref[...] = jnp.concatenate([cv_ref[...], cvb_ref[...][None], jnp.zeros((3, inner), F32)], 0)
    rows = [-jnp.exp(decay_ref[...])[None], bias_ref[...][None], skip_ref[...][None]]
    count = decay_ref.shape[0]
    heads_ref[...] = jnp.pad(
        jnp.concatenate(rows + [jnp.zeros((5, count), F32)], 0), ((0, 0), (0, LANES - count))
    )
    norm_out_ref[...] = norm_ref[...][None]
    gain_out_ref[...] = gain_ref[...][None]
    wstep_out_ref[...] = jnp.concatenate([wstep_ref[...].astype(F32), jnp.zeros((16 - count, width), F32)], 0).astype(BF16)
    shape = picks_ref.shape
    picks_ref[...] = jnp.where(iota(shape, 0) % LANES == iota(shape, 1) // WIDTH, 1.0, 0.0).astype(BF16)
    shape = sums_ref.shape
    sums_ref[...] = jnp.where(iota(shape, 0) // WIDTH == iota(shape, 1), 1.0, 0.0).astype(BF16)


def prepare(w_state_t, conv_state, conv_state_bias, conv_value, conv_value_bias, decay, bias, skip, norm, gain, w_step_t
):
    state_local, width = w_state_t.shape
    inner = conv_value.shape[1]
    return pl.pallas_call(
        prepare_kernel,
        out_shape=[
            jax.ShapeDtypeStruct((state_local, width + 4 * LANES), BF16),
            jax.ShapeDtypeStruct((8, inner), F32),
            jax.ShapeDtypeStruct((8, LANES), F32),
            jax.ShapeDtypeStruct((1, width), F32),
            jax.ShapeDtypeStruct((1, inner), F32),
            jax.ShapeDtypeStruct((16, width), BF16),
            jax.ShapeDtypeStruct((2 * LANES, inner), BF16),
            jax.ShapeDtypeStruct((inner, LANES), BF16),
        ],
        name="prepare",
    )(w_state_t, conv_state, conv_state_bias, conv_value, conv_value_bias, decay, bias, skip, norm, gain, w_step_t)


def project_kernel(x_ref, gain_ref, wg_ref, wv_ref, ws_ref, normed_ref, gate_ref, conv_ref, step_ref):
    x = x_ref[...].astype(F32)
    inverse = lax.rsqrt(jnp.mean(x * x, -1, keepdims=True) + EPSILON)
    normed = (x * inverse * gain_ref[...]).astype(BF16)
    normed_ref[...] = normed
    gate_ref[...] = nn(normed, wg_ref[...]).astype(BF16)
    conv_ref[...] = nn(normed, wv_ref[...]).astype(BF16)
    step = nt(normed, ws_ref[...])
    step_ref[...] = jnp.concatenate([step, jnp.zeros((CHUNK, LANES - step.shape[1]), F32)], 1)


def project(hidden, gain, w_gate, w_value, w_step_t):
    tokens, width = hidden.shape
    inner = w_gate.shape[1]
    rows = lambda n: pl.BlockSpec((CHUNK, n), lambda i: (i, 0))
    whole = lambda a: pl.BlockSpec(a.shape, lambda i: (0, 0), pipeline_mode=ONE)
    return pl.pallas_call(
        project_kernel,
        grid=(tokens // CHUNK,),
        in_specs=[rows(width), whole(gain), whole(w_gate), whole(w_value), whole(w_step_t)],
        out_specs=[rows(width), rows(inner), rows(inner), rows(LANES)],
        out_shape=[
            jax.ShapeDtypeStruct((tokens, width), BF16),
            jax.ShapeDtypeStruct((tokens, inner), BF16),
            jax.ShapeDtypeStruct((tokens, inner), BF16),
            jax.ShapeDtypeStruct((tokens, LANES), F32),
        ],
        cost_estimate=pl.CostEstimate(
            flops=2 * tokens * width * (2 * inner + LANES),
            bytes_accessed=tokens * (4 * width + 6 * inner) + 4 * width * inner,
            transcendentals=0,
        ),
        name="project",
    )(hidden, gain, w_gate, w_value, w_step_t)


def scan_kernel(
    cv_ref, normed_ref, halo_ref, step_ref, ids_ref, heads_ref, taps_value_ref, gathered_ref, picks_ref,
    y_ref, bc_ref, cum_ref, reach_ref, enter_ref, end_ref, kept_ref, tok_ref, seg_ref, cs_ref, taps_ref, rim_ref,
    carry, state, offset, reached, before, projected,
):
    at = pl.program_id(0)
    inner, width = cv_ref.shape[1], normed_ref.shape[1]
    count = SPAN

    @pl.when(at == 0)
    def _():
        columns = sum(gathered_ref[:, width + LANES * k : width + LANES * (k + 1)].astype(F32) for k in range(3))
        taps_ref[:, :inner] = taps_value_ref[...]
        taps_ref[:, inner:] = jnp.transpose(columns)[:8]
        halo = halo_ref[...].astype(F32)
        rim_rows = halo[:, inner + LANES :].astype(BF16)
        rim_state = nt(jnp.concatenate([rim_rows, rim_rows], 0), gathered_ref[:, :width])[:8].astype(BF16)
        rim = jnp.concatenate([halo[:, :inner], rim_state.astype(F32)], 1)
        carry[...] = rim
        rim_ref[...] = rim
        turned = jnp.concatenate([halo[:, inner : inner + LANES], jnp.zeros((LANES - 8, LANES), F32)], 0)
        turned = pltpu.roll(jnp.transpose(turned)[:8], LANES - 8, 1)
        before[...] = jnp.where(lax.axis_index("seq") == 0, -1.0, turned)
        state[...] = jnp.zeros_like(state)
        offset[...] = jnp.zeros_like(offset)
        reached[...] = jnp.ones_like(reached)

    blocks = ids_ref.shape[0]
    own_row = lambda index: ids_ref[pl.ds(index, 1), :].astype(F32)
    previous = before[0:1]
    here = own_row(at)
    earlier = jnp.where(at == 0, previous, own_row(jnp.maximum(at - 1, 0)))
    later = jnp.where(at == blocks - 1, -2.0, own_row(jnp.minimum(at + 1, blocks - 1)))
    lane = iota((1, LANES), 1)
    seg = here
    flags = [here == here]
    for steps in range(1, 4):
        moved = jnp.where(lane < steps, pltpu.roll(earlier, steps, 1), pltpu.roll(here, steps, 1))
        flags.append(moved == here)
    for steps in range(1, 4):
        end = lane >= LANES - steps
        moved = jnp.where(end, pltpu.roll(later, LANES - steps, 1), pltpu.roll(here, LANES - steps, 1))
        flags.append(moved == here)
    first_id = own_row(0)[:, :1]
    flags.append(here == earlier[:, LANES - 1 :])
    flags.append(here == here[:, LANES - 1 :])
    flags.append((here == first_id) & (previous[:, LANES - 1 :] == first_id))
    rows = [seg] + [jnp.where(flag, 1.0, 0.0) for flag in flags[1:]]
    tokens = jnp.transpose(jnp.concatenate(rows + [jnp.zeros((LANES - len(rows), LANES), F32)], 0))
    tok_ref[...] = tokens
    seg_ref[0] = jnp.broadcast_to(seg, (8, LANES))
    heads = heads_ref[...]
    step = softplus(step_ref[...] + heads[1:2])
    log_decay = heads[0:1] * step
    lower = jnp.where(iota((count, count), 0) >= iota((count, count), 1), 1.0, 0.0)
    cum = exact(lower, log_decay)
    cum_ref[...] = cum
    kept_ref[0] = reached[...]
    reach = jnp.exp(cum + offset[0:1]) * column(tokens, 9)
    reach_ref[...] = reach
    last = cum[count - 1 : count]
    offset[...] = offset[...] + last
    reached[...] = jnp.broadcast_to(reach[count - 1 : count], reached.shape)
    start = jnp.exp(cum) * column(tokens, 7)
    end = jnp.exp(last - cum) * column(tokens, 8)
    through = start[count - 1 : count]
    cum_t = jnp.transpose(cum)
    visible = [column(tokens, 1 + k, 2 * LANES) for k in range(3)]

    def conv(rows, at_column):
        width = rows.shape[1]
        wide = slice(at_column, at_column + width)
        pre, _ = conv_taps(taps_ref[:, wide], rows, carry[:, wide], [v[:, :width] for v in visible])
        carry[:, wide] = rows[count - 8 :]
        return pre * sigmoid(pre)


    @pl.when(at % TOGETHER == 0)
    def _():
        projected[...] = nt(normed_ref[...], gathered_ref[:, :width]).astype(BF16)

    cs = projected[pl.ds(pl.multiple_of(at % TOGETHER * count, count), count), :]
    cs_ref[...] = cs
    both = conv(cs.astype(F32), inner).astype(BF16)
    bc_ref[...] = both
    b_low, c_low = both[:, :LANES], both[:, LANES:]
    scores = nt(c_low, b_low)
    hidden_pairs = mask_of(tokens, seg)
    enter_ref[0] = state[...]
    left = iota((count, LANES), 1) < WIDTH
    b_t = jnp.transpose(b_low.astype(F32)).astype(BF16)
    factors = jnp.concatenate(halves(jnp.concatenate([step, start, end], 0)), 1)

    for low, width in groups(inner):
        wide = slice(low, low + width)
        values = conv(cv_ref[:, wide].astype(F32), low)
        steps_wide, starts, ends = jnp.split(nn(factors, picks_ref[:, wide]), 3)
        scaled = values * steps_wide
        entering = state[:, wide]
        y = starts * nn(c_low, entering.astype(BF16))
        y = y + spread(heads[2:3], low, width) * values
        inside = []
        for part in range(0, width, LANES):
            weights, mine = [], []
            for side in range(2):
                head = (low + part) // WIDTH + side
                decay = jnp.exp(cum[:, head : head + 1] - cum_t[head : head + 1] + hidden_pairs)
                here = left if side == 0 else ~left
                mine.append(jnp.where(here, scaled[:, part : part + LANES], 0.0).astype(BF16))
                weights.append((decay * scores).astype(BF16))
            inside.append(nn(jnp.concatenate(weights, 1), jnp.concatenate(mine, 0)))
        y_ref[:, wide] = (y + jnp.concatenate(inside, 1)).astype(BF16)
        state[:, wide] = spread(through, low, width) * entering + nn(
            b_t, (scaled * ends).astype(BF16)
        )
    end_ref[...] = state[...]


def scan(cv, normed, halo, step_raw, ids, heads, taps_value, gathered, picks):
    tokens, inner = cv.shape
    blocks, total = tokens // SPAN, inner + 2 * STATE
    fixed = lambda n: pl.BlockSpec((8, n), lambda i: (0, 0))
    together = pl.BlockSpec((TOGETHER * SPAN, normed.shape[1]), lambda i: (i // TOGETHER, 0))
    rows = lambda n: pl.BlockSpec((SPAN, n), lambda i: (i, 0))
    whole = lambda a: pl.BlockSpec(a.shape, lambda i: (0, 0), pipeline_mode=ONE)
    return pl.pallas_call(
        scan_kernel,
        grid=(blocks,),
        in_specs=[
            rows(inner), together, whole(halo), rows(LANES), whole(ids), whole(heads), whole(taps_value),
            whole(gathered), whole(picks),
        ],
        out_specs=[
            rows(inner), rows(2 * STATE), rows(LANES), rows(LANES),
            pl.BlockSpec((1, STATE, inner), lambda i: (i, 0, 0)),
            pl.BlockSpec((STATE, inner), lambda i: (0, 0)),
            pl.BlockSpec((1, 8, LANES), lambda i: (i, 0, 0)), rows(LANES), pl.BlockSpec((1, 8, SPAN), lambda i: (i, 0, 0)),
            rows(2 * STATE), fixed(total), fixed(total),
        ],
        out_shape=[
            jax.ShapeDtypeStruct((tokens, inner), BF16),
            jax.ShapeDtypeStruct((tokens, 2 * STATE), BF16),
            jax.ShapeDtypeStruct((tokens, LANES), F32),
            jax.ShapeDtypeStruct((tokens, LANES), F32),
            jax.ShapeDtypeStruct((blocks, STATE, inner), F32),
            jax.ShapeDtypeStruct((STATE, inner), F32),
            jax.ShapeDtypeStruct((blocks, 8, LANES), F32),
            jax.ShapeDtypeStruct((tokens, LANES), F32),
            jax.ShapeDtypeStruct((blocks, 8, SPAN), F32),
            jax.ShapeDtypeStruct((tokens, 2 * STATE), BF16),
            jax.ShapeDtypeStruct((8, total), F32),
            jax.ShapeDtypeStruct((8, total), F32),
        ],
        scratch_shapes=[
            pltpu.VMEM((8, inner + 2 * STATE), F32),
            pltpu.VMEM((STATE, inner), F32),
            pltpu.VMEM((8, LANES), F32),
            pltpu.VMEM((8, LANES), F32),
            pltpu.VMEM((8, LANES), F32),
            pltpu.VMEM((TOGETHER * SPAN, 2 * STATE), BF16),
        ],
        cost_estimate=pl.CostEstimate(
            flops=2 * tokens * inner * (2 * SPAN + 2 * STATE),
            bytes_accessed=tokens * (6 * inner + 4 * STATE + 8 * LANES),
            transcendentals=tokens * inner * 4,
        ),
        name="scan",
    )(cv, normed, halo, step_raw, ids, heads, taps_value, gathered, picks)


def gate_kernel(
    y_ref, reach_ref, bc_ref, state_ref, gate_ref, gg_ref, gain_ref, picks_ref, low_ref, sums_ref
):
    inner = y_ref.shape[1]
    c_low = bc_ref[:, LANES:]
    reach = jnp.concatenate(halves(reach_ref[...]), 1)
    squares = jnp.zeros((CHUNK, LANES), F32)
    dots = jnp.zeros((CHUNK, LANES), F32)
    for pair in range(inner // LANES):
        wide = slice(pair * LANES, (pair + 1) * LANES)
        reach_pair = nn(reach, picks_ref[:, wide])
        ssm = y_ref[:, wide].astype(F32) + reach_pair * nn(c_low, state_ref[:, wide].astype(BF16))
        gate = gate_ref[:, wide].astype(F32)
        gated = ssm * gate * sigmoid(gate)
        weighted = gated * gain_ref[:, wide]
        low_ref[:, wide] = weighted.astype(BF16)
        squares = squares + gated * gated
        dots = dots + gg_ref[:, wide].astype(F32) * weighted
    square = jnp.sum(squares, 1, keepdims=True)
    dot = jnp.sum(dots, 1, keepdims=True)
    sums_ref[...] = jnp.transpose(jnp.where(iota((CHUNK, LANES), 1) == 0, square, dot))[:8]


def gate_sums(y, reach, bc, state_in, gate_raw, gg, gain, picks):
    tokens, inner = y.shape
    rows = lambda n: pl.BlockSpec((CHUNK, n), lambda i: (i, 0))
    whole = lambda a: pl.BlockSpec(a.shape, lambda i: (0, 0), pipeline_mode=ONE)
    return pl.pallas_call(
        gate_kernel,
        grid=(tokens // CHUNK,),
        in_specs=[
            rows(inner), rows(LANES), rows(2 * STATE), whole(state_in), rows(inner), rows(inner), whole(gain),
            whole(picks),
        ],
        out_specs=[rows(inner), pl.BlockSpec((8, CHUNK), lambda i: (0, i))],
        out_shape=[
            jax.ShapeDtypeStruct((tokens, inner), BF16),
            jax.ShapeDtypeStruct((8, tokens), F32),
        ],
        cost_estimate=pl.CostEstimate(
            flops=2 * tokens * inner * STATE, bytes_accessed=tokens * inner * 12, transcendentals=tokens * inner
        ),
        name="gate",
    )(y, reach, bc, state_in, gate_raw, gg, gain, picks)


def ungate_kernel(count, y_ref, gate_ref, gg_ref, gain_ref, reach_ref, bc_ref, in_ref, picks_ref, *refs):
    sums_refs, (gs_ref, ggr_ref, low_ref, scale_ref, gain_sum_ref, state_ref, gain_acc, state_acc) = (
        refs[:count], refs[count:]
    )
    at = pl.program_id(0)
    inner = y_ref.shape[1]

    @pl.when(at == 0)
    def _():
        gain_acc[...] = jnp.zeros_like(gain_acc)
        state_acc[...] = jnp.zeros_like(state_acc)

    sums = sum(ref[...] for ref in sums_refs)
    sums = jnp.transpose(jnp.concatenate([sums, jnp.zeros((LANES - 8, CHUNK), F32)], 0))
    all_inner = count * inner
    scale = lax.rsqrt(column(sums, 0) / all_inner + EPSILON)
    shift = scale * scale * scale * column(sums, 1) / all_inner
    scale_ref[...] = scale
    reach = jnp.concatenate(halves(reach_ref[...]), 1)
    c_low = bc_ref[:, LANES:]
    c_t = jnp.transpose(c_low.astype(F32)).astype(BF16)
    for pair in range(inner // LANES):
        wide = slice(pair * LANES, (pair + 1) * LANES)
        reach_pair = nn(reach, picks_ref[:, wide])
        ssm = y_ref[:, wide].astype(F32) + reach_pair * nn(c_low, in_ref[:, wide].astype(BF16))
        gate, gg = gate_ref[:, wide].astype(F32), gg_ref[:, wide].astype(F32)
        sg = sigmoid(gate)
        act = gate * sg
        gated = ssm * act
        scaled = gated * scale
        low_ref[:, wide] = (scaled * gain_ref[:, wide]).astype(BF16)
        gain_acc[:, wide] += jnp.sum((gg * scaled).reshape(CHUNK // 8, 8, LANES), 0)
        grad_gated = scale * gg * gain_ref[:, wide] - gated * shift
        grad_ssm = grad_gated * act
        gs_ref[:, wide] = grad_ssm
        ggr_ref[:, wide] = (grad_gated * ssm * sg * (1.0 + gate * (1.0 - sg))).astype(BF16)
        state_acc[:, wide] += nn(c_t, (grad_ssm * reach_pair).astype(BF16))
    gain_sum_ref[...] = gain_acc[...]
    state_ref[...] = state_acc[...]


def ungate(y, gate_raw, gg, gain, reach, bc, state_in, picks, sums):
    tokens, inner = y.shape
    rows = lambda n: pl.BlockSpec((CHUNK, n), lambda i: (i, 0))
    whole = lambda a: pl.BlockSpec(a.shape, lambda i: (0, 0), pipeline_mode=ONE)
    fixed = lambda m, n: pl.BlockSpec((m, n), lambda i: (0, 0))
    return pl.pallas_call(
        partial(ungate_kernel, len(sums)),
        grid=(tokens // CHUNK,),
        in_specs=[
            rows(inner), rows(inner), rows(inner), whole(gain), rows(LANES), rows(2 * STATE), whole(state_in),
            whole(picks),
        ] + [pl.BlockSpec((8, CHUNK), lambda i: (0, i))] * len(sums),
        out_specs=[rows(inner), rows(inner), rows(inner), rows(LANES), fixed(8, inner), fixed(STATE, inner)],
        out_shape=[
            jax.ShapeDtypeStruct((tokens, inner), F32),
            jax.ShapeDtypeStruct((tokens, inner), BF16),
            jax.ShapeDtypeStruct((tokens, inner), BF16),
            jax.ShapeDtypeStruct((tokens, LANES), F32),
            jax.ShapeDtypeStruct((8, inner), F32),
            jax.ShapeDtypeStruct((STATE, inner), F32),
        ],
        scratch_shapes=[pltpu.VMEM((8, inner), F32), pltpu.VMEM((STATE, inner), F32)],
        cost_estimate=pl.CostEstimate(
            flops=2 * tokens * inner * STATE, bytes_accessed=tokens * inner * 16, transcendentals=tokens * inner
        ),
        name="ungate",
    )(y, gate_raw, gg, gain, reach, bc, state_in, picks, *sums)


def unscan_kernel(
    gs_ref, cv_ref, cv_before_ref, cs_ref, cs_before_ref, halo_ref, bc_ref, step_ref, cum_ref, tok_ref, seg_ref,
    heads_ref, taps_ref, enter_ref, kept_ref, state_in_ref, grad_end_ref, gain_sum_ref, picks_ref, sums_ref,
    value_ref, rest_ref, small_ref, head_rows_ref,
    carry, grad, taps_acc, heads_acc, skip_acc,
):
    turn = pl.program_id(0)
    at = pl.num_programs(0) - 1 - turn
    inner = gs_ref.shape[1]
    count = SPAN

    @pl.when(turn == 0)
    def _():
        carry[...] = jnp.zeros_like(carry)
        grad[...] = grad_end_ref[...]
        taps_acc[...] = jnp.zeros_like(taps_acc)
        heads_acc[...] = jnp.zeros_like(heads_acc)
        skip_acc[...] = jnp.zeros_like(skip_acc)

    first = at == 0
    tokens = tok_ref[...]
    heads = heads_ref[...]
    step_in = step_ref[...] + heads[1:2]
    step = softplus(step_in)
    log_decay = heads[0:1] * step
    cum = cum_ref[...]
    last = cum[count - 1 : count]
    start = jnp.exp(cum) * column(tokens, 7)
    end = jnp.exp(last - cum) * column(tokens, 8)
    through = start[count - 1 : count]
    cum_t = jnp.transpose(cum)
    visible = [column(tokens, 1 + k, 2 * LANES) for k in range(3)]
    seen = [column(tokens, 4 + k, 2 * LANES) for k in range(3)]
    left = iota((count, LANES), 1) < WIDTH
    b_low, c_low = bc_ref[:, :LANES], bc_ref[:, LANES:]
    scores = nt(c_low, b_low)
    hidden_pairs = mask_of(tokens, seg_ref[0, 0:1])
    c_t = jnp.transpose(c_low.astype(F32)).astype(BF16)
    kept = kept_ref[0]

    def conv(ref, before_ref, low, at_column, width):
        rows = ref[:, low : low + width].astype(F32)
        wide = slice(at_column, at_column + width)
        before = before_ref[8:16, low : low + width].astype(F32)
        before = jnp.where(first, halo_ref[:, wide].astype(F32), before)
        pre, shifted = conv_taps(taps_ref[:, wide], rows, before, [v[:, :width] for v in visible])
        return pre, shifted, sigmoid(pre)

    def unconv(grad_out, pre, sg, shifted, at_column, width):
        wide = slice(at_column, at_column + width)
        gp = grad_out * sg * (1.0 + pre * (1.0 - sg))
        eighths = lambda v: jnp.sum(v.reshape(count // 8, 8, width), 0)
        for k in range(4):
            taps_acc[8 * k : 8 * k + 8, wide] += eighths(gp * shifted[3 - k])
        taps_acc[32:40, wide] += eighths(gp)
        taps = taps_ref[:, wide]
        following = carry[:, wide]
        total = taps[3:4] * gp
        for steps in range(1, 4):
            moved = from_after(gp, following, steps) * seen[steps - 1][:, :width]
            total = total + taps[3 - steps : 4 - steps] * moved
        if at_column < inner:
            value_ref[:, wide] = total.astype(BF16)
        else:
            rest_ref[:, :width], rest_ref[:, width : 2 * width] = halves(total)
        carry[:, wide] = gp[:8]

        @pl.when(first)
        def _():
            back = jnp.zeros((8, width), F32)
            for steps in range(1, 4):
                moved = pltpu.roll(gp[:8] * visible[steps - 1][:8, :width], 8 - steps, 0)
                back = back + jnp.where(iota((8, width), 0) >= 8 - steps, taps[3 - steps : 4 - steps] * moved, 0.0)
            head_rows_ref[:, wide] = back

    grad_b = jnp.zeros((count, STATE), F32)
    grad_c = jnp.zeros((count, STATE), F32)
    grad_scores = jnp.zeros((count, count), F32)
    grad_cum = jnp.zeros((count, LANES), F32)
    grad_step = jnp.zeros((count, LANES), F32)
    at_end = jnp.zeros((8, LANES), F32)
    down = []
    factors = jnp.concatenate(halves(jnp.concatenate([step, start, end], 0)), 1)
    for low, width in groups(inner):
        wide = slice(low, low + width)
        pre, shifted, sg = conv(cv_ref, cv_before_ref, low, low, width)
        values = pre * sg
        step_wide, starts, ends = jnp.split(nn(factors, picks_ref[:, wide]), 3)
        scaled = values * step_wide
        scaled_low = scaled.astype(BF16)
        grad_y = gs_ref[:, wide]
        entering = enter_ref[0, :, wide] + spread(kept[0:1], low, width) * state_in_ref[:, wide]
        grad_state = grad[:, wide]
        grad_low = grad_state.astype(BF16)
        state_low, state_rest = halves(entering)
        to_end = ends * nn(b_low, grad_low)
        grad_y_in = grad_y * starts
        moved = scaled * to_end
        grad_cum = grad_cum + head_sums(grad_y_in * nn(c_low, state_low) - moved, sums_ref[wide])
        through_wide = spread(through, low, width)
        ending = jnp.sum(moved, 0, keepdims=True) + through_wide * jnp.sum(grad_state * entering, 0, keepdims=True)
        at_end = at_end + head_sums(jnp.broadcast_to(ending, (8, width)), sums_ref[wide])
        y_rest = grad_y - grad_y.astype(BF16).astype(F32)
        scaled_rest = (scaled - scaled_low.astype(F32)).astype(BF16)
        inside = []
        for part in range(0, width, LANES):
            here_lanes = slice(part, part + LANES)
            y_part, x_part = grad_y[:, here_lanes], scaled[:, here_lanes]
            y_turned, x_turned = pltpu.roll(y_rest[:, here_lanes], WIDTH, 1), pltpu.roll(x_part, WIDTH, 1)
            low_weights, low_mine = [], []
            for side in range(2):
                head = (low + part) // WIDTH + side
                here = left if side == 0 else ~left
                decay = jnp.exp(cum[:, head : head + 1] - cum_t[head : head + 1] + hidden_pairs)
                mine = jnp.where(here, y_part, 0.0).astype(BF16)
                weights = decay * scores
                grad_weights = nt(
                    jnp.concatenate([jnp.where(here, y_part, y_turned).astype(BF16), mine], 1),
                    jnp.concatenate([jnp.where(here, x_part, x_turned).astype(BF16), scaled_rest[:, here_lanes]], 1),
                )
                grad_scores = grad_scores + grad_weights * decay
                change = grad_weights * weights
                across = jnp.sum(change, 1, keepdims=True)
                down.append(jnp.sum(change, 0, keepdims=True))
                grad_cum = grad_cum + jnp.where(iota((count, LANES), 1) == head, across, 0.0)
                low_weights.append(weights.astype(BF16))
                low_mine.append(mine)
            inside.append(tn(jnp.concatenate(low_weights, 0), jnp.concatenate(low_mine, 0)))
        grad_scaled = to_end + jnp.concatenate(inside, 1)
        grad_low_in, grad_rest_in = halves(grad_y_in)
        grad_c = grad_c + nt(grad_low_in, state_low) + nt(grad_rest_in, state_low) + nt(grad_low_in, state_rest)
        grad_b = grad_b + nt((scaled * ends).astype(BF16), grad_low)
        grad[:, wide] = through_wide * grad_state + nn(c_t, grad_low_in)
        grad_step = grad_step + head_sums(grad_scaled * values, sums_ref[wide])
        skip_acc[:, wide] += jnp.sum((grad_y * values).reshape(count // 8, 8, width), 0)
        grad_values = grad_scaled * step_wide + spread(heads[2:3], low, width) * grad_y
        unconv(grad_values, pre, sg, shifted, low, width)
    down.append(jnp.zeros((LANES - len(down), count), F32))
    grad_cum = grad_cum - jnp.transpose(jnp.concatenate(down, 0))
    for part in halves(grad_scores):
        grad_c = grad_c + nn(part, b_low)
        grad_b = grad_b + tn(part, c_low)
    pre, shifted, sg = conv(cs_ref, cs_before_ref, 0, inner, 2 * STATE)
    unconv(jnp.concatenate([grad_b, grad_c], 1), pre, sg, shifted, inner, 2 * STATE)
    upper = jnp.where(iota((count, count), 0) <= iota((count, count), 1), 1.0, 0.0)
    grad_log = exact(upper, grad_cum) + at_end[0:1]
    grad_step = grad_step + heads[0:1] * grad_log
    grad_raw = grad_step * sigmoid(step_in)
    rest_ref[:, 4 * STATE :] = grad_raw.astype(BF16)
    heads_acc[...] += jnp.concatenate(
        [
            jnp.sum(grad_log * log_decay, 0, keepdims=True),
            jnp.sum(grad_raw, 0, keepdims=True),
            jnp.zeros((6, LANES), F32),
        ],
        0,
    )

    @pl.when(first)
    def _():
        down_rows = lambda v: jnp.sum(v, 0, keepdims=True)
        skip = sum(head_sums(skip_acc[:, low : low + width], sums_ref[low : low + width]) for low, width in groups(inner))
        wide = [down_rows(taps_acc[8 * k : 8 * k + 8]) for k in range(5)]
        wide += [heads_acc[0:1], heads_acc[1:2], down_rows(skip), down_rows(gain_sum_ref[...])]
        full = small_ref.shape[1]
        wide = [jnp.concatenate([v, jnp.zeros((1, full - v.shape[1]), F32)], 1) for v in wide]
        small_ref[...] = jnp.concatenate(wide + [jnp.zeros((16 - len(wide), full), F32)], 0)


def unscan(
    gs, cv, cs, halo, bc, step_raw, cum, tokens_info, seg_rows, heads, taps, enter, kept, state_in, grad_end, gain_sum,
    picks, sums, full,
):
    tokens, inner = gs.shape
    blocks = tokens // SPAN
    total = inner + 2 * STATE
    back = lambda i: blocks - 1 - i
    rows = lambda n: pl.BlockSpec((SPAN, n), lambda i: (back(i), 0))
    before = lambda n: pl.BlockSpec((16, n), lambda i: (jnp.maximum(back(i) * (SPAN // 16) - 1, 0), 0))
    whole = lambda a: pl.BlockSpec(a.shape, lambda i: (0, 0), pipeline_mode=ONE)
    fixed = lambda m, n: pl.BlockSpec((m, n), lambda i: (0, 0))
    return pl.pallas_call(
        unscan_kernel,
        grid=(blocks,),
        in_specs=[
            rows(inner), rows(inner), before(inner), rows(2 * STATE), before(2 * STATE), whole(halo), rows(2 * STATE),
            rows(LANES), rows(LANES), rows(LANES), pl.BlockSpec((1, 8, SPAN), lambda i: (back(i), 0, 0)),
            whole(heads), whole(taps), pl.BlockSpec((1, STATE, inner), lambda i: (back(i), 0, 0)),
            pl.BlockSpec((1, 8, LANES), lambda i: (back(i), 0, 0)), whole(state_in), whole(grad_end), whole(gain_sum),
            whole(picks), whole(sums),
        ],
        out_specs=[rows(inner), rows(4 * STATE + LANES), fixed(16, full), fixed(8, total)],
        out_shape=[
            jax.ShapeDtypeStruct((tokens, inner), BF16),
            jax.ShapeDtypeStruct((tokens, 4 * STATE + LANES), BF16),
            jax.ShapeDtypeStruct((16, full), F32),
            jax.ShapeDtypeStruct((8, total), F32),
        ],
        scratch_shapes=[
            pltpu.VMEM((8, total), F32),
            pltpu.VMEM((STATE, inner), F32),
            pltpu.VMEM((40, total), F32),
            pltpu.VMEM((8, LANES), F32),
            pltpu.VMEM((8, inner), F32),
        ],
        cost_estimate=pl.CostEstimate(
            flops=2 * tokens * inner * (6 * SPAN + 4 * STATE),
            bytes_accessed=tokens * (12 * inner),
            transcendentals=tokens * inner * 6,
        ),
        name="unscan",
    )(gs, cv, cv, cs, cs, halo, bc, step_raw, cum, tokens_info, seg_rows, heads, taps, enter, kept, state_in, grad_end, gain_sum, picks, sums)


def chain_kernel(
    first, size, part_ref, ggr_ref, gv_ref, gr_ref, wg_ref, wv_ref, wb_ref, ws_ref, out_ref,
    mine, outer, inner, sent_in, sent_out, came_outer, came_inner,
):
    turn = pl.program_id(0)
    items = mine.shape[0]
    place = lax.axis_index("head")
    half = size // 2
    low_side = place < half
    depth = jnp.where(low_side, place, size - 1 - place)
    toward = jnp.where(low_side, place + 1, place - 1)
    away = jnp.where(low_side, place - 1, place + 1)
    middle, edge = depth == half - 1, depth == 0
    away = jnp.where(edge, toward, away)

    def signal(target):
        pl.semaphore_signal(
            pltpu.get_barrier_semaphore(), inc=1, device_id={"head": target}, device_id_type=pl.DeviceIdType.MESH
        )

    def copy(source, target, sent, came, device):
        return pltpu.make_async_remote_copy(
            src_ref=source, dst_ref=target, send_sem=sent, recv_sem=came,
            device_id={"head": device}, device_id_type=pl.DeviceIdType.MESH,
        )

    def across(item):
        return copy(mine.at[item], inner.at[item], sent_in.at[item], came_inner.at[item], toward)

    def inward(item):
        return copy(mine.at[item], outer.at[item], sent_in.at[item], came_outer.at[item], toward)

    def outward(item):
        return copy(inner.at[item], inner.at[item], sent_out.at[item], came_inner.at[item], away)

    @pl.when(turn == 0)
    def _():
        signal(toward)

        @pl.when(jnp.logical_not(edge))
        def _():
            signal(away)
            pl.semaphore_wait(pltpu.get_barrier_semaphore(), 2)

        @pl.when(edge)
        def _():
            pl.semaphore_wait(pltpu.get_barrier_semaphore(), 1)

    @pl.when(turn < first)
    def _():
        mine[turn] = part_ref[...]

    @pl.when((turn >= first) & (turn < items) & ((turn - first) % GROUP == 0))
    def _():
        product = nt(ggr_ref[...], wg_ref[...]) + nt(gv_ref[...], wv_ref[...])
        both, steps = wb_ref.shape[0], ws_ref.shape[0]
        product = product + nn(gr_ref[:, :both], wb_ref[...]) + nn(gr_ref[:, both : 2 * both], wb_ref[...])
        product = product + nn(gr_ref[:, 2 * both : 2 * both + steps], ws_ref[...])
        for k in range(GROUP):
            mine[turn + k] = product[k * ITEM : (k + 1) * ITEM].astype(BF16)

    done = turn - behind(size)

    @pl.when(done >= 0)
    def _():
        across(done).wait_recv()

        @pl.when(middle)
        def _():
            inner[done] = (inner[done].astype(F32) + mine[done].astype(F32)).astype(BF16)

        @pl.when(jnp.logical_not(edge))
        def _():
            outward(done).start()

        out_ref[...] = inner[done]
        across(done).wait_send()

    item = turn - LAG * depth

    @pl.when((item >= 0) & (item < items))
    def _():
        @pl.when(jnp.logical_not(edge))
        def _():
            inward(item).wait_recv()
            mine[item] = (mine[item].astype(F32) + outer[item].astype(F32)).astype(BF16)

        @pl.when(middle)
        def _():
            across(item).start()

        @pl.when(jnp.logical_not(middle))
        def _():
            inward(item).start()

    @pl.when(turn == pl.num_programs(0) - 1)
    def _():
        @pl.when(jnp.logical_not(edge))
        def _():
            def wait(item, none):
                outward(item).wait_send()
                return none

            lax.fori_loop(0, items, wait, 0)


LAG = 8


def behind(size):
    return LAG * (size // 2 - 1) + 3


ITEM = 32
GROUP = 8


def chain_sums(part, ggr, grad_value, grad_rest, w_gate, w_value, w_both_t, w_step_t):
    tokens, inner = ggr.shape
    width, columns = w_gate.shape[0], grad_rest.shape[1]
    first = part.shape[0] // ITEM
    items = first + tokens // ITEM
    size = lax.axis_size("head")
    rows = lambda n, at: pl.BlockSpec((ITEM, n), lambda i: (at(i), 0))
    own = lambda n: pl.BlockSpec(
        (GROUP * ITEM, n), lambda i: (jnp.clip((i - first) // GROUP, 0, tokens // ITEM // GROUP - 1), 0)
    )
    whole = lambda a: pl.BlockSpec(a.shape, lambda i: (0, 0), pipeline_mode=ONE)
    slots = lambda: pltpu.VMEM((items, ITEM, width), BF16)
    return pl.pallas_call(
        partial(chain_kernel, first, size),
        grid=(items + behind(size),),
        in_specs=[
            rows(width, lambda i: jnp.minimum(i, first - 1)), own(inner), own(inner), own(columns), whole(w_gate),
            whole(w_value), pl.BlockSpec((2 * STATE, width), lambda i: (0, 0), pipeline_mode=ONE), whole(w_step_t),
        ],
        out_specs=rows(width, lambda i: jnp.maximum(i - behind(size), 0)),
        out_shape=jax.ShapeDtypeStruct((items * ITEM, width), BF16),
        scratch_shapes=[slots(), slots(), slots()] + [pltpu.SemaphoreType.DMA((items,))] * 4,
        compiler_params=pltpu.CompilerParams(collective_id=0, has_side_effects=True),
        cost_estimate=pl.CostEstimate(
            flops=2 * tokens * width * (2 * inner + columns), bytes_accessed=600_000_000, transcendentals=0
        ),
        name="chain",
    )(part, ggr, grad_value, grad_rest, w_gate, w_value, w_both_t, w_step_t)


def finish_kernel(
    early, scale_ref, early_a_ref, early_b_ref, late_a_ref, late_b_ref, grad_a_ref, grad_b_ref, x_ref, cot_ref, gain_ref,
    a_ref, b_ref, c_ref, mixed_ref, grad_out_ref, a_out_ref, b_out_ref, c_out_ref,
):
    at = pl.program_id(0)
    width = x_ref.shape[1]

    def half(side, early_ref, late_ref, grad_ref):
        def part(k, none):
            own = pl.ds(pl.multiple_of(k * 64, 64), 64)
            rows = pl.ds(pl.multiple_of(side * SPAN + k * 64, 64), 64)
            x = x_ref[rows, :].astype(F32)
            is_early = 2 * at + side < early
            total = jnp.where(is_early, early_ref[own, :].astype(F32), late_ref[own, :].astype(F32))
            mixed_ref[rows, :] = (x + scale_ref[rows, 0:1] * total).astype(BF16)
            inverse = lax.rsqrt(jnp.mean(x * x, -1, keepdims=True) + EPSILON)
            weighted = grad_ref[own, :].astype(F32) * gain_ref[...]
            dot = jnp.sum(weighted * x, -1, keepdims=True)
            grad_out_ref[rows, :] = cot_ref[rows, :].astype(F32) + inverse * weighted - x * (inverse**3 * dot / width)
            return none

        lax.fori_loop(0, SPAN // 64, part, 0)

    half(0, early_a_ref, late_a_ref, grad_a_ref)
    half(1, early_b_ref, late_b_ref, grad_b_ref)
    for source, target in ((a_ref, a_out_ref), (b_ref, b_out_ref), (c_ref, c_out_ref)):
        target[...] = source[...].astype(F32)


def finish(scale, out_early, chained, hidden, cotangent, gain, sums):
    tokens, width = hidden.shape
    steps = tokens // CHUNK
    early = out_early.shape[0] // SPAN
    late = tokens // SPAN - early
    rows = lambda n: pl.BlockSpec((CHUNK, n), lambda i: (i, 0))
    some = lambda at: pl.BlockSpec((SPAN, width), lambda i: (at(i), 0))
    parts = [pl.BlockSpec((a.shape[0] // steps, a.shape[1]), lambda i: (i, 0)) for a in sums]
    return pl.pallas_call(
        partial(finish_kernel, early),
        grid=(steps,),
        in_specs=[
            rows(LANES),
            some(lambda i: jnp.minimum(2 * i, early - 1)), some(lambda i: jnp.minimum(2 * i + 1, early - 1)),
            some(lambda i: jnp.maximum(2 * i - early, 0)), some(lambda i: jnp.maximum(2 * i + 1 - early, 0)),
            some(lambda i: late + 2 * i), some(lambda i: late + 2 * i + 1),
            rows(width), rows(width), pl.BlockSpec((1, width), lambda i: (0, 0)),
        ] + parts,
        out_specs=[rows(width), rows(width)] + parts,
        out_shape=[jax.ShapeDtypeStruct((tokens, width), BF16), jax.ShapeDtypeStruct((tokens, width), F32)]
        + [jax.ShapeDtypeStruct(a.shape, F32) for a in sums],
        cost_estimate=pl.CostEstimate(flops=0, bytes_accessed=80_000_000, transcendentals=0),
        name="finish",
    )(scale, out_early, out_early, chained, chained, chained, chained, hidden, cotangent, gain, *sums)


def pack_kernel(rest_ref, wb_ref, ws_ref, pg_ref, pv_ref, norm_ref, small_ref, packed_ref):
    both, steps, width = wb_ref.shape[0], ws_ref.shape[0], ws_ref.shape[1]
    state = rest_ref[:both] + rest_ref[both : 2 * both]
    step = rest_ref[2 * both : 2 * both + steps]
    products = jnp.sum(state * wb_ref[:, :width].astype(F32), 0, keepdims=True) + pg_ref[...][None] + pv_ref[...][None]
    products = products + jnp.sum(step * ws_ref[...].astype(F32), 0, keepdims=True)
    packed_ref[:both] = state
    packed_ref[both : both + 16] = rest_ref[2 * both : 2 * both + 16]
    small = small_ref[...]
    packed_ref[both + 16 :] = jnp.where(iota(small.shape, 0) == 9, products / norm_ref[...], small)


def pack(grad_rest_t, w_both_t, w_step_t, products_gate, products_value, norm, small):
    both, width = w_both_t.shape[0], w_step_t.shape[1]
    return pl.pallas_call(
        pack_kernel,
        out_shape=jax.ShapeDtypeStruct((both + 32, width), F32),
        name="pack",
    )(grad_rest_t, w_both_t, w_step_t, products_gate, products_value, norm, small)


def late_kernel(packed_ref, *parts):
    state_local, count = parts[0].shape[0] - 16, len(parts) + 1
    place = lax.axis_index("head")
    small = packed_ref[count * state_local + 16 :].astype(BF16)
    for steps, part in enumerate(parts, 1):
        at = pl.multiple_of(lax.rem(place + steps, count) * state_local, state_local)
        part[:state_local] = packed_ref[pl.ds(at, state_local), :].astype(BF16)
        part[state_local:] = small


def late_parts(packed, state_local, count):
    shape = jax.ShapeDtypeStruct((state_local + 16, packed.shape[1]), BF16)
    return pl.pallas_call(late_kernel, out_shape=[shape] * (count - 1), name="late")(packed)


def unpack_kernel(count, packed_ref, *refs):
    others, refs = refs[: count - 1], refs[count - 1 :]
    state_ref, step_ref, norm_ref, cv_ref, cvb_ref, cs_ref, csb_ref, decay_ref, bias_ref, skip_ref, gain_ref = refs
    state_local, heads, inner = state_ref.shape[0], step_ref.shape[0], cv_ref.shape[1]
    both = state_local * count
    place = lax.axis_index("head")
    own = packed_ref[pl.ds(pl.multiple_of(place * state_local, state_local), state_local), :]
    state_ref[...] = own + sum(ref[:state_local].astype(F32) for ref in others)
    step_ref[...] = packed_ref[both : both + heads]
    small = packed_ref[both + 16 :]
    total = small + sum(ref[state_local:].astype(F32) for ref in others)
    norm_ref[...] = total[9]
    cv_ref[...] = small[:4, :inner]
    cvb_ref[...] = small[4, :inner]
    for q in range(count):
        @pl.when(place == q)
        def _(q=q):
            mine = total[:8, inner + q * state_local : inner + (q + 1) * state_local]
            cs_ref[...] = mine[:4]
            csb_ref[...] = mine[4]
    decay_ref[...] = small[5, :heads]
    bias_ref[...] = small[6, :heads]
    skip_ref[...] = small[7, :heads]
    gain_ref[...] = small[8, :inner]


def unpack(packed, others, inner, heads, state_local):
    width = packed.shape[1]
    shapes = [
        (state_local, width), (heads, width), (width,), (4, inner), (inner,), (4, state_local), (state_local,),
        (heads,), (heads,), (heads,), (inner,),
    ]
    return pl.pallas_call(
        partial(unpack_kernel, len(others) + 1),
        out_shape=[jax.ShapeDtypeStruct(shape, F32) for shape in shapes],
        name="unpack",
    )(packed, *others)


def passed_along(value, axis, steps):
    count = lax.axis_size(axis)
    first, last = (max(0, -steps), min(count, count - steps))
    return lax.ppermute(value, axis, [(source, source + steps) for source in range(first, last)])


def from_all(value, axis):
    count = lax.axis_size(axis)
    moved = lambda steps: lax.ppermute(value, axis, [(s, (s + steps) % count) for s in range(count)])
    return [value] + [moved(steps) for steps in range(1, count)]


def row_major(value):
    return with_layout_constraint(value, Layout(major_to_minor=(0, 1)))


def on_device(
    hidden, segment_ids, norm_gain, w_gate, w_value, w_state, w_step, conv_value, conv_value_bias, conv_state,
    conv_state_bias, decay_log, step_bias, skip_gain, gate_gain, w_out, cotangent,
):
    tokens, width = hidden.shape
    inner, heads_local, state_local = w_value.shape[1], w_step.shape[1], w_state.shape[1]
    count = lax.axis_size("head")

    ids = segment_ids.reshape(tokens // SPAN, SPAN)
    packed, taps_value, heads, norm, gain, w_step_t, picks, sums_of = prepare(
        w_state.T, conv_state, conv_state_bias, conv_value, conv_value_bias, decay_log, step_bias, skip_gain,
        norm_gain, gate_gain, w_step.T,
    )
    gathered = lax.all_gather(packed, "head", axis=0, tiled=True)

    normed, gate_raw, cv, step_raw = project(hidden, norm, w_gate, w_value, w_step_t)
    last_ids = jnp.pad(segment_ids[tokens - 8 :].astype(F32).astype(BF16)[:, None], ((0, 0), (0, LANES - 1)))
    tail = jnp.concatenate([cv[tokens - 8 :], last_ids, normed[tokens - 8 :]], 1)
    halo = passed_along(tail, "seq", 1)
    gg = nt(cotangent, w_out).astype(BF16)
    y, bc, cum, reach, enter, local_end, kept, tokens_info, seg_rows, cs, taps, rim = scan(
        cv, normed, halo, step_raw, ids, heads, taps_value, gathered, picks
    )
    state_in = passed_along(local_end, "seq", 1)
    low, sums = gate_sums(y, reach, bc, state_in, gate_raw, gg, gain, picks)
    early = EARLY * ITEM
    out_early = lax.psum(nn(low[:early], w_out).astype(BF16), "head")
    sums = from_all(sums, "head")
    out_late = nn(low[early:], w_out).astype(BF16)

    gs, grad_gate_raw, gate_low, scale, gain_sum, grad_state_in = ungate(
        y, gate_raw, gg, gain, reach, bc, state_in, picks, sums
    )
    grad_end = passed_along(grad_state_in, "seq", -1)
    grad_w_out = row_major(tn(gate_low, cotangent))
    grad_value, grad_rest, small, head_rows = unscan(
        gs, cv, cs, rim, bc, step_raw, cum, tokens_info, seg_rows, heads, taps, enter, kept, state_in, grad_end,
        gain_sum, picks, sums_of, width,
    )
    from_next = passed_along(head_rows, "seq", -1)
    grad_w_gate = row_major(tn(normed, grad_gate_raw))
    products_gate = jnp.sum(w_gate.astype(F32) * grad_w_gate, 1)

    def with_next(a, low, high):
        tail = (a[tokens - 8 :, : high - low].astype(F32) + from_next[:, low:high]).astype(BF16)
        return lax.dynamic_update_slice(a, tail, (tokens - 8, 0))

    grad_value = with_next(grad_value, 0, inner)
    grad_rest = with_next(grad_rest, inner, inner + 2 * STATE)
    grad_w_value = row_major(tn(normed, grad_value))
    grad_rest_t = row_major(tn(grad_rest, normed))
    chained = chain_sums(out_late, grad_gate_raw, grad_value, grad_rest, w_gate, w_value, gathered, w_step_t)

    packed = pack(
        grad_rest_t, gathered, w_step_t, products_gate,
        jnp.sum(w_value.astype(F32) * grad_w_value, 1), norm, small,
    )
    weights = lax.psum(tuple(a.astype(BF16) for a in (grad_w_gate, grad_w_value, grad_w_out)), "seq")
    packed = lax.psum(packed, "seq")

    others = [
        lax.ppermute(part, "head", [(s, (s + steps) % count) for s in range(count)])
        for steps, part in enumerate(late_parts(packed, state_local, count), 1)
    ]
    mixed, grad_hidden, *weights = finish(scale, out_early, chained, hidden, cotangent, norm, weights)
    state_t, step_t, *rest = unpack(packed, others, inner, heads_local, state_local)
    return (mixed, grad_hidden, rest[0], weights[0], weights[1], state_t.T, step_t.T, *rest[1:], weights[2])


def solution(mesh):
    columns, split = P(None, "head"), P("head")
    rows = P("seq", None)

    return jax.shard_map(
        on_device,
        mesh=mesh,
        in_specs=(
            rows, P("seq"), P(), columns, columns, columns, columns, columns, split, columns, split, split, split,
            split, split, P("head", None), rows,
        ),
        out_specs=(
            rows, rows, P(), columns, columns, columns, columns, columns, split, columns, split, split, split, split,
            split, P("head", None),
        ),
        check_vma=False,
    )
```

```python
from functools import partial

import jax
import jax.numpy as jnp
from jax import lax
from jax.experimental import pallas as pl
from jax.experimental.layout import Layout, with_layout_constraint
from jax.experimental.pallas import tpu as pltpu
from jax.sharding import PartitionSpec as P


EPSILON = 1e-05
VERY_NEGATIVE = -1e30
CHUNK = 256
SPAN = 128
STATE = 128
WIDTH = 64
LANES = 128
F32 = jnp.float32
BF16 = jnp.bfloat16
ONE = pl.Buffered(1)
EARLY = 40


def nn(a, b):
    return lax.dot_general(a, b, (((1,), (0,)), ((), ())), preferred_element_type=F32)


def nt(a, b):
    return lax.dot_general(a, b, (((1,), (1,)), ((), ())), preferred_element_type=F32)


def tn(a, b):
    return lax.dot_general(a, b, (((0,), (0,)), ((), ())), preferred_element_type=F32)


def exact(a, b):
    return lax.dot_general(
        a, b, (((1,), (0,)), ((), ())), preferred_element_type=F32, precision=lax.Precision.HIGHEST
    )


def iota(shape, axis):
    return lax.broadcasted_iota(jnp.int32, shape, axis)


def pair_of(columns, pair):
    rows = columns.shape[0]
    first = jnp.broadcast_to(columns[:, 2 * pair : 2 * pair + 1], (rows, LANES))
    second = jnp.broadcast_to(columns[:, 2 * pair + 1 : 2 * pair + 2], (rows, LANES))
    return jnp.where(iota((rows, LANES), 1) < WIDTH, first, second)


def spread(columns, low, width):
    parts = [pair_of(columns, (low + at) // LANES) for at in range(0, width, LANES)]
    return jnp.concatenate(parts, 1) if len(parts) > 1 else parts[0]


def head_sums(values, sums):
    high, rest = halves(values)
    return nn(high, sums) + nn(rest, sums)


def groups(inner):
    return [(low, min(2 * LANES, inner - low)) for low in range(0, inner, 2 * LANES)]


def from_before(rows, previous, steps):
    turned = pltpu.roll(rows, steps, 0)
    head = pltpu.roll(previous, steps, 0)
    top = jnp.where(iota(head.shape, 0) < steps, head, turned[:8])
    return jnp.concatenate([top, turned[8:]], 0)


def from_after(rows, following, steps):
    count = rows.shape[0]
    turned = pltpu.roll(rows, count - steps, 0)
    tail = pltpu.roll(following, 8 - steps, 0)
    bottom = jnp.where(iota(tail.shape, 0) >= 8 - steps, tail, turned[count - 8 :])
    return jnp.concatenate([turned[: count - 8], bottom], 0)


def softplus(v):
    return jnp.maximum(v, 0.0) + jnp.log1p(jnp.exp(-jnp.abs(v)))


def sigmoid(v):
    return 0.5 + 0.5 * jnp.tanh(0.5 * v)


def halves(value):
    high = value.astype(BF16)
    return high, (value - high.astype(F32)).astype(BF16)


def column(tokens, index, width=LANES):
    return jnp.broadcast_to(tokens[:, index : index + 1], (tokens.shape[0], width))


def conv_taps(taps, rows, previous, visible):
    pre = taps[4:5] + taps[3:4] * rows
    shifted = [rows]
    for steps in range(1, 4):
        moved = from_before(rows, previous, steps) * visible[steps - 1]
        shifted.append(moved)
        pre = pre + taps[3 - steps : 4 - steps] * moved
    return pre, shifted


def mask_of(tokens, seg_row):
    same = tokens[:, 0:1] == seg_row
    count = tokens.shape[0]
    causal = iota((count, count), 0) >= iota((count, count), 1)
    return jnp.where(same & causal, 0.0, VERY_NEGATIVE)


def prepare_kernel(
    ws_ref, cs_ref, csb_ref, cv_ref, cvb_ref, decay_ref, bias_ref, skip_ref, norm_ref, gain_ref, wstep_ref,
    packed_ref, taps_ref, heads_ref, norm_out_ref, gain_out_ref, wstep_out_ref, picks_ref, sums_ref,
):
    width = ws_ref.shape[1]
    packed_ref[:, :width] = ws_ref[...]
    taps = jnp.concatenate([cs_ref[...], csb_ref[...][None], jnp.zeros((3, cs_ref.shape[1]), F32)], 0)
    taps = jnp.transpose(jnp.pad(taps, ((0, LANES - 8), (0, LANES - taps.shape[1]))))[: taps.shape[1]]
    for k in range(3):
        high = taps.astype(BF16)
        packed_ref[:, width + LANES * k : width + LANES * (k + 1)] = high
        taps = taps - high.astype(F32)
    packed_ref[:, width + 3 * LANES :] = jnp.zeros((taps.shape[0], LANES), BF16)
    inner = cv_ref.shape[1]
    taps_ref[...] = jnp.concatenate([cv_ref[...], cvb_ref[...][None], jnp.zeros((3, inner), F32)], 0)
    rows = [-jnp.exp(decay_ref[...])[None], bias_ref[...][None], skip_ref[...][None]]
    count = decay_ref.shape[0]
    heads_ref[...] = jnp.pad(
        jnp.concatenate(rows + [jnp.zeros((5, count), F32)], 0), ((0, 0), (0, LANES - count))
    )
    norm_out_ref[...] = norm_ref[...][None]
    gain_out_ref[...] = gain_ref[...][None]
    wstep_out_ref[...] = jnp.concatenate([wstep_ref[...].astype(F32), jnp.zeros((16 - count, width), F32)], 0).astype(BF16)
    shape = picks_ref.shape
    picks_ref[...] = jnp.where(iota(shape, 0) % LANES == iota(shape, 1) // WIDTH, 1.0, 0.0).astype(BF16)
    shape = sums_ref.shape
    sums_ref[...] = jnp.where(iota(shape, 0) // WIDTH == iota(shape, 1), 1.0, 0.0).astype(BF16)


def prepare(w_state_t, conv_state, conv_state_bias, conv_value, conv_value_bias, decay, bias, skip, norm, gain, w_step_t
):
    state_local, width = w_state_t.shape
    inner = conv_value.shape[1]
    return pl.pallas_call(
        prepare_kernel,
        out_shape=[
            jax.ShapeDtypeStruct((state_local, width + 4 * LANES), BF16),
            jax.ShapeDtypeStruct((8, inner), F32),
            jax.ShapeDtypeStruct((8, LANES), F32),
            jax.ShapeDtypeStruct((1, width), F32),
            jax.ShapeDtypeStruct((1, inner), F32),
            jax.ShapeDtypeStruct((16, width), BF16),
            jax.ShapeDtypeStruct((2 * LANES, inner), BF16),
            jax.ShapeDtypeStruct((inner, LANES), BF16),
        ],
        name="prepare",
    )(w_state_t, conv_state, conv_state_bias, conv_value, conv_value_bias, decay, bias, skip, norm, gain, w_step_t)


def project_kernel(x_ref, gain_ref, wg_ref, wv_ref, ws_ref, normed_ref, gate_ref, conv_ref, step_ref):
    x = x_ref[...].astype(F32)
    inverse = lax.rsqrt(jnp.mean(x * x, -1, keepdims=True) + EPSILON)
    normed = (x * inverse * gain_ref[...]).astype(BF16)
    normed_ref[...] = normed
    gate_ref[...] = nn(normed, wg_ref[...]).astype(BF16)
    conv_ref[...] = nn(normed, wv_ref[...]).astype(BF16)
    step = nt(normed, ws_ref[...])
    step_ref[...] = jnp.concatenate([step, jnp.zeros((CHUNK, LANES - step.shape[1]), F32)], 1)


def project(hidden, gain, w_gate, w_value, w_step_t):
    tokens, width = hidden.shape
    inner = w_gate.shape[1]
    rows = lambda n: pl.BlockSpec((CHUNK, n), lambda i: (i, 0))
    whole = lambda a: pl.BlockSpec(a.shape, lambda i: (0, 0), pipeline_mode=ONE)
    return pl.pallas_call(
        project_kernel,
        grid=(tokens // CHUNK,),
        in_specs=[rows(width), whole(gain), whole(w_gate), whole(w_value), whole(w_step_t)],
        out_specs=[rows(width), rows(inner), rows(inner), rows(LANES)],
        out_shape=[
            jax.ShapeDtypeStruct((tokens, width), BF16),
            jax.ShapeDtypeStruct((tokens, inner), BF16),
            jax.ShapeDtypeStruct((tokens, inner), BF16),
            jax.ShapeDtypeStruct((tokens, LANES), F32),
        ],
        cost_estimate=pl.CostEstimate(
            flops=2 * tokens * width * (2 * inner + LANES),
            bytes_accessed=tokens * (4 * width + 6 * inner) + 4 * width * inner,
            transcendentals=0,
        ),
        name="project",
    )(hidden, gain, w_gate, w_value, w_step_t)


def scan_kernel(
    cv_ref, cs_ref, halo_ref, step_ref, ids_ref, heads_ref, taps_value_ref, gathered_ref, picks_ref,
    y_ref, bc_ref, cum_ref, reach_ref, enter_ref, end_ref, kept_ref, tok_ref, seg_ref, taps_ref, rim_ref,
    carry, state, offset, reached, before,
):
    at = pl.program_id(0)
    inner, width = cv_ref.shape[1], gathered_ref.shape[1] - 4 * LANES
    count = SPAN

    @pl.when(at == 0)
    def _():
        columns = sum(gathered_ref[:, width + LANES * k : width + LANES * (k + 1)].astype(F32) for k in range(3))
        taps_ref[:, :inner] = taps_value_ref[...]
        taps_ref[:, inner:] = jnp.transpose(columns)[:8]
        halo = halo_ref[...].astype(F32)
        rim_rows = halo[:, inner + LANES :].astype(BF16)
        rim_state = nt(jnp.concatenate([rim_rows, rim_rows], 0), gathered_ref[:, :width])[:8].astype(BF16)
        rim = jnp.concatenate([halo[:, :inner], rim_state.astype(F32)], 1)
        carry[...] = rim
        rim_ref[...] = rim
        turned = jnp.concatenate([halo[:, inner : inner + LANES], jnp.zeros((LANES - 8, LANES), F32)], 0)
        turned = pltpu.roll(jnp.transpose(turned)[:8], LANES - 8, 1)
        before[...] = jnp.where(lax.axis_index("seq") == 0, -1.0, turned)
        state[...] = jnp.zeros_like(state)
        offset[...] = jnp.zeros_like(offset)
        reached[...] = jnp.ones_like(reached)

    blocks = ids_ref.shape[0]
    own_row = lambda index: ids_ref[pl.ds(index, 1), :].astype(F32)
    previous = before[0:1]
    here = own_row(at)
    earlier = jnp.where(at == 0, previous, own_row(jnp.maximum(at - 1, 0)))
    later = jnp.where(at == blocks - 1, -2.0, own_row(jnp.minimum(at + 1, blocks - 1)))
    lane = iota((1, LANES), 1)
    seg = here
    flags = [here == here]
    for steps in range(1, 4):
        moved = jnp.where(lane < steps, pltpu.roll(earlier, steps, 1), pltpu.roll(here, steps, 1))
        flags.append(moved == here)
    for steps in range(1, 4):
        end = lane >= LANES - steps
        moved = jnp.where(end, pltpu.roll(later, LANES - steps, 1), pltpu.roll(here, LANES - steps, 1))
        flags.append(moved == here)
    first_id = own_row(0)[:, :1]
    flags.append(here == earlier[:, LANES - 1 :])
    flags.append(here == here[:, LANES - 1 :])
    flags.append((here == first_id) & (previous[:, LANES - 1 :] == first_id))
    rows = [seg] + [jnp.where(flag, 1.0, 0.0) for flag in flags[1:]]
    tokens = jnp.transpose(jnp.concatenate(rows + [jnp.zeros((LANES - len(rows), LANES), F32)], 0))
    tok_ref[...] = tokens
    seg_ref[0] = jnp.broadcast_to(seg, (8, LANES))
    heads = heads_ref[...]
    step = softplus(step_ref[...] + heads[1:2])
    log_decay = heads[0:1] * step
    lower = jnp.where(iota((count, count), 0) >= iota((count, count), 1), 1.0, 0.0)
    cum = exact(lower, log_decay)
    cum_ref[...] = cum
    kept_ref[0] = reached[...]
    reach = jnp.exp(cum + offset[0:1]) * column(tokens, 9)
    reach_ref[...] = reach
    last = cum[count - 1 : count]
    offset[...] = offset[...] + last
    reached[...] = jnp.broadcast_to(reach[count - 1 : count], reached.shape)
    start = jnp.exp(cum) * column(tokens, 7)
    end = jnp.exp(last - cum) * column(tokens, 8)
    through = start[count - 1 : count]
    cum_t = jnp.transpose(cum)
    visible = [column(tokens, 1 + k, 2 * LANES) for k in range(3)]

    def conv(rows, at_column):
        width = rows.shape[1]
        wide = slice(at_column, at_column + width)
        pre, _ = conv_taps(taps_ref[:, wide], rows, carry[:, wide], [v[:, :width] for v in visible])
        carry[:, wide] = rows[count - 8 :]
        return pre * sigmoid(pre)

    both = conv(cs_ref[...].astype(F32), inner).astype(BF16)
    bc_ref[...] = both
    b_low, c_low = both[:, :LANES], both[:, LANES:]
    scores = nt(c_low, b_low)
    hidden_pairs = mask_of(tokens, seg)
    enter_ref[0] = state[...]
    left = iota((count, LANES), 1) < WIDTH
    b_t = jnp.transpose(b_low.astype(F32)).astype(BF16)
    factors = jnp.concatenate(halves(jnp.concatenate([step, start, end], 0)), 1)

    for low, width in groups(inner):
        wide = slice(low, low + width)
        values = conv(cv_ref[:, wide].astype(F32), low)
        steps_wide, starts, ends = jnp.split(nn(factors, picks_ref[:, wide]), 3)
        scaled = values * steps_wide
        entering = state[:, wide]
        y = starts * nn(c_low, entering.astype(BF16))
        y = y + spread(heads[2:3], low, width) * values
        inside = []
        for part in range(0, width, LANES):
            weights, mine = [], []
            for side in range(2):
                head = (low + part) // WIDTH + side
                decay = jnp.exp(cum[:, head : head + 1] - cum_t[head : head + 1] + hidden_pairs)
                here = left if side == 0 else ~left
                mine.append(jnp.where(here, scaled[:, part : part + LANES], 0.0).astype(BF16))
                weights.append((decay * scores).astype(BF16))
            inside.append(nn(jnp.concatenate(weights, 1), jnp.concatenate(mine, 0)))
        y_ref[:, wide] = (y + jnp.concatenate(inside, 1)).astype(BF16)
        state[:, wide] = spread(through, low, width) * entering + nn(
            b_t, (scaled * ends).astype(BF16)
        )
    end_ref[...] = state[...].astype(BF16)


def scan(cv, cs, halo, step_raw, ids, heads, taps_value, gathered, picks):
    tokens, inner = cv.shape
    blocks, total = tokens // SPAN, inner + 2 * STATE
    fixed = lambda n: pl.BlockSpec((8, n), lambda i: (0, 0))
    rows = lambda n: pl.BlockSpec((SPAN, n), lambda i: (i, 0))
    whole = lambda a: pl.BlockSpec(a.shape, lambda i: (0, 0), pipeline_mode=ONE)
    return pl.pallas_call(
        scan_kernel,
        grid=(blocks,),
        in_specs=[
            rows(inner), rows(2 * STATE), whole(halo), rows(LANES), whole(ids), whole(heads), whole(taps_value),
            whole(gathered), whole(picks),
        ],
        out_specs=[
            rows(inner), rows(2 * STATE), rows(LANES), rows(LANES),
            pl.BlockSpec((1, STATE, inner), lambda i: (i, 0, 0)),
            pl.BlockSpec((STATE, inner), lambda i: (0, 0)),
            pl.BlockSpec((1, 8, LANES), lambda i: (i, 0, 0)), rows(LANES), pl.BlockSpec((1, 8, SPAN), lambda i: (i, 0, 0)),
            fixed(total), fixed(total),
        ],
        out_shape=[
            jax.ShapeDtypeStruct((tokens, inner), BF16),
            jax.ShapeDtypeStruct((tokens, 2 * STATE), BF16),
            jax.ShapeDtypeStruct((tokens, LANES), F32),
            jax.ShapeDtypeStruct((tokens, LANES), F32),
            jax.ShapeDtypeStruct((blocks, STATE, inner), F32),
            jax.ShapeDtypeStruct((STATE, inner), BF16),
            jax.ShapeDtypeStruct((blocks, 8, LANES), F32),
            jax.ShapeDtypeStruct((tokens, LANES), F32),
            jax.ShapeDtypeStruct((blocks, 8, SPAN), F32),
            jax.ShapeDtypeStruct((8, total), F32),
            jax.ShapeDtypeStruct((8, total), F32),
        ],
        scratch_shapes=[
            pltpu.VMEM((8, inner + 2 * STATE), F32),
            pltpu.VMEM((STATE, inner), F32),
            pltpu.VMEM((8, LANES), F32),
            pltpu.VMEM((8, LANES), F32),
            pltpu.VMEM((8, LANES), F32),
        ],
        cost_estimate=pl.CostEstimate(
            flops=2 * tokens * inner * (2 * SPAN + 2 * STATE),
            bytes_accessed=tokens * (6 * inner + 4 * STATE + 8 * LANES),
            transcendentals=tokens * inner * 4,
        ),
        name="scan",
    )(cv, cs, halo, step_raw, ids, heads, taps_value, gathered, picks)


def gate_kernel(
    y_ref, reach_ref, bc_ref, state_ref, gate_ref, gg_ref, gain_ref, picks_ref, low_ref, sums_ref
):
    inner = y_ref.shape[1]
    c_low = bc_ref[:, LANES:]
    reach = jnp.concatenate(halves(reach_ref[...]), 1)
    squares = jnp.zeros((CHUNK, LANES), F32)
    dots = jnp.zeros((CHUNK, LANES), F32)
    for pair in range(inner // LANES):
        wide = slice(pair * LANES, (pair + 1) * LANES)
        reach_pair = nn(reach, picks_ref[:, wide])
        ssm = y_ref[:, wide].astype(F32) + reach_pair * nn(c_low, state_ref[:, wide])
        gate = gate_ref[:, wide].astype(F32)
        gated = ssm * gate * sigmoid(gate)
        weighted = gated * gain_ref[:, wide]
        low_ref[:, wide] = weighted.astype(BF16)
        squares = squares + gated * gated
        dots = dots + gg_ref[:, wide].astype(F32) * weighted
    square = jnp.sum(squares, 1, keepdims=True)
    dot = jnp.sum(dots, 1, keepdims=True)
    sums_ref[...] = jnp.transpose(jnp.where(iota((CHUNK, LANES), 1) == 0, square, dot))[:8]


def gate_sums(y, reach, bc, state_in, gate_raw, gg, gain, picks):
    tokens, inner = y.shape
    rows = lambda n: pl.BlockSpec((CHUNK, n), lambda i: (i, 0))
    whole = lambda a: pl.BlockSpec(a.shape, lambda i: (0, 0), pipeline_mode=ONE)
    return pl.pallas_call(
        gate_kernel,
        grid=(tokens // CHUNK,),
        in_specs=[
            rows(inner), rows(LANES), rows(2 * STATE), whole(state_in), rows(inner), rows(inner), whole(gain),
            whole(picks),
        ],
        out_specs=[rows(inner), pl.BlockSpec((8, CHUNK), lambda i: (0, i))],
        out_shape=[
            jax.ShapeDtypeStruct((tokens, inner), BF16),
            jax.ShapeDtypeStruct((8, tokens), F32),
        ],
        cost_estimate=pl.CostEstimate(
            flops=2 * tokens * inner * STATE, bytes_accessed=tokens * inner * 12, transcendentals=tokens * inner
        ),
        name="gate",
    )(y, reach, bc, state_in, gate_raw, gg, gain, picks)


def ungate_kernel(count, y_ref, gate_ref, gg_ref, gain_ref, reach_ref, bc_ref, in_ref, picks_ref, *refs):
    sums_refs, (gs_ref, ggr_ref, low_ref, scale_ref, gain_sum_ref, state_ref, gain_acc, state_acc) = (
        refs[:count], refs[count:]
    )
    at = pl.program_id(0)
    inner = y_ref.shape[1]

    @pl.when(at == 0)
    def _():
        gain_acc[...] = jnp.zeros_like(gain_acc)
        state_acc[...] = jnp.zeros_like(state_acc)

    sums = sum(ref[...] for ref in sums_refs)
    sums = jnp.transpose(jnp.concatenate([sums, jnp.zeros((LANES - 8, CHUNK), F32)], 0))
    all_inner = count * inner
    scale = lax.rsqrt(column(sums, 0) / all_inner + EPSILON)
    shift = scale * scale * scale * column(sums, 1) / all_inner
    scale_ref[...] = scale
    reach = jnp.concatenate(halves(reach_ref[...]), 1)
    c_low = bc_ref[:, LANES:]
    c_t = jnp.transpose(c_low.astype(F32)).astype(BF16)
    for pair in range(inner // LANES):
        wide = slice(pair * LANES, (pair + 1) * LANES)
        reach_pair = nn(reach, picks_ref[:, wide])
        ssm = y_ref[:, wide].astype(F32) + reach_pair * nn(c_low, in_ref[:, wide])
        gate, gg = gate_ref[:, wide].astype(F32), gg_ref[:, wide].astype(F32)
        sg = sigmoid(gate)
        act = gate * sg
        gated = ssm * act
        scaled = gated * scale
        low_ref[:, wide] = (scaled * gain_ref[:, wide]).astype(BF16)
        gain_acc[:, wide] += jnp.sum((gg * scaled).reshape(CHUNK // 8, 8, LANES), 0)
        grad_gated = scale * gg * gain_ref[:, wide] - gated * shift
        grad_ssm = grad_gated * act
        gs_ref[:, wide] = grad_ssm
        ggr_ref[:, wide] = (grad_gated * ssm * sg * (1.0 + gate * (1.0 - sg))).astype(BF16)
        state_acc[:, wide] += nn(c_t, (grad_ssm * reach_pair).astype(BF16))
    gain_sum_ref[...] = gain_acc[...]
    state_ref[...] = state_acc[...]


def ungate(y, gate_raw, gg, gain, reach, bc, state_in, picks, sums):
    tokens, inner = y.shape
    rows = lambda n: pl.BlockSpec((CHUNK, n), lambda i: (i, 0))
    whole = lambda a: pl.BlockSpec(a.shape, lambda i: (0, 0), pipeline_mode=ONE)
    fixed = lambda m, n: pl.BlockSpec((m, n), lambda i: (0, 0))
    return pl.pallas_call(
        partial(ungate_kernel, len(sums)),
        grid=(tokens // CHUNK,),
        in_specs=[
            rows(inner), rows(inner), rows(inner), whole(gain), rows(LANES), rows(2 * STATE), whole(state_in),
            whole(picks),
        ] + [pl.BlockSpec((8, CHUNK), lambda i: (0, i))] * len(sums),
        out_specs=[rows(inner), rows(inner), rows(inner), rows(LANES), fixed(8, inner), fixed(STATE, inner)],
        out_shape=[
            jax.ShapeDtypeStruct((tokens, inner), F32),
            jax.ShapeDtypeStruct((tokens, inner), BF16),
            jax.ShapeDtypeStruct((tokens, inner), BF16),
            jax.ShapeDtypeStruct((tokens, LANES), F32),
            jax.ShapeDtypeStruct((8, inner), F32),
            jax.ShapeDtypeStruct((STATE, inner), F32),
        ],
        scratch_shapes=[pltpu.VMEM((8, inner), F32), pltpu.VMEM((STATE, inner), F32)],
        cost_estimate=pl.CostEstimate(
            flops=2 * tokens * inner * STATE, bytes_accessed=tokens * inner * 16, transcendentals=tokens * inner
        ),
        name="ungate",
    )(y, gate_raw, gg, gain, reach, bc, state_in, picks, *sums)


def unscan_kernel(
    gs_ref, cv_ref, cv_before_ref, cs_ref, cs_before_ref, halo_ref, bc_ref, step_ref, cum_ref, tok_ref, seg_ref,
    heads_ref, taps_ref, enter_ref, kept_ref, state_in_ref, grad_end_ref, gain_sum_ref, picks_ref, sums_ref,
    value_ref, rest_ref, small_ref, head_rows_ref,
    carry, grad, taps_acc, heads_acc, skip_acc,
):
    turn = pl.program_id(0)
    at = pl.num_programs(0) - 1 - turn
    inner = gs_ref.shape[1]
    count = SPAN

    @pl.when(turn == 0)
    def _():
        carry[...] = jnp.zeros_like(carry)
        grad[...] = grad_end_ref[...]
        taps_acc[...] = jnp.zeros_like(taps_acc)
        heads_acc[...] = jnp.zeros_like(heads_acc)
        skip_acc[...] = jnp.zeros_like(skip_acc)

    first = at == 0
    tokens = tok_ref[...]
    heads = heads_ref[...]
    step_in = step_ref[...] + heads[1:2]
    step = softplus(step_in)
    log_decay = heads[0:1] * step
    cum = cum_ref[...]
    last = cum[count - 1 : count]
    start = jnp.exp(cum) * column(tokens, 7)
    end = jnp.exp(last - cum) * column(tokens, 8)
    through = start[count - 1 : count]
    cum_t = jnp.transpose(cum)
    visible = [column(tokens, 1 + k, 2 * LANES) for k in range(3)]
    seen = [column(tokens, 4 + k, 2 * LANES) for k in range(3)]
    left = iota((count, LANES), 1) < WIDTH
    b_low, c_low = bc_ref[:, :LANES], bc_ref[:, LANES:]
    scores = nt(c_low, b_low)
    hidden_pairs = mask_of(tokens, seg_ref[0, 0:1])
    c_t = jnp.transpose(c_low.astype(F32)).astype(BF16)
    kept = kept_ref[0]

    def conv(ref, before_ref, low, at_column, width):
        rows = ref[:, low : low + width].astype(F32)
        wide = slice(at_column, at_column + width)
        before = before_ref[8:16, low : low + width].astype(F32)
        before = jnp.where(first, halo_ref[:, wide].astype(F32), before)
        pre, shifted = conv_taps(taps_ref[:, wide], rows, before, [v[:, :width] for v in visible])
        return pre, shifted, sigmoid(pre)

    def unconv(grad_out, pre, sg, shifted, at_column, width):
        wide = slice(at_column, at_column + width)
        gp = grad_out * sg * (1.0 + pre * (1.0 - sg))
        eighths = lambda v: jnp.sum(v.reshape(count // 8, 8, width), 0)
        for k in range(4):
            taps_acc[8 * k : 8 * k + 8, wide] += eighths(gp * shifted[3 - k])
        taps_acc[32:40, wide] += eighths(gp)
        taps = taps_ref[:, wide]
        following = carry[:, wide]
        total = taps[3:4] * gp
        for steps in range(1, 4):
            moved = from_after(gp, following, steps) * seen[steps - 1][:, :width]
            total = total + taps[3 - steps : 4 - steps] * moved
        if at_column < inner:
            value_ref[:, wide] = total.astype(BF16)
        else:
            rest_ref[:, :width], rest_ref[:, width : 2 * width] = halves(total)
        carry[:, wide] = gp[:8]

        @pl.when(first)
        def _():
            back = jnp.zeros((8, width), F32)
            for steps in range(1, 4):
                moved = pltpu.roll(gp[:8] * visible[steps - 1][:8, :width], 8 - steps, 0)
                back = back + jnp.where(iota((8, width), 0) >= 8 - steps, taps[3 - steps : 4 - steps] * moved, 0.0)
            head_rows_ref[:, wide] = back

    grad_b = jnp.zeros((count, STATE), F32)
    grad_c = jnp.zeros((count, STATE), F32)
    grad_scores = jnp.zeros((count, count), F32)
    grad_cum = jnp.zeros((count, LANES), F32)
    grad_step = jnp.zeros((count, LANES), F32)
    at_end = jnp.zeros((8, LANES), F32)
    down = []
    factors = jnp.concatenate(halves(jnp.concatenate([step, start, end], 0)), 1)
    for low, width in groups(inner):
        wide = slice(low, low + width)
        pre, shifted, sg = conv(cv_ref, cv_before_ref, low, low, width)
        values = pre * sg
        step_wide, starts, ends = jnp.split(nn(factors, picks_ref[:, wide]), 3)
        scaled = values * step_wide
        scaled_low = scaled.astype(BF16)
        grad_y = gs_ref[:, wide]
        entering = enter_ref[0, :, wide] + spread(kept[0:1], low, width) * state_in_ref[:, wide].astype(F32)
        grad_state = grad[:, wide]
        grad_low = grad_state.astype(BF16)
        state_low, state_rest = halves(entering)
        to_end = ends * nn(b_low, grad_low)
        grad_y_in = grad_y * starts
        moved = scaled * to_end
        grad_cum = grad_cum + head_sums(grad_y_in * nn(c_low, state_low) - moved, sums_ref[wide])
        through_wide = spread(through, low, width)
        ending = jnp.sum(moved, 0, keepdims=True) + through_wide * jnp.sum(grad_state * entering, 0, keepdims=True)
        at_end = at_end + head_sums(jnp.broadcast_to(ending, (8, width)), sums_ref[wide])
        y_rest = grad_y - grad_y.astype(BF16).astype(F32)
        scaled_rest = (scaled - scaled_low.astype(F32)).astype(BF16)
        inside = []
        for part in range(0, width, LANES):
            here_lanes = slice(part, part + LANES)
            y_part, x_part = grad_y[:, here_lanes], scaled[:, here_lanes]
            y_turned, x_turned = pltpu.roll(y_rest[:, here_lanes], WIDTH, 1), pltpu.roll(x_part, WIDTH, 1)
            low_weights, low_mine = [], []
            for side in range(2):
                head = (low + part) // WIDTH + side
                here = left if side == 0 else ~left
                decay = jnp.exp(cum[:, head : head + 1] - cum_t[head : head + 1] + hidden_pairs)
                mine = jnp.where(here, y_part, 0.0).astype(BF16)
                weights = decay * scores
                grad_weights = nt(
                    jnp.concatenate([jnp.where(here, y_part, y_turned).astype(BF16), mine], 1),
                    jnp.concatenate([jnp.where(here, x_part, x_turned).astype(BF16), scaled_rest[:, here_lanes]], 1),
                )
                grad_scores = grad_scores + grad_weights * decay
                change = grad_weights * weights
                across = jnp.sum(change, 1, keepdims=True)
                down.append(jnp.sum(change, 0, keepdims=True))
                grad_cum = grad_cum + jnp.where(iota((count, LANES), 1) == head, across, 0.0)
                low_weights.append(weights.astype(BF16))
                low_mine.append(mine)
            inside.append(tn(jnp.concatenate(low_weights, 0), jnp.concatenate(low_mine, 0)))
        grad_scaled = to_end + jnp.concatenate(inside, 1)
        grad_low_in, grad_rest_in = halves(grad_y_in)
        grad_c = grad_c + nt(grad_low_in, state_low) + nt(grad_rest_in, state_low) + nt(grad_low_in, state_rest)
        grad_b = grad_b + nt((scaled * ends).astype(BF16), grad_low)
        grad[:, wide] = through_wide * grad_state + nn(c_t, grad_low_in)
        grad_step = grad_step + head_sums(grad_scaled * values, sums_ref[wide])
        skip_acc[:, wide] += jnp.sum((grad_y * values).reshape(count // 8, 8, width), 0)
        grad_values = grad_scaled * step_wide + spread(heads[2:3], low, width) * grad_y
        unconv(grad_values, pre, sg, shifted, low, width)
    down.append(jnp.zeros((LANES - len(down), count), F32))
    grad_cum = grad_cum - jnp.transpose(jnp.concatenate(down, 0))
    for part in halves(grad_scores):
        grad_c = grad_c + nn(part, b_low)
        grad_b = grad_b + tn(part, c_low)
    pre, shifted, sg = conv(cs_ref, cs_before_ref, 0, inner, 2 * STATE)
    unconv(jnp.concatenate([grad_b, grad_c], 1), pre, sg, shifted, inner, 2 * STATE)
    upper = jnp.where(iota((count, count), 0) <= iota((count, count), 1), 1.0, 0.0)
    grad_log = exact(upper, grad_cum) + at_end[0:1]
    grad_step = grad_step + heads[0:1] * grad_log
    grad_raw = grad_step * sigmoid(step_in)
    rest_ref[:, 4 * STATE :] = grad_raw.astype(BF16)
    heads_acc[...] += jnp.concatenate(
        [
            jnp.sum(grad_log * log_decay, 0, keepdims=True),
            jnp.sum(grad_raw, 0, keepdims=True),
            jnp.zeros((6, LANES), F32),
        ],
        0,
    )

    @pl.when(first)
    def _():
        down_rows = lambda v: jnp.sum(v, 0, keepdims=True)
        skip = sum(head_sums(skip_acc[:, low : low + width], sums_ref[low : low + width]) for low, width in groups(inner))
        wide = [down_rows(taps_acc[8 * k : 8 * k + 8]) for k in range(5)]
        wide += [heads_acc[0:1], heads_acc[1:2], down_rows(skip), down_rows(gain_sum_ref[...])]
        full = small_ref.shape[1]
        wide = [jnp.concatenate([v, jnp.zeros((1, full - v.shape[1]), F32)], 1) for v in wide]
        small_ref[...] = jnp.concatenate(wide + [jnp.zeros((16 - len(wide), full), F32)], 0)


def unscan(
    gs, cv, cs, halo, bc, step_raw, cum, tokens_info, seg_rows, heads, taps, enter, kept, state_in, grad_end, gain_sum,
    picks, sums, full,
):
    tokens, inner = gs.shape
    blocks = tokens // SPAN
    total = inner + 2 * STATE
    back = lambda i: blocks - 1 - i
    rows = lambda n: pl.BlockSpec((SPAN, n), lambda i: (back(i), 0))
    before = lambda n: pl.BlockSpec((16, n), lambda i: (jnp.maximum(back(i) * (SPAN // 16) - 1, 0), 0))
    whole = lambda a: pl.BlockSpec(a.shape, lambda i: (0, 0), pipeline_mode=ONE)
    fixed = lambda m, n: pl.BlockSpec((m, n), lambda i: (0, 0))
    return pl.pallas_call(
        unscan_kernel,
        grid=(blocks,),
        in_specs=[
            rows(inner), rows(inner), before(inner), rows(2 * STATE), before(2 * STATE), whole(halo), rows(2 * STATE),
            rows(LANES), rows(LANES), rows(LANES), pl.BlockSpec((1, 8, SPAN), lambda i: (back(i), 0, 0)),
            whole(heads), whole(taps), pl.BlockSpec((1, STATE, inner), lambda i: (back(i), 0, 0)),
            pl.BlockSpec((1, 8, LANES), lambda i: (back(i), 0, 0)), whole(state_in), whole(grad_end), whole(gain_sum),
            whole(picks), whole(sums),
        ],
        out_specs=[rows(inner), rows(4 * STATE + LANES), fixed(16, full), fixed(8, total)],
        out_shape=[
            jax.ShapeDtypeStruct((tokens, inner), BF16),
            jax.ShapeDtypeStruct((tokens, 4 * STATE + LANES), BF16),
            jax.ShapeDtypeStruct((16, full), F32),
            jax.ShapeDtypeStruct((8, total), F32),
        ],
        scratch_shapes=[
            pltpu.VMEM((8, total), F32),
            pltpu.VMEM((STATE, inner), F32),
            pltpu.VMEM((40, total), F32),
            pltpu.VMEM((8, LANES), F32),
            pltpu.VMEM((8, inner), F32),
        ],
        cost_estimate=pl.CostEstimate(
            flops=2 * tokens * inner * (6 * SPAN + 4 * STATE),
            bytes_accessed=tokens * (12 * inner),
            transcendentals=tokens * inner * 6,
        ),
        name="unscan",
    )(gs, cv, cv, cs, cs, halo, bc, step_raw, cum, tokens_info, seg_rows, heads, taps, enter, kept, state_in, grad_end, gain_sum, picks, sums)


def chain_kernel(
    first, size, part_ref, ggr_ref, gv_ref, gr_ref, wg_ref, wv_ref, wb_ref, ws_ref, out_ref,
    mine, outer, inner, sent_in, sent_out, came_outer, came_inner,
):
    turn = pl.program_id(0)
    items = mine.shape[0]
    place = lax.axis_index("head")
    half = size // 2
    low_side = place < half
    depth = jnp.where(low_side, place, size - 1 - place)
    toward = jnp.where(low_side, place + 1, place - 1)
    away = jnp.where(low_side, place - 1, place + 1)
    middle, edge = depth == half - 1, depth == 0
    away = jnp.where(edge, toward, away)

    def signal(target):
        pl.semaphore_signal(
            pltpu.get_barrier_semaphore(), inc=1, device_id={"head": target}, device_id_type=pl.DeviceIdType.MESH
        )

    def copy(source, target, sent, came, device):
        return pltpu.make_async_remote_copy(
            src_ref=source, dst_ref=target, send_sem=sent, recv_sem=came,
            device_id={"head": device}, device_id_type=pl.DeviceIdType.MESH,
        )

    def across(item):
        return copy(mine.at[item], inner.at[item], sent_in.at[item], came_inner.at[item], toward)

    def inward(item):
        return copy(mine.at[item], outer.at[item], sent_in.at[item], came_outer.at[item], toward)

    def outward(item):
        return copy(inner.at[item], inner.at[item], sent_out.at[item], came_inner.at[item], away)

    @pl.when(turn == 0)
    def _():
        signal(toward)

        @pl.when(jnp.logical_not(edge))
        def _():
            signal(away)
            pl.semaphore_wait(pltpu.get_barrier_semaphore(), 2)

        @pl.when(edge)
        def _():
            pl.semaphore_wait(pltpu.get_barrier_semaphore(), 1)

    @pl.when(turn < first)
    def _():
        mine[turn] = part_ref[...]

    @pl.when((turn >= first) & (turn < items) & ((turn - first) % GROUP == 0))
    def _():
        product = nt(ggr_ref[...], wg_ref[...]) + nt(gv_ref[...], wv_ref[...])
        both, steps = wb_ref.shape[0], ws_ref.shape[0]
        product = product + nn(gr_ref[:, :both], wb_ref[...]) + nn(gr_ref[:, both : 2 * both], wb_ref[...])
        product = product + nn(gr_ref[:, 2 * both : 2 * both + steps], ws_ref[...])
        for k in range(GROUP):
            mine[turn + k] = product[k * ITEM : (k + 1) * ITEM].astype(BF16)

    done = turn - behind(size)

    @pl.when(done >= 0)
    def _():
        across(done).wait_recv()

        @pl.when(middle)
        def _():
            inner[done] = (inner[done].astype(F32) + mine[done].astype(F32)).astype(BF16)

        @pl.when(jnp.logical_not(edge))
        def _():
            outward(done).start()

        out_ref[...] = inner[done]
        across(done).wait_send()

    item = turn - LAG * depth

    @pl.when((item >= 0) & (item < items))
    def _():
        @pl.when(jnp.logical_not(edge))
        def _():
            inward(item).wait_recv()
            mine[item] = (mine[item].astype(F32) + outer[item].astype(F32)).astype(BF16)

        @pl.when(middle)
        def _():
            across(item).start()

        @pl.when(jnp.logical_not(middle))
        def _():
            inward(item).start()

    @pl.when(turn == pl.num_programs(0) - 1)
    def _():
        @pl.when(jnp.logical_not(edge))
        def _():
            def wait(item, none):
                outward(item).wait_send()
                return none

            lax.fori_loop(0, items, wait, 0)


LAG = 8


def behind(size):
    return LAG * (size // 2 - 1) + 3


ITEM = 32
GROUP = 8


def chain_sums(part, ggr, grad_value, grad_rest, w_gate, w_value, w_both_t, w_step_t):
    tokens, inner = ggr.shape
    width, columns = w_gate.shape[0], grad_rest.shape[1]
    first = part.shape[0] // ITEM
    items = first + tokens // ITEM
    size = lax.axis_size("head")
    rows = lambda n, at: pl.BlockSpec((ITEM, n), lambda i: (at(i), 0))
    own = lambda n: pl.BlockSpec(
        (GROUP * ITEM, n), lambda i: (jnp.clip((i - first) // GROUP, 0, tokens // ITEM // GROUP - 1), 0)
    )
    whole = lambda a: pl.BlockSpec(a.shape, lambda i: (0, 0), pipeline_mode=ONE)
    slots = lambda: pltpu.VMEM((items, ITEM, width), BF16)
    return pl.pallas_call(
        partial(chain_kernel, first, size),
        grid=(items + behind(size),),
        in_specs=[
            rows(width, lambda i: jnp.minimum(i, first - 1)), own(inner), own(inner), own(columns), whole(w_gate),
            whole(w_value), pl.BlockSpec((2 * STATE, width), lambda i: (0, 0), pipeline_mode=ONE), whole(w_step_t),
        ],
        out_specs=rows(width, lambda i: jnp.maximum(i - behind(size), 0)),
        out_shape=jax.ShapeDtypeStruct((items * ITEM, width), BF16),
        scratch_shapes=[slots(), slots(), slots()] + [pltpu.SemaphoreType.DMA((items,))] * 4,
        compiler_params=pltpu.CompilerParams(collective_id=0, has_side_effects=True),
        cost_estimate=pl.CostEstimate(
            flops=2 * tokens * width * (2 * inner + columns), bytes_accessed=600_000_000, transcendentals=0
        ),
        name="chain",
    )(part, ggr, grad_value, grad_rest, w_gate, w_value, w_both_t, w_step_t)


def finish_kernel(
    early, scale_ref, early_a_ref, early_b_ref, late_a_ref, late_b_ref, grad_a_ref, grad_b_ref, x_ref, cot_ref, gain_ref,
    a_ref, b_ref, c_ref, mixed_ref, grad_out_ref, a_out_ref, b_out_ref, c_out_ref,
):
    at = pl.program_id(0)
    width = x_ref.shape[1]

    def half(side, early_ref, late_ref, grad_ref):
        def part(k, none):
            own = pl.ds(pl.multiple_of(k * 64, 64), 64)
            rows = pl.ds(pl.multiple_of(side * SPAN + k * 64, 64), 64)
            x = x_ref[rows, :].astype(F32)
            is_early = 2 * at + side < early
            total = jnp.where(is_early, early_ref[own, :].astype(F32), late_ref[own, :].astype(F32))
            mixed_ref[rows, :] = (x + scale_ref[rows, 0:1] * total).astype(BF16)
            inverse = lax.rsqrt(jnp.mean(x * x, -1, keepdims=True) + EPSILON)
            weighted = grad_ref[own, :].astype(F32) * gain_ref[...]
            dot = jnp.sum(weighted * x, -1, keepdims=True)
            grad_out_ref[rows, :] = cot_ref[rows, :].astype(F32) + inverse * weighted - x * (inverse**3 * dot / width)
            return none

        lax.fori_loop(0, SPAN // 64, part, 0)

    half(0, early_a_ref, late_a_ref, grad_a_ref)
    half(1, early_b_ref, late_b_ref, grad_b_ref)
    for source, target in ((a_ref, a_out_ref), (b_ref, b_out_ref), (c_ref, c_out_ref)):
        target[...] = source[...].astype(F32)


def finish(scale, out_early, chained, hidden, cotangent, gain, sums):
    tokens, width = hidden.shape
    steps = tokens // CHUNK
    early = out_early.shape[0] // SPAN
    late = tokens // SPAN - early
    rows = lambda n: pl.BlockSpec((CHUNK, n), lambda i: (i, 0))
    some = lambda at: pl.BlockSpec((SPAN, width), lambda i: (at(i), 0))
    parts = [pl.BlockSpec((a.shape[0] // steps, a.shape[1]), lambda i: (i, 0)) for a in sums]
    return pl.pallas_call(
        partial(finish_kernel, early),
        grid=(steps,),
        in_specs=[
            rows(LANES),
            some(lambda i: jnp.minimum(2 * i, early - 1)), some(lambda i: jnp.minimum(2 * i + 1, early - 1)),
            some(lambda i: jnp.maximum(2 * i - early, 0)), some(lambda i: jnp.maximum(2 * i + 1 - early, 0)),
            some(lambda i: late + 2 * i), some(lambda i: late + 2 * i + 1),
            rows(width), rows(width), pl.BlockSpec((1, width), lambda i: (0, 0)),
        ] + parts,
        out_specs=[rows(width), rows(width)] + parts,
        out_shape=[jax.ShapeDtypeStruct((tokens, width), BF16), jax.ShapeDtypeStruct((tokens, width), F32)]
        + [jax.ShapeDtypeStruct(a.shape, F32) for a in sums],
        cost_estimate=pl.CostEstimate(flops=0, bytes_accessed=80_000_000, transcendentals=0),
        name="finish",
    )(scale, out_early, out_early, chained, chained, chained, chained, hidden, cotangent, gain, *sums)


def pack_kernel(rest_ref, wb_ref, ws_ref, pg_ref, pv_ref, norm_ref, small_ref, packed_ref):
    both, steps, width = wb_ref.shape[0], ws_ref.shape[0], ws_ref.shape[1]
    state = rest_ref[:both] + rest_ref[both : 2 * both]
    step = rest_ref[2 * both : 2 * both + steps]
    products = jnp.sum(state * wb_ref[:, :width].astype(F32), 0, keepdims=True) + pg_ref[...][None] + pv_ref[...][None]
    products = products + jnp.sum(step * ws_ref[...].astype(F32), 0, keepdims=True)
    packed_ref[:both] = state
    packed_ref[both : both + 16] = rest_ref[2 * both : 2 * both + 16]
    small = small_ref[...]
    packed_ref[both + 16 :] = jnp.where(iota(small.shape, 0) == 9, products / norm_ref[...], small)


def pack(grad_rest_t, w_both_t, w_step_t, products_gate, products_value, norm, small):
    both, width = w_both_t.shape[0], w_step_t.shape[1]
    return pl.pallas_call(
        pack_kernel,
        out_shape=jax.ShapeDtypeStruct((both + 32, width), F32),
        name="pack",
    )(grad_rest_t, w_both_t, w_step_t, products_gate, products_value, norm, small)


def late_kernel(packed_ref, *parts):
    state_local, count = parts[0].shape[0] - 16, len(parts) + 1
    place = lax.axis_index("head")
    small = packed_ref[count * state_local + 16 :].astype(BF16)
    for steps, part in enumerate(parts, 1):
        at = pl.multiple_of(lax.rem(place + steps, count) * state_local, state_local)
        part[:state_local] = packed_ref[pl.ds(at, state_local), :].astype(BF16)
        part[state_local:] = small


def late_parts(packed, state_local, count):
    shape = jax.ShapeDtypeStruct((state_local + 16, packed.shape[1]), BF16)
    return pl.pallas_call(late_kernel, out_shape=[shape] * (count - 1), name="late")(packed)


def unpack_kernel(count, packed_ref, *refs):
    others, refs = refs[: count - 1], refs[count - 1 :]
    state_ref, step_ref, norm_ref, cv_ref, cvb_ref, cs_ref, csb_ref, decay_ref, bias_ref, skip_ref, gain_ref = refs
    state_local, heads, inner = state_ref.shape[0], step_ref.shape[0], cv_ref.shape[1]
    both = state_local * count
    place = lax.axis_index("head")
    own = packed_ref[pl.ds(pl.multiple_of(place * state_local, state_local), state_local), :]
    state_ref[...] = own + sum(ref[:state_local].astype(F32) for ref in others)
    step_ref[...] = packed_ref[both : both + heads]
    small = packed_ref[both + 16 :]
    total = small + sum(ref[state_local:].astype(F32) for ref in others)
    norm_ref[...] = total[9]
    cv_ref[...] = small[:4, :inner]
    cvb_ref[...] = small[4, :inner]
    for q in range(count):
        @pl.when(place == q)
        def _(q=q):
            mine = total[:8, inner + q * state_local : inner + (q + 1) * state_local]
            cs_ref[...] = mine[:4]
            csb_ref[...] = mine[4]
    decay_ref[...] = small[5, :heads]
    bias_ref[...] = small[6, :heads]
    skip_ref[...] = small[7, :heads]
    gain_ref[...] = small[8, :inner]


def unpack(packed, others, inner, heads, state_local):
    width = packed.shape[1]
    shapes = [
        (state_local, width), (heads, width), (width,), (4, inner), (inner,), (4, state_local), (state_local,),
        (heads,), (heads,), (heads,), (inner,),
    ]
    return pl.pallas_call(
        partial(unpack_kernel, len(others) + 1),
        out_shape=[jax.ShapeDtypeStruct(shape, F32) for shape in shapes],
        name="unpack",
    )(packed, *others)


def passed_along(value, axis, steps):
    count = lax.axis_size(axis)
    first, last = (max(0, -steps), min(count, count - steps))
    return lax.ppermute(value, axis, [(source, source + steps) for source in range(first, last)])


def from_all(value, axis):
    count = lax.axis_size(axis)
    moved = lambda steps: lax.ppermute(value, axis, [(s, (s + steps) % count) for s in range(count)])
    return [value] + [moved(steps) for steps in range(1, count)]


def row_major(value):
    return with_layout_constraint(value, Layout(major_to_minor=(0, 1)))


def on_device(
    hidden, segment_ids, norm_gain, w_gate, w_value, w_state, w_step, conv_value, conv_value_bias, conv_state,
    conv_state_bias, decay_log, step_bias, skip_gain, gate_gain, w_out, cotangent,
):
    tokens, width = hidden.shape
    inner, heads_local, state_local = w_value.shape[1], w_step.shape[1], w_state.shape[1]
    count = lax.axis_size("head")

    ids = segment_ids.reshape(tokens // SPAN, SPAN)
    packed, taps_value, heads, norm, gain, w_step_t, picks, sums_of = prepare(
        w_state.T, conv_state, conv_state_bias, conv_value, conv_value_bias, decay_log, step_bias, skip_gain,
        norm_gain, gate_gain, w_step.T,
    )
    gathered = lax.all_gather(packed, "head", axis=0, tiled=True)

    normed, gate_raw, cv, step_raw = project(hidden, norm, w_gate, w_value, w_step_t)
    last_ids = jnp.pad(segment_ids[tokens - 8 :].astype(F32).astype(BF16)[:, None], ((0, 0), (0, LANES - 1)))
    tail = jnp.concatenate([cv[tokens - 8 :], last_ids, normed[tokens - 8 :]], 1)
    halo = passed_along(tail, "seq", 1)
    gg = nt(cotangent, w_out).astype(BF16)
    cs = nt(normed, gathered[:, :width]).astype(BF16)
    y, bc, cum, reach, enter, local_end, kept, tokens_info, seg_rows, taps, rim = scan(
        cv, cs, halo, step_raw, ids, heads, taps_value, gathered, picks
    )
    state_in = passed_along(local_end, "seq", 1)
    low, sums = gate_sums(y, reach, bc, state_in, gate_raw, gg, gain, picks)
    early = EARLY * ITEM
    out_early = lax.psum(nn(low[:early], w_out).astype(BF16), "head")
    sums = from_all(sums, "head")
    out_late = nn(low[early:], w_out).astype(BF16)

    gs, grad_gate_raw, gate_low, scale, gain_sum, grad_state_in = ungate(
        y, gate_raw, gg, gain, reach, bc, state_in, picks, sums
    )
    grad_end = passed_along(grad_state_in, "seq", -1)
    grad_w_out = row_major(tn(gate_low, cotangent))
    grad_value, grad_rest, small, head_rows = unscan(
        gs, cv, cs, rim, bc, step_raw, cum, tokens_info, seg_rows, heads, taps, enter, kept, state_in, grad_end,
        gain_sum, picks, sums_of, width,
    )
    from_next = passed_along(head_rows, "seq", -1)
    grad_w_gate = row_major(tn(normed, grad_gate_raw))
    products_gate = jnp.sum(w_gate.astype(F32) * grad_w_gate, 1)

    def with_next(a, low, high):
        tail = (a[tokens - 8 :, : high - low].astype(F32) + from_next[:, low:high]).astype(BF16)
        return lax.dynamic_update_slice(a, tail, (tokens - 8, 0))

    grad_value = with_next(grad_value, 0, inner)
    grad_rest = with_next(grad_rest, inner, inner + 2 * STATE)
    grad_w_value = row_major(tn(normed, grad_value))
    grad_rest_t = row_major(tn(grad_rest, normed))
    chained = chain_sums(out_late, grad_gate_raw, grad_value, grad_rest, w_gate, w_value, gathered, w_step_t)

    packed = pack(
        grad_rest_t, gathered, w_step_t, products_gate,
        jnp.sum(w_value.astype(F32) * grad_w_value, 1), norm, small,
    )
    weights = lax.psum(tuple(a.astype(BF16) for a in (grad_w_gate, grad_w_value, grad_w_out)), "seq")
    packed = lax.psum(packed, "seq")

    others = [
        lax.ppermute(part, "head", [(s, (s + steps) % count) for s in range(count)])
        for steps, part in enumerate(late_parts(packed, state_local, count), 1)
    ]
    mixed, grad_hidden, *weights = finish(scale, out_early, chained, hidden, cotangent, norm, weights)
    state_t, step_t, *rest = unpack(packed, others, inner, heads_local, state_local)
    return (mixed, grad_hidden, rest[0], weights[0], weights[1], state_t.T, step_t.T, *rest[1:], weights[2])


def solution(mesh):
    columns, split = P(None, "head"), P("head")
    rows = P("seq", None)

    return jax.shard_map(
        on_device,
        mesh=mesh,
        in_specs=(
            rows, P("seq"), P(), columns, columns, columns, columns, columns, split, columns, split, split, split,
            split, split, P("head", None), rows,
        ),
        out_specs=(
            rows, rows, P(), columns, columns, columns, columns, columns, split, columns, split, split, split, split,
            split, P("head", None),
        ),
        check_vma=False,
    )
```
